256 devices in a mesh: grp: 2 (over z), dap: 128 (over y, x, core).
Axes of the slice: x: 8, y: 8, z: 2, core: 2. Of those that a mesh axis runs over, the one named last changes fastest.
The devices are a block of a 8x8x16 slice.
Arguments:
- homolog_stack_tensor: bfloat16 [512, 512, 256], P(('grp', 'dap')), parts along dimension 0, may hold values from -6.5 to 6.5
- occupancy_indicator: int32 [512, 512], P('grp'), parts along dimension 0, may hold values from 0 to 1, as said below
- chain_existence_flags: int32 [512], P('grp'), parts along dimension 0, may hold values from 0 to 1, as said below
- focus_normal_factor: float32 [256], replicated, may hold values from 0.25 to 1.75
- focus_normal_addend: float32 [256], replicated, may hold values from -3 to 3
- probe_index_weights: bfloat16 [256, 512], replicated, may hold values from -3 to 3
- payload_valve_weights: bfloat16 [256, 512], replicated, may hold values from -0.375 to 0.375
- logistic_valve_addend: float32 [256], replicated, may hold values from -4 to 4
- focus_exit_weights: bfloat16 [256, 256], replicated, may hold values from -0.375 to 0.375
- focus_exit_addend: float32 [256], replicated, may hold values from -3 to 3
- product_mean_layer_stretch: float32 [256], replicated, may hold values from 0.25 to 1.75
- product_mean_layer_shift: float32 [256], replicated, may hold values from -2 to 2
- twin_map_matrix: bfloat16 [256, 64], replicated, may hold values from -0.375 to 0.375
- twin_map_shift: float32 [64], replicated, may hold values from -2 to 2
- couple_map_matrix: bfloat16 [1024, 128], replicated, may hold values from -0.75 to 0.75
- couple_map_shift: float32 [128], replicated, may hold values from -3 to 3
Outputs:
- alignment_after: bfloat16 [512, 512, 256], P('grp', 'dap'), parts along dimension 0
- pair_features_after: bfloat16 [1024, 512, 128], P(('grp', 'dap')), parts along dimension 0
The draws below stay inside these ranges and needn't reach their ends.
There are 2 independent parts, one for each index of `grp`. The reference program is written for one: setup_inputs(seed, part) draws one part's arguments, and reference() takes and returns one part's arrays. A program takes and returns all parts, laid end to end along the dimension named above; an argument that names none is the same for every part. Nothing has to cross between parts.
Inputs may be any that keep to these rules, and one draw needn't show every extreme that they name: `chain_existence_flags`: 1 for the first 128 sequences, 0 for the last one. `occupancy_indicator`: every sequence is 0 from some residue on (the last residue always, never more than the last 256); before it sequence 0 is all 1 and the others have gaps.
All inputs are finite; a program needn't handle non-finite values.
Results may differ from the reference program's by a relative error of at most 0.008.
Values may be sent and summed in bfloat16 or wider, within the bound.
A program may use at most 64 MiB of HBM per device.

```python
import jax
import jax.numpy as jnp
from jax import lax

ALIGN_CHANNELS = 256
HEAD_COUNT = 8
HEAD_CHANNELS = 32
OUTER_CHANNELS = 32
PAIR_DIM = 128
SITES_EACH_SLICE = 4
SEQUENCE_COUNT = 256
RESIDUE_COUNT = 512


def draw_homolog_stack_tensor(key, part):
    random_root_key = jax.random.fold_in(jax.random.fold_in(key, 101), 0)
    value_vectors = jax.random.normal(random_root_key, (SEQUENCE_COUNT, RESIDUE_COUNT, ALIGN_CHANNELS), jnp.float32)
    return jnp.clip(value_vectors, -6.5, 6.5).astype(jnp.bfloat16)


def draw_probe_index_weights(key, part):
    query_seed_value, second_seed_value = jax.random.split(jax.random.fold_in(key, 202))
    inner_channel_width = HEAD_COUNT * HEAD_CHANNELS
    square_root_width = jnp.sqrt(jnp.float32(ALIGN_CHANNELS))
    query_rows_all = jnp.clip(jax.random.normal(query_seed_value, (ALIGN_CHANNELS, inner_channel_width), jnp.float32), -6.0, 6.0) / square_root_width
    key_portion = jnp.clip(jax.random.normal(second_seed_value, (ALIGN_CHANNELS, inner_channel_width), jnp.float32), -6.0, 6.0) / square_root_width
    combined = jnp.concatenate([query_rows_all, key_portion], axis=1)
    return jnp.clip(combined, -3.0, 3.0).astype(jnp.bfloat16)


def draw_chain_existence_flags(key, part):
    coin_flips = jax.random.randint(jax.random.fold_in(key, 303), (SEQUENCE_COUNT,), 0, 2)
    position = jnp.arange(SEQUENCE_COUNT, dtype=jnp.int32)
    forced_on = position < SEQUENCE_COUNT // 2
    forced_off = position == SEQUENCE_COUNT - 1
    return jnp.where(forced_on, 1, jnp.where(forced_off, 0, coin_flips)).astype(jnp.int32)


def draw_occupancy_indicator(key, part):
    length_key, gap_key = jax.random.split(jax.random.fold_in(key, 404))
    length = jax.random.randint(length_key, (), RESIDUE_COUNT // 2, RESIDUE_COUNT)
    gap_draw = jax.random.randint(gap_key, (SEQUENCE_COUNT, RESIDUE_COUNT), 0, 8)
    inside = jnp.arange(RESIDUE_COUNT, dtype=jnp.int32)[None, :] < length
    first_row = jnp.arange(SEQUENCE_COUNT, dtype=jnp.int32)[:, None] == 0
    return (inside & ((gap_draw != 0) | first_row)).astype(jnp.int32)


def gaussian(own_key, shape, scale, limit, kind=jnp.bfloat16):
    entries = jax.random.normal(own_key, shape, jnp.float32) * scale
    return jnp.minimum(jnp.maximum(entries, -limit), limit).astype(kind)


def setup_inputs(seed: int = 0, part: int = 0) -> dict:
    key_list = jax.random.split(jax.random.key(seed), 17)
    part_keys = jax.random.split(jax.random.fold_in(key_list[16], part), 17)
    return {
        "homolog_stack_tensor": draw_homolog_stack_tensor(jax.random.fold_in(jax.random.fold_in(key_list[16], part), 71), part),
        "occupancy_indicator": draw_occupancy_indicator(jax.random.fold_in(jax.random.fold_in(key_list[16], part), 71), part),
        "chain_existence_flags": draw_chain_existence_flags(jax.random.fold_in(jax.random.fold_in(key_list[16], part), 71), part),
        "focus_normal_factor": jnp.clip(1.0 + 0.15 * jax.random.normal(key_list[3], (ALIGN_CHANNELS,), jnp.float32), 0.25, 1.75),
        "focus_normal_addend": gaussian(key_list[4], (ALIGN_CHANNELS,), 0.5, 3.0, jnp.float32),
        "probe_index_weights": draw_probe_index_weights(jax.random.fold_in(key_list[16], 71), part),
        "payload_valve_weights": gaussian(key_list[6], (ALIGN_CHANNELS, 2 * HEAD_COUNT * HEAD_CHANNELS), ALIGN_CHANNELS ** -0.5, 0.375),
        "logistic_valve_addend": gaussian(key_list[7], (HEAD_COUNT * HEAD_CHANNELS,), 1.0, 4.0, jnp.float32),
        "focus_exit_weights": gaussian(key_list[8], (HEAD_COUNT * HEAD_CHANNELS, ALIGN_CHANNELS), (HEAD_COUNT * HEAD_CHANNELS) ** -0.5, 0.375),
        "focus_exit_addend": gaussian(key_list[9], (ALIGN_CHANNELS,), 0.5, 3.0, jnp.float32),
        "product_mean_layer_stretch": jnp.clip(1.0 + 0.15 * jax.random.normal(key_list[10], (ALIGN_CHANNELS,), jnp.float32), 0.25, 1.75),
        "product_mean_layer_shift": gaussian(key_list[11], (ALIGN_CHANNELS,), 0.3, 2.0, jnp.float32),
        "twin_map_matrix": gaussian(key_list[12], (ALIGN_CHANNELS, 2 * OUTER_CHANNELS), ALIGN_CHANNELS ** -0.5, 0.375),
        "twin_map_shift": gaussian(key_list[13], (2 * OUTER_CHANNELS,), 0.3, 2.0, jnp.float32),
        "couple_map_matrix": gaussian(key_list[14], (OUTER_CHANNELS * OUTER_CHANNELS, PAIR_DIM), (OUTER_CHANNELS * OUTER_CHANNELS // 16) ** -0.5, 0.75),
        "couple_map_shift": gaussian(key_list[15], (PAIR_DIM,), 0.5, 3.0, jnp.float32),
    }


EPSILON = 1e-05
MASKED = -100000.0

def layer_norm(value_vectors, scale_vec, shift_vec):
    widened = value_vectors.astype(jnp.float32)
    centred = widened - lax.optimization_barrier(jnp.mean(widened, axis=-1, keepdims=True))
    variance = lax.optimization_barrier(jnp.mean(centred * centred, axis=-1, keepdims=True))
    scaled = centred * lax.rsqrt(variance + EPSILON)
    return (scaled * scale_vec.astype(jnp.float32) + shift_vec.astype(jnp.float32)).astype(jnp.bfloat16)

def heed_across_lanes(vertical_pieces, present_mask, focus_normal_factor, focus_normal_addend, probe_index_weights, payload_valve_weights, logistic_valve_addend, focus_exit_weights, focus_exit_addend):
    seq_count, res_count, feature_width = vertical_pieces.shape
    inner_channel_width = HEAD_COUNT * HEAD_CHANNELS
    normed = layer_norm(vertical_pieces, focus_normal_factor, focus_normal_addend).reshape(seq_count * res_count, feature_width)
    query_key = jnp.dot(normed, probe_index_weights, preferred_element_type=jnp.float32)
    value_gate = jnp.dot(normed, payload_valve_weights, preferred_element_type=jnp.float32)
    head_shape = (seq_count, res_count, HEAD_COUNT, HEAD_CHANNELS)
    query_rows_all = (query_key[:, :inner_channel_width] * HEAD_CHANNELS ** (-0.5)).astype(jnp.bfloat16).reshape(head_shape)
    key_rows = query_key[:, inner_channel_width:].astype(jnp.bfloat16).reshape(head_shape)
    value_rows = value_gate[:, :inner_channel_width].astype(jnp.bfloat16).reshape(head_shape)
    gating = jax.nn.sigmoid(value_gate[:, inner_channel_width:] + logistic_valve_addend.astype(jnp.float32))
    scores = jnp.einsum('srhd,trhd->rhst', query_rows_all.astype(jnp.float32), key_rows.astype(jnp.float32))
    allowed = jnp.transpose(present_mask > 0)[:, None, None, :]
    scores = jnp.where(allowed, scores, MASKED)
    exponent = jnp.exp(scores - lax.optimization_barrier(jnp.max(scores, axis=-1, keepdims=True)))
    weights = (exponent / lax.optimization_barrier(jnp.sum(exponent, axis=-1, keepdims=True))).astype(jnp.bfloat16)
    attended = jnp.einsum('rhst,trhd->srhd', weights.astype(jnp.float32), value_rows.astype(jnp.float32))
    gated_rows = (attended.reshape(seq_count * res_count, inner_channel_width) * gating).astype(jnp.bfloat16)
    update = jnp.dot(gated_rows, focus_exit_weights, preferred_element_type=jnp.float32) + focus_exit_addend.astype(jnp.float32)
    return (vertical_pieces.astype(jnp.float32) + update.reshape(seq_count, res_count, feature_width)).astype(jnp.bfloat16)

def project_pairs(revised_tensor, present_mask, product_mean_layer_stretch, product_mean_layer_shift, twin_map_matrix, twin_map_shift):
    seq_count, res_count, feature_width = revised_tensor.shape
    normed = layer_norm(revised_tensor, product_mean_layer_stretch, product_mean_layer_shift).reshape(seq_count * res_count, feature_width)
    projected = jnp.dot(normed, twin_map_matrix, preferred_element_type=jnp.float32) + twin_map_shift.astype(jnp.float32)
    projected = projected.reshape(seq_count, res_count, 2 * OUTER_CHANNELS) * present_mask[:, :, None].astype(jnp.float32)
    projected = projected.astype(jnp.bfloat16)
    return (projected[:, :, :OUTER_CHANNELS], projected[:, :, OUTER_CHANNELS:])

def pair_tile(left_rows, right_cols, live_rows, live_cols, couple_map_matrix, couple_map_shift):
    row_count = left_rows.shape[1]
    col_count = right_cols.shape[1]
    outer_sum = jnp.einsum('sic,sje->ijce', left_rows.astype(jnp.float32), right_cols.astype(jnp.float32))
    counts = jnp.einsum('si,sj->ij', live_rows.astype(jnp.float32), live_cols.astype(jnp.float32))
    mean_terms = (outer_sum.reshape(row_count, col_count, OUTER_CHANNELS * OUTER_CHANNELS) / jnp.maximum(counts, 1.0)[:, :, None]).astype(jnp.bfloat16)
    result = jnp.dot(mean_terms.reshape(row_count * col_count, OUTER_CHANNELS * OUTER_CHANNELS), couple_map_matrix, preferred_element_type=jnp.float32)
    result = result + couple_map_shift.astype(jnp.float32)
    return result.astype(jnp.bfloat16).reshape(row_count, col_count, PAIR_DIM)

def reference(homolog_stack_tensor, occupancy_indicator, chain_existence_flags, focus_normal_factor, focus_normal_addend, probe_index_weights, payload_valve_weights, logistic_valve_addend, focus_exit_weights, focus_exit_addend, product_mean_layer_stretch, product_mean_layer_shift, twin_map_matrix, twin_map_shift, couple_map_matrix, couple_map_shift):
    present_mask = occupancy_indicator * chain_existence_flags[:, None]
    block_count = RESIDUE_COUNT // SITES_EACH_SLICE

    def column_block(block_index):
        opening_index = (block_index * SITES_EACH_SLICE).astype(jnp.int32)
        homolog_owned_block = lax.dynamic_slice_in_dim(homolog_stack_tensor, opening_index, SITES_EACH_SLICE, 1)
        current_fraction = lax.dynamic_slice_in_dim(present_mask, opening_index, SITES_EACH_SLICE, 1)
        revised_tensor = heed_across_lanes(homolog_owned_block, current_fraction, focus_normal_factor, focus_normal_addend, probe_index_weights, payload_valve_weights, logistic_valve_addend, focus_exit_weights, focus_exit_addend)
        left_part, right_part = project_pairs(revised_tensor, current_fraction, product_mean_layer_stretch, product_mean_layer_shift, twin_map_matrix, twin_map_shift)
        return (revised_tensor, left_part, right_part)
    refreshed_blocks, left_blocks, right_blocks = lax.map(column_block, jnp.arange(block_count, dtype=jnp.int32))
    alignment_after = jnp.transpose(refreshed_blocks, (1, 0, 2, 3)).reshape(SEQUENCE_COUNT, RESIDUE_COUNT, ALIGN_CHANNELS)
    left_all = jnp.transpose(left_blocks, (1, 0, 2, 3)).reshape(SEQUENCE_COUNT, RESIDUE_COUNT, OUTER_CHANNELS)
    right_all = jnp.transpose(right_blocks, (1, 0, 2, 3)).reshape(SEQUENCE_COUNT, RESIDUE_COUNT, OUTER_CHANNELS)

    def pair_block(block_index):
        opening_index = (block_index * SITES_EACH_SLICE).astype(jnp.int32)
        rows_left = lax.dynamic_slice_in_dim(left_all, opening_index, SITES_EACH_SLICE, 1)
        rows_live = lax.dynamic_slice_in_dim(present_mask, opening_index, SITES_EACH_SLICE, 1)
        return pair_tile(rows_left, right_all, rows_live, present_mask, couple_map_matrix, couple_map_shift)
    pair_blocks = lax.map(pair_block, jnp.arange(block_count, dtype=jnp.int32))
    pair_features_after = pair_blocks.reshape(RESIDUE_COUNT, RESIDUE_COUNT, PAIR_DIM)
    return (alignment_after, pair_features_after)
```

```python
import functools

import jax
import jax.numpy as jnp
from jax import lax
from jax.experimental import pallas as pl
from jax.experimental.pallas import tpu as pltpu
from jax.sharding import Mesh
from jax.sharding import PartitionSpec as P

HEAD_COUNT = 8
HEAD_CHANNELS = 32
OUTER_CHANNELS = 32
PAIR_DIM = 128
DAP = ("dap_0", "dap_1", "dap_2")
GRP_DAP = ("grp", "dap_0", "dap_1", "dap_2")
F32 = jnp.float32
BF16 = jnp.bfloat16
VMEM_LIMIT = 60 * 1024 * 1024


EPSILON = 1e-05
MASKED = -100000.0


def in_blocks(value, dim, count):
    shape = value.shape
    parts = value.reshape(*shape[:dim], count, shape[dim] // count, *shape[dim + 1 :])
    return jnp.moveaxis(parts, dim, 0)


def joined_along(parts, dim):
    parts = jnp.moveaxis(parts, 0, dim)
    shape = parts.shape
    return parts.reshape(*shape[:dim], shape[dim] * shape[dim + 1], *shape[dim + 2 :])


def exchange_in_order(parts, axes, turns):
    shape = [lax.axis_size(a) for a in axes]
    parts = parts.reshape(*shape, *parts.shape[1:])
    for k in turns:
        parts = lax.all_to_all(parts, axes[k], split_axis=k, concat_axis=k, tiled=True)
    return parts.reshape(-1, *parts.shape[len(axes) :])


def exchange_by_chip(value, groups, turns, split_dim, concat_dim):
    count = lax.axis_size(groups[0]) * lax.axis_size(groups[1])
    parts = in_blocks(value, split_dim, count)
    return joined_along(exchange_in_order(parts, groups, turns), concat_dim)


def normalize(widened, gain, offset):
    centred = widened - jnp.mean(widened, axis=-1, keepdims=True)
    variance = jnp.mean(centred * centred, axis=-1, keepdims=True)
    return (centred * lax.rsqrt(variance + EPSILON) * gain + offset).astype(BF16)


def contract_lanes(a, b):
    return lax.dot_general(a, b, (((1,), (1,)), ((), ())), preferred_element_type=F32)


def attend_kernel(
    x_ref, keep_ref, gain_ref, offset_ref, qk_ref, vg_ref, gate_ref, exit_ref, exit_add_ref,
    gain2_ref, offset2_ref, twin_l_ref, twin_r_ref, shift_l_ref, shift_r_ref, live_l_ref,
    live_r_ref, after_ref, left_ref, right_ref, left_sum, right_sum,
):
    sites, seqs, width = x_ref.shape
    inner = HEAD_COUNT * HEAD_CHANNELS
    head_of_lane = lax.broadcasted_iota(jnp.int32, (1, inner), 1) // HEAD_CHANNELS
    left_sum[...] = jnp.zeros_like(left_sum)
    right_sum[...] = jnp.zeros_like(right_sum)

    def one_site(r, carry):
        x = x_ref[r].astype(F32)
        normed = normalize(x, gain_ref[...], offset_ref[...])
        query_key = jnp.dot(normed, qk_ref[...], preferred_element_type=F32)
        value_gate = jnp.dot(normed, vg_ref[...], preferred_element_type=F32)
        query = (query_key[:, :inner] * HEAD_CHANNELS ** (-0.5)).astype(BF16)
        key = query_key[:, inner:].astype(BF16)
        value = value_gate[:, :inner].astype(BF16)
        gate = jax.nn.sigmoid(value_gate[:, inner:] + gate_ref[...])
        keep = keep_ref[r] > 0
        mixed = jnp.zeros((seqs, inner), F32)
        for h in range(HEAD_COUNT):
            own = head_of_lane == h
            query_h = query * own.astype(F32).astype(BF16)
            scores = jnp.where(keep, contract_lanes(query_h, key), MASKED)
            exponent = jnp.exp(scores - jnp.max(scores, axis=-1, keepdims=True))
            total = jnp.sum(exponent, axis=-1, keepdims=True)
            part = jnp.dot(exponent.astype(BF16), value, preferred_element_type=F32)
            mixed = jnp.where(own, part * (1.0 / total), mixed)
        gated = (mixed * gate).astype(BF16)
        update = jnp.dot(gated, exit_ref[...], preferred_element_type=F32) + exit_add_ref[...]
        after = (x + update).astype(BF16)
        after_ref[r] = after
        again = normalize(after.astype(F32), gain2_ref[...], offset2_ref[...])
        site_of_lane = (
            lax.broadcasted_iota(jnp.int32, (1, sites * OUTER_CHANNELS), 1) // OUTER_CHANNELS
        )
        site_of_row = lax.broadcasted_iota(jnp.int32, (sites * OUTER_CHANNELS, 1), 0) % sites
        twin_l = twin_l_ref[...] * (site_of_lane == r).astype(F32).astype(BF16)
        twin_r = twin_r_ref[...] * (site_of_row == r).astype(F32).astype(BF16)
        left_sum[...] += jnp.dot(again, twin_l, preferred_element_type=F32)
        right_sum[...] += contract_lanes(twin_r, again)
        return carry

    lax.fori_loop(0, sites, one_site, 0)
    left_ref[...] = ((left_sum[...] + shift_l_ref[...]) * live_l_ref[...]).astype(BF16)
    right_ref[...] = ((right_sum[...] + shift_r_ref[...]) * live_r_ref[...]).astype(BF16)


def attend(x, keep, *rest):
    sites, seqs, width = x.shape
    pack = sites * OUTER_CHANNELS
    return pl.pallas_call(
        attend_kernel,
        out_shape=(
            jax.ShapeDtypeStruct(x.shape, BF16),
            jax.ShapeDtypeStruct((seqs, pack), BF16),
            jax.ShapeDtypeStruct((pack, seqs), BF16),
        ),
        scratch_shapes=[pltpu.VMEM((seqs, pack), F32), pltpu.VMEM((pack, seqs), F32)],
        compiler_params=pltpu.CompilerParams(vmem_limit_bytes=VMEM_LIMIT),
        name="attend",
    )(x, keep, *rest)


def pair_kernel(
    right_ref, left_ref, live_t_ref, live_l_ref, couple_ref, shift_ref, out_ref,
    inverse, terms, blocks,
):
    step = pl.program_id(0)
    owners, pack, seqs = right_ref.shape
    sites = out_ref.shape[0]
    chip_rows = 2 * sites
    halves = OUTER_CHANNELS // 2

    @pl.when(step == 0)
    def _():
        counts = jnp.dot(live_t_ref[...], live_l_ref[...], preferred_element_type=F32)
        inverse[...] = 1.0 / jnp.maximum(counts, 1.0)
        blocks[...] = jnp.zeros_like(blocks)
        for e in range(OUTER_CHANNELS):
            for i in range(sites):
                row = (e % 2) * pack + i * OUTER_CHANNELS
                blocks[e // 2, row : row + OUTER_CHANNELS, i * PAIR_DIM : (i + 1) * PAIR_DIM] = (
                    couple_ref[e]
                )

    lower = lax.broadcasted_iota(jnp.int32, (1, chip_rows, 1), 1) < sites
    left = left_ref[...]

    def four(u, carry):
        quad = right_ref[pl.ds(4 * u, 4)].reshape(4 * pack, seqs)
        sums = jnp.dot(quad, left, preferred_element_type=F32)
        sums = sums.reshape(4, halves, chip_rows, pack)
        even, odd = [], []
        for t in range(2):
            a, b = sums[2 * t], sums[2 * t + 1]
            first = pl.multiple_of((step * owners + 4 * u + 2 * t) * sites, chip_rows)
            scale = inverse[pl.ds(first, chip_rows), :][None]
            even.append(jnp.where(lower, a, pltpu.roll(b, sites, 1)) * scale)
            odd.append(jnp.where(lower, pltpu.roll(a, sites, 1), b) * scale)
        rows = pl.ds(pl.multiple_of((step * owners + 4 * u) * sites, 2 * chip_rows), 2 * chip_rows)
        terms[:, rows, :pack] = jnp.concatenate(even, axis=1).astype(BF16)
        terms[:, rows, pack:] = jnp.concatenate(odd, axis=1).astype(BF16)
        return carry

    lax.fori_loop(0, owners // 4, four, 0)

    @pl.when(step == pl.num_programs(0) - 1)
    def _():
        total = jnp.dot(terms[0], blocks[0], preferred_element_type=F32)
        for e in range(1, halves):
            total = total + jnp.dot(terms[e], blocks[e], preferred_element_type=F32)
        for i in range(sites):
            part = total[:, i * PAIR_DIM : (i + 1) * PAIR_DIM] + shift_ref[...]
            out_ref[i] = part.astype(BF16)


def pairs(right_all, left, live_t, live_l, couple, shift):
    owners, pack, seqs = right_all.shape
    residues = live_t.shape[0]
    sites = pack // OUTER_CHANNELS
    steps = 4
    whole = lambda *shape: pl.BlockSpec(shape, lambda g: (0,) * len(shape))
    return pl.pallas_call(
        pair_kernel,
        grid=(steps,),
        in_specs=[
            pl.BlockSpec((owners // steps, pack, seqs), lambda g: (g, 0, 0)),
            whole(*left.shape),
            whole(*live_t.shape),
            whole(*live_l.shape),
            whole(*couple.shape),
            whole(*shift.shape),
        ],
        out_specs=whole(sites, residues, PAIR_DIM),
        out_shape=jax.ShapeDtypeStruct((sites, residues, PAIR_DIM), BF16),
        scratch_shapes=[
            pltpu.VMEM((residues, pack), F32),
            pltpu.VMEM((OUTER_CHANNELS // 2, residues, 2 * pack), BF16),
            pltpu.VMEM((OUTER_CHANNELS // 2, 2 * pack, sites * PAIR_DIM), BF16),
        ],
        compiler_params=pltpu.CompilerParams(
            vmem_limit_bytes=VMEM_LIMIT, dimension_semantics=("arbitrary",)
        ),
        name="pairs",
    )(right_all, left, live_t, live_l, couple, shift)


GATHER_RING = pltpu.CompilerParams(
    vmem_limit_bytes=VMEM_LIMIT, collective_id=1, has_side_effects=True
)


def ring_order(size):
    far = size // 2
    offsets = [0]
    for hop in range(1, far):
        offsets += [-hop, hop]
    offsets.append(far)
    events = []
    for hop in range(1, far + 1):
        events.append((3.0 * hop, 0, hop, 0))
    for offset in offsets:
        ready = 3.0 * abs(offset)
        for hop in range(1, far + 1):
            events.append((ready + 2.7 * hop + 0.01, 1, hop, offset))
    return sorted(events, key=lambda event: event[:2]), offsets


def gather_kernel(size, own_ref, all_ref, held, p_recv, s_recv, x_recv, send_sem, out_sem, in_sem):
    far = size // 2
    y, x, core = (lax.axis_index(a) for a in DAP)
    half = own_ref.shape[0] // 2

    def at(first, second):
        row = jnp.where(core == 0, second, first)
        column = jnp.where(core == 0, first, second)
        return lax.rem(row + size, size), lax.rem(column + size, size)

    main = jnp.where(core == 0, x, y)
    side = jnp.where(core == 0, y, x)

    def device(first, second):
        row, column = at(first, second)
        return {"dap_0": row, "dap_1": column}

    def slot(first, second, which):
        row, column = at(first, second)
        return (row * size + column) * 2 + which

    partner = {"dap_2": 1 - core}
    neighbours = [
        device(main + 1, side), device(main - 1, side), device(main, side + 1),
        device(main, side - 1), partner,
    ]
    barrier = pltpu.get_barrier_semaphore()
    own_copy = pltpu.make_async_copy(own_ref, held.at[slot(main, side, core)], in_sem)
    own_copy.start()
    for neighbour in neighbours:
        pl.semaphore_signal(
            barrier, inc=1, device_id=neighbour, device_id_type=pl.DeviceIdType.MESH
        )
    pl.semaphore_wait(barrier, len(neighbours))
    own_copy.wait()

    def piece(first, second, which, hop, sign):
        ref = held.at[slot(first, second, which)]
        if hop < far:
            return ref
        return ref.at[pl.ds(0 if sign > 0 else half, half)]

    def remote(ref, recv, target):
        return pltpu.make_async_remote_copy(
            src_ref=ref, dst_ref=ref, send_sem=send_sem, recv_sem=recv,
            device_id=target, device_id_type=pl.DeviceIdType.MESH,
        )

    def along_main(hop, sign):
        ref = piece(main - sign * (hop - 1), side, core, hop, sign)
        remote(ref, p_recv.at[(sign + 1) // 2, hop - 1], device(main + sign, side)).start()

    def along_side(offset, index, hop, sign):
        ref = piece(main + offset, side - sign * (hop - 1), core, hop, sign)
        remote(ref, s_recv.at[index, (sign + 1) // 2, hop - 1], device(main, side + sign)).start()

    def finished(first, second, order):
        ref = held.at[slot(first, second, core)]
        remote(ref, x_recv.at[order], partner).start()
        pltpu.make_async_copy(ref, all_ref.at[slot(first, second, core)], out_sem).start()
        done.append((first, second))

    def from_partner(order):
        first, second = done[order]
        ref = held.at[swapped_slot(first, second)]
        remote(ref, x_recv.at[order], partner).wait_recv()
        pltpu.make_async_copy(ref, all_ref.at[swapped_slot(first, second)], out_sem).start()

    def swapped_slot(first, second):
        d_first, d_second = first - main, second - side
        row = jnp.where(core == 0, main_row + d_first, main_row + d_second)
        column = jnp.where(core == 0, main_column + d_second, main_column + d_first)
        row, column = lax.rem(row + size, size), lax.rem(column + size, size)
        return (row * size + column) * 2 + (1 - core)

    main_row, main_column = y, x
    done = []
    events, offsets = ring_order(size)
    for sign in (1, -1):
        along_main(1, sign)
        along_side(0, 0, 1, sign)
    finished(main, side, 0)
    lag, taken = 6, 0
    for _, kind, hop, offset in events:
        if kind == 0:
            for sign in (1, -1):
                ref = piece(main - sign * hop, side, core, hop, sign)
                remote(ref, p_recv.at[(sign + 1) // 2, hop - 1], partner).wait_recv()
                if hop < far:
                    along_main(hop + 1, sign)
                    index = offsets.index(-sign * hop)
                    for way in (1, -1):
                        along_side(-sign * hop, index, 1, way)
                    finished(main - sign * hop, side, len(done))
            if hop == far:
                for way in (1, -1):
                    along_side(far, offsets.index(far), 1, way)
                finished(main + far, side, len(done))
        else:
            index = offsets.index(offset)
            for sign in (1, -1):
                ref = piece(main + offset, side - sign * hop, core, hop, sign)
                remote(ref, s_recv.at[index, (sign + 1) // 2, hop - 1], partner).wait_recv()
                if hop < far:
                    along_side(offset, index, hop + 1, sign)
                    finished(main + offset, side - sign * hop, len(done))
            if hop == far:
                finished(main + offset, side + far, len(done))
        while taken < len(done) - lag:
            from_partner(taken)
            taken += 1
    while taken < len(done):
        from_partner(taken)
        taken += 1
    sent = (size - 1) * (size + 1) + size * size
    drained = held.at[pl.ds(0, sent)]
    pltpu.make_async_copy(drained, drained, send_sem).wait()
    pltpu.make_async_copy(held, all_ref, out_sem).wait()


def gather_right(own, size):
    owners = 2 * size * size
    return pl.pallas_call(
        functools.partial(gather_kernel, size),
        out_shape=jax.ShapeDtypeStruct((owners, *own.shape), own.dtype),
        in_specs=[pl.BlockSpec(memory_space=pl.ANY)],
        out_specs=pl.BlockSpec(memory_space=pl.ANY),
        scratch_shapes=[
            pltpu.VMEM((owners, *own.shape), own.dtype),
            pltpu.SemaphoreType.DMA((2, size // 2)),
            pltpu.SemaphoreType.DMA((size, 2, size // 2)),
            pltpu.SemaphoreType.DMA((size * size,)),
            pltpu.SemaphoreType.DMA,
            pltpu.SemaphoreType.DMA,
            pltpu.SemaphoreType.DMA,
        ],
        compiler_params=GATHER_RING,
        name="gather_right",
    )(own)


def shards(
    homolog_stack_tensor,
    occupancy_indicator,
    chain_existence_flags,
    focus_normal_factor,
    focus_normal_addend,
    probe_index_weights,
    payload_valve_weights,
    logistic_valve_addend,
    focus_exit_weights,
    focus_exit_addend,
    product_mean_layer_stretch,
    product_mean_layer_shift,
    twin_map_matrix,
    twin_map_shift,
    couple_map_matrix,
    couple_map_shift,
):
    vertical_pieces = exchange_by_chip(
        homolog_stack_tensor, (("dap_0", "dap_1"), "dap_2"), (1, 0), 1, 0
    )
    seq_count, res_local, feature_width = vertical_pieces.shape
    position = lax.axis_index(DAP)
    present = occupancy_indicator * chain_existence_flags[:, None]
    live_own = lax.dynamic_slice_in_dim(present, position * res_local, res_local, 1)
    live_t = present.T.astype(BF16)
    own_t = live_own.T.astype(F32)
    live_l = jnp.repeat(live_own, OUTER_CHANNELS, axis=1)
    live_r = jnp.tile(own_t, (OUTER_CHANNELS, 1))
    row = lambda v: v[None, :]
    after, left, right = attend(
        jnp.transpose(vertical_pieces, (1, 0, 2)),
        own_t[:, None, :],
        row(focus_normal_factor),
        row(focus_normal_addend),
        probe_index_weights,
        payload_valve_weights,
        row(logistic_valve_addend),
        focus_exit_weights,
        row(focus_exit_addend),
        row(product_mean_layer_stretch),
        row(product_mean_layer_shift),
        jnp.tile(twin_map_matrix[:, :OUTER_CHANNELS], (1, res_local)),
        jnp.repeat(twin_map_matrix[:, OUTER_CHANNELS:].T, res_local, axis=0),
        row(jnp.tile(twin_map_shift[:OUTER_CHANNELS], res_local)),
        jnp.repeat(twin_map_shift[OUTER_CHANNELS:], res_local)[:, None],
        live_l.astype(F32),
        live_r,
    )
    right_all = gather_right(right, lax.axis_size("dap_0"))
    couple = jnp.transpose(
        couple_map_matrix.reshape(OUTER_CHANNELS, OUTER_CHANNELS, PAIR_DIM), (1, 0, 2)
    )
    pair_rows = pairs(
        right_all, left, live_t, live_l.astype(BF16), couple, row(couple_map_shift)
    )
    return (jnp.transpose(after, (1, 0, 2)), pair_rows)


def solution(mesh):
    split = Mesh(
        mesh.devices.reshape(mesh.shape["grp"], 8, 8, 2), ("grp", "dap_0", "dap_1", "dap_2")
    )
    return jax.shard_map(
        shards,
        mesh=split,
        in_specs=(
            P(GRP_DAP, None, None),
            P("grp", None),
            P("grp"),
            P(),
            P(),
            P(),
            P(),
            P(),
            P(),
            P(),
            P(),
            P(),
            P(),
            P(),
            P(),
            P(),
        ),
        out_specs=(P("grp", DAP, None), P(GRP_DAP, None, None)),
        check_vma=False,
    )
```

```python
import functools

import jax
import jax.numpy as jnp
from jax import lax
from jax.experimental import pallas as pl
from jax.experimental.pallas import tpu as pltpu
from jax.sharding import Mesh
from jax.sharding import PartitionSpec as P

HEAD_COUNT = 8
HEAD_CHANNELS = 32
OUTER_CHANNELS = 32
PAIR_DIM = 128
DAP = ("dap_0", "dap_1", "dap_2")
GRP_DAP = ("grp", "dap_0", "dap_1", "dap_2")
F32 = jnp.float32
BF16 = jnp.bfloat16
VMEM_LIMIT = 60 * 1024 * 1024


EPSILON = 1e-05
MASKED = -100000.0


def normalize(widened, gain, offset):
    centred = widened - jnp.mean(widened, axis=-1, keepdims=True)
    variance = jnp.mean(centred * centred, axis=-1, keepdims=True)
    return (centred * lax.rsqrt(variance + EPSILON) * gain + offset).astype(BF16)


def contract_lanes(a, b):
    return lax.dot_general(a, b, (((1,), (1,)), ((), ())), preferred_element_type=F32)


def one_hot(rows, columns, test):
    row = lax.broadcasted_iota(jnp.int32, (rows, columns), 0)
    column = lax.broadcasted_iota(jnp.int32, (rows, columns), 1)
    return jnp.where(test(row, column), 1.0, 0.0)


def attend_kernel(
    place_ref, x_ref, present_ref, chain_ref, gain_ref, offset_ref, qk_ref, vg_ref, gate_ref,
    exit_ref, exit_add_ref, gain2_ref, offset2_ref, twin_ref, shift_ref,
    after_ref, left_ref, right_ref, inverse_ref,
    xs, ys, keep, left_sum, right_sum,
):
    sites, seqs, width = xs.shape
    residues = present_ref.shape[1]
    pack = sites * OUTER_CHANNELS
    inner = HEAD_COUNT * HEAD_CHANNELS
    place = place_ref[0]
    core = lax.rem(place, 2)
    blocks = x_ref.shape[0] // (2 * sites * OUTER_CHANNELS)
    span = seqs // blocks

    pick = one_hot(
        sites * span, 2 * sites * span,
        lambda o, k: k == (o % span) * (2 * sites) + core * sites + o // span,
    ).astype(BF16)
    for b in range(blocks):
        rows = jnp.dot(
            pick, x_ref[2 * sites * span * b : 2 * sites * span * (b + 1), :],
            preferred_element_type=F32,
        ).astype(BF16)
        for r in range(sites):
            xs[r, span * b : span * (b + 1), :] = rows[span * r : span * (r + 1)]

    half = seqs // 2
    order = one_hot(
        seqs, seqs,
        lambda o, k: k == ((o % half) // 2) * 4 + (o // half) * 2 + o % 2,
    )
    order = (order * chain_ref[...].astype(F32)).astype(BF16)
    present = present_ref[...].astype(F32)
    live = jnp.dot(order, present.astype(BF16), preferred_element_type=F32).astype(BF16)
    select = one_hot(
        residues, pack, lambda j, c: j == place * sites + c // OUTER_CHANNELS
    ).astype(BF16)
    select_t = one_hot(
        pack, residues, lambda c, j: j == place * sites + c % sites
    ).astype(BF16)
    live_l = jnp.dot(live, select, preferred_element_type=F32)
    live_r = contract_lanes(select_t, live)
    keep[...] = live_r[:8]
    live_t = contract_lanes(present.T.astype(BF16), order).astype(BF16)
    counts = jnp.dot(live_t, live_l.astype(BF16), preferred_element_type=F32)
    inverse_ref[...] = 1.0 / jnp.maximum(counts, 1.0)

    head_of_lane = lax.broadcasted_iota(jnp.int32, (1, inner), 1) // HEAD_CHANNELS
    left_sum[...] = jnp.zeros_like(left_sum)
    right_sum[...] = jnp.zeros_like(right_sum)

    def one_site(r, carry):
        x = xs[r].astype(F32)
        normed = normalize(x, gain_ref[...], offset_ref[...])
        query_key = jnp.dot(normed, qk_ref[...], preferred_element_type=F32)
        value_gate = jnp.dot(normed, vg_ref[...], preferred_element_type=F32)
        query = (query_key[:, :inner] * HEAD_CHANNELS ** (-0.5)).astype(BF16)
        key = query_key[:, inner:].astype(BF16)
        value = value_gate[:, :inner].astype(BF16)
        gate = jax.nn.sigmoid(value_gate[:, inner:] + gate_ref[...])
        alive = keep[pl.ds(r, 1), :] > 0
        mixed = jnp.zeros((seqs, inner), F32)
        for h in range(HEAD_COUNT):
            own = head_of_lane == h
            query_h = query * own.astype(F32).astype(BF16)
            scores = jnp.where(alive, contract_lanes(query_h, key), MASKED)
            exponent = jnp.exp(scores - jnp.max(scores, axis=-1, keepdims=True))
            total = jnp.sum(exponent, axis=-1, keepdims=True)
            part = jnp.dot(exponent.astype(BF16), value, preferred_element_type=F32)
            mixed = jnp.where(own, part * (1.0 / total), mixed)
        gated = (mixed * gate).astype(BF16)
        update = jnp.dot(gated, exit_ref[...], preferred_element_type=F32) + exit_add_ref[...]
        after = (x + update).astype(BF16)
        ys[r] = after
        again = normalize(after.astype(F32), gain2_ref[...], offset2_ref[...])
        channels = 2 * OUTER_CHANNELS
        spread_l = one_hot(
            pack, channels,
            lambda o, c: (c == o % OUTER_CHANNELS) & (o // OUTER_CHANNELS == r),
        ).astype(BF16)
        spread_r = one_hot(
            pack, channels,
            lambda o, c: (c == OUTER_CHANNELS + o // sites) & (o % sites == r),
        ).astype(BF16)
        twin_l = jnp.dot(spread_l, twin_ref[...], preferred_element_type=F32).astype(BF16)
        twin_r = jnp.dot(spread_r, twin_ref[...], preferred_element_type=F32).astype(BF16)
        left_sum[...] += contract_lanes(again, twin_l)
        right_sum[...] += contract_lanes(twin_r, again)
        return carry

    lax.fori_loop(0, sites, one_site, 0)
    channels = 2 * OUTER_CHANNELS
    shift = shift_ref[...]
    across = one_hot(pack, channels, lambda o, c: c == OUTER_CHANNELS + o // sites)
    shift_r = jnp.sum(across * shift, axis=1, keepdims=True)
    column = jnp.sum(
        one_hot(channels, channels, lambda a, c: a == c) * shift, axis=1, keepdims=True
    )
    down = one_hot(channels, pack, lambda c, o: c == o % OUTER_CHANNELS)
    shift_l = jnp.sum(down * column, axis=0, keepdims=True)
    left_ref[...] = ((left_sum[...] + shift_l) * live_l).astype(BF16)
    right_ref[...] = ((right_sum[...] + shift_r) * live_r).astype(BF16)

    group = 2 * span
    place_back = one_hot(
        group * sites, group * sites,
        lambda o, k: k
        == (
            ((o % sites) * 2 + (o // (2 * sites)) % 2) * span
            + (o // (4 * sites)) * 2
            + (o // sites) % 2
        ),
    ).astype(BF16)
    for g in range(seqs // group):
        stack = jnp.concatenate(
            [
                ys[r, half * c + span * g : half * c + span * (g + 1), :]
                for r in range(sites)
                for c in range(2)
            ],
            axis=0,
        )
        rows = jnp.dot(place_back, stack, preferred_element_type=F32).astype(BF16)
        after_ref[group * g : group * (g + 1)] = rows.reshape(group, sites, width)


def attend(place, x, present, *rest):
    seqs, residues = present.shape
    width = x.shape[1]
    sites = x.shape[0] // (2 * seqs)
    pack = sites * OUTER_CHANNELS
    vmem = pl.BlockSpec(memory_space=pltpu.VMEM)
    return pl.pallas_call(
        attend_kernel,
        out_shape=(
            jax.ShapeDtypeStruct((seqs, sites, width), BF16),
            jax.ShapeDtypeStruct((seqs, pack), BF16),
            jax.ShapeDtypeStruct((pack, seqs), BF16),
            jax.ShapeDtypeStruct((residues, pack), F32),
        ),
        in_specs=[pl.BlockSpec(memory_space=pltpu.SMEM)] + [vmem] * (2 + len(rest)),
        out_specs=(vmem,) * 4,
        scratch_shapes=[
            pltpu.VMEM((sites, seqs, width), BF16),
            pltpu.VMEM((sites, seqs, width), BF16),
            pltpu.VMEM((8, seqs), F32),
            pltpu.VMEM((seqs, pack), F32),
            pltpu.VMEM((pack, seqs), F32),
        ],
        compiler_params=pltpu.CompilerParams(vmem_limit_bytes=VMEM_LIMIT),
        name="attend",
    )(place, x, present, *rest)


def pair_kernel(right_ref, left_ref, inverse_ref, couple_ref, shift_ref, out_ref, terms, blocks, wide):
    step = pl.program_id(0)
    owners, pack, seqs = right_ref.shape
    sites = out_ref.shape[0]
    chip_rows = 2 * sites
    halves = OUTER_CHANNELS // 2

    @pl.when(step == 0)
    def _():
        wide[...] = couple_ref[...].astype(F32)
        blocks[...] = jnp.zeros_like(blocks)
        for e in range(OUTER_CHANNELS):
            part = wide[pl.ds(e, OUTER_CHANNELS, stride=OUTER_CHANNELS), :].astype(BF16)
            for i in range(sites):
                row = e * pack + i * OUTER_CHANNELS
                blocks[row : row + OUTER_CHANNELS, i * PAIR_DIM : (i + 1) * PAIR_DIM] = part

    lower = lax.broadcasted_iota(jnp.int32, (1, chip_rows, 1), 1) < sites
    left = left_ref[...]

    def four(u, carry):
        quad = right_ref[pl.ds(4 * u, 4)].reshape(4 * pack, seqs)
        sums = jnp.dot(quad, left, preferred_element_type=F32)
        sums = sums.reshape(4, halves, chip_rows, pack)
        even, odd = [], []
        for t in range(2):
            a, b = sums[2 * t], sums[2 * t + 1]
            first = pl.multiple_of((step * owners + 4 * u + 2 * t) * sites, chip_rows)
            scale = inverse_ref[pl.ds(first, chip_rows), :][None]
            even.append(jnp.where(lower, a, pltpu.roll(b, sites, 1)) * scale)
            odd.append(jnp.where(lower, pltpu.roll(a, sites, 1), b) * scale)
        rows = pl.ds(pl.multiple_of((step * owners + 4 * u) * sites, 2 * chip_rows), 2 * chip_rows)
        even = jnp.concatenate(even, axis=1).astype(BF16)
        odd = jnp.concatenate(odd, axis=1).astype(BF16)
        for e in range(halves):
            terms[rows, 2 * e * pack : (2 * e + 1) * pack] = even[e]
            terms[rows, (2 * e + 1) * pack : (2 * e + 2) * pack] = odd[e]
        return carry

    lax.fori_loop(0, owners // 4, four, 0)

    @pl.when(step == pl.num_programs(0) - 1)
    def _():
        total = jnp.dot(terms[...], blocks[...], preferred_element_type=F32)
        for i in range(sites):
            part = total[:, i * PAIR_DIM : (i + 1) * PAIR_DIM] + shift_ref[...]
            out_ref[i] = part.astype(BF16)


def pairs(right_all, left, inverse, couple, shift):
    owners, pack, seqs = right_all.shape
    residues = inverse.shape[0]
    sites = pack // OUTER_CHANNELS
    steps = 4
    whole = lambda *shape: pl.BlockSpec(shape, lambda g: (0,) * len(shape))
    return pl.pallas_call(
        pair_kernel,
        grid=(steps,),
        in_specs=[
            pl.BlockSpec((owners // steps, pack, seqs), lambda g: (g, 0, 0)),
            whole(*left.shape),
            whole(*inverse.shape),
            whole(*couple.shape),
            whole(*shift.shape),
        ],
        out_specs=whole(sites, residues, PAIR_DIM),
        out_shape=jax.ShapeDtypeStruct((sites, residues, PAIR_DIM), BF16),
        scratch_shapes=[
            pltpu.VMEM((residues, OUTER_CHANNELS * pack), BF16),
            pltpu.VMEM((OUTER_CHANNELS * pack, sites * PAIR_DIM), BF16),
            pltpu.VMEM(couple.shape, F32),
        ],
        compiler_params=pltpu.CompilerParams(
            vmem_limit_bytes=VMEM_LIMIT, dimension_semantics=("arbitrary",)
        ),
        name="pairs",
    )(right_all, left, inverse, couple, shift)


def exchange_kernel(size, x_ref, out_ref, sent, got, swap_send, swap_got, own_sem):
    y, x, core = (lax.axis_index(a) for a in DAP)
    chips = size * size
    partner = {"dap_2": 1 - core}
    here = y * size + x
    far = size // 2
    steps = [(dy, dx) for dy in range(size) for dx in range(size) if dy or dx]
    away = lambda d: min(d, size - d)
    steps.sort(key=lambda d: -(away(d[0]) + away(d[1])))
    mesh = pl.DeviceIdType.MESH

    def chip(step):
        return lax.rem(y + step[0], size), lax.rem(x + step[1], size)

    own = pltpu.make_async_copy(x_ref.at[:, here], out_ref.at[core, here], own_sem)
    own.start()
    barrier = pltpu.get_barrier_semaphore()
    for step in steps:
        row, column = chip(step)
        pl.semaphore_signal(
            barrier, inc=1, device_id={"dap_0": row, "dap_1": column}, device_id_type=mesh
        )
    pl.semaphore_signal(barrier, inc=1, device_id=partner, device_id_type=mesh)
    pl.semaphore_wait(barrier, chips)
    for step in steps:
        row, column = chip(step)
        pltpu.make_async_remote_copy(
            src_ref=x_ref.at[:, row * size + column], dst_ref=out_ref.at[core, here],
            send_sem=sent, recv_sem=got, device_id={"dap_0": row, "dap_1": column},
            device_id_type=mesh,
        ).start()
    own.wait()
    others = out_ref.at[core, pl.ds(0, chips - 1)]
    pltpu.make_async_copy(others, others, got).wait()
    swap = pltpu.make_async_remote_copy(
        src_ref=out_ref.at[core], dst_ref=out_ref.at[core], send_sem=swap_send,
        recv_sem=swap_got, device_id=partner, device_id_type=mesh,
    )
    swap.start()
    pltpu.make_async_copy(others, others, sent).wait()
    swap.wait()


def exchange(x, size):
    seqs, residues, width = x.shape
    chips = size * size
    x = x.reshape(seqs, chips, residues // chips, width)
    out = pl.pallas_call(
        functools.partial(exchange_kernel, size),
        out_shape=jax.ShapeDtypeStruct((2, chips, seqs, residues // chips, width), x.dtype),
        in_specs=[pl.BlockSpec(memory_space=pl.ANY)],
        out_specs=pl.BlockSpec(memory_space=pl.ANY),
        scratch_shapes=[pltpu.SemaphoreType.DMA] * 5,
        compiler_params=pltpu.CompilerParams(
            vmem_limit_bytes=VMEM_LIMIT, collective_id=2, has_side_effects=True
        ),
        name="exchange",
    )(x)
    return out.reshape(2 * seqs * residues, width)


GATHER_RING = pltpu.CompilerParams(
    vmem_limit_bytes=VMEM_LIMIT, collective_id=1, has_side_effects=True
)


def ring_order(size):
    far = size // 2
    offsets = [0]
    for hop in range(1, far):
        offsets += [-hop, hop]
    offsets.append(far)
    events = []
    for offset in offsets:
        ready = 2.6 + 1.4 * abs(offset) if offset else 0.0
        if offset:
            events.append((ready, 0, 0, offset))
        for hop in range(1, far + 1):
            events.append((ready + 3.3 * hop + 0.01, 1, hop, offset))
    return sorted(events, key=lambda event: event[:2]), offsets


def gather_kernel(size, own_ref, all_ref, held, p_recv, s_recv, x_recv, send_sem, out_sem, in_sem):
    far = size // 2
    y, x, core = (lax.axis_index(a) for a in DAP)
    half = own_ref.shape[0] // 2

    def at(first, second):
        row = jnp.where(core == 0, second, first)
        column = jnp.where(core == 0, first, second)
        return lax.rem(row + size, size), lax.rem(column + size, size)

    main = jnp.where(core == 0, x, y)
    side = jnp.where(core == 0, y, x)

    def device(first, second):
        row, column = at(first, second)
        return {"dap_0": row, "dap_1": column}

    def slot(first, second, which):
        row, column = at(first, second)
        return (row * size + column) * 2 + which

    partner = {"dap_2": 1 - core}
    events, offsets = ring_order(size)
    neighbours = [device(main + offset, side) for offset in offsets if offset]
    neighbours += [device(main, side + 1), device(main, side - 1), partner]
    barrier = pltpu.get_barrier_semaphore()
    own_copy = pltpu.make_async_copy(own_ref, held.at[slot(main, side, core)], in_sem)
    own_copy.start()
    for neighbour in neighbours:
        pl.semaphore_signal(
            barrier, inc=1, device_id=neighbour, device_id_type=pl.DeviceIdType.MESH
        )
    pl.semaphore_wait(barrier, len(neighbours))
    own_copy.wait()

    def piece(first, second, which, hop, sign):
        ref = held.at[slot(first, second, which)]
        if hop < far:
            return ref
        return ref.at[pl.ds(0 if sign > 0 else half, half)]

    def remote(ref, recv, target):
        return pltpu.make_async_remote_copy(
            src_ref=ref, dst_ref=ref, send_sem=send_sem, recv_sem=recv,
            device_id=target, device_id_type=pl.DeviceIdType.MESH,
        )

    def along_main(offset):
        ref = held.at[slot(main, side, core)]
        remote(ref, p_recv.at[offsets.index(offset)], device(main - offset, side)).start()

    def along_side(offset, index, hop, sign):
        ref = piece(main + offset, side - sign * (hop - 1), core, hop, sign)
        remote(ref, s_recv.at[index, (sign + 1) // 2, hop - 1], device(main, side + sign)).start()

    def finished(first, second, order):
        ref = held.at[slot(first, second, core)]
        remote(ref, x_recv.at[order], partner).start()
        pltpu.make_async_copy(ref, all_ref.at[slot(first, second, core)], out_sem).start()
        done.append((first, second))

    def from_partner(order):
        first, second = done[order]
        ref = held.at[swapped_slot(first, second)]
        remote(ref, x_recv.at[order], partner).wait_recv()
        pltpu.make_async_copy(ref, all_ref.at[swapped_slot(first, second)], out_sem).start()

    def swapped_slot(first, second):
        d_first, d_second = first - main, second - side
        row = jnp.where(core == 0, main_row + d_first, main_row + d_second)
        column = jnp.where(core == 0, main_column + d_second, main_column + d_first)
        row, column = lax.rem(row + size, size), lax.rem(column + size, size)
        return (row * size + column) * 2 + (1 - core)

    main_row, main_column = y, x
    done = []
    for sign in (1, -1):
        along_side(0, 0, 1, sign)
    for offset in offsets:
        if offset:
            along_main(offset)
    finished(main, side, 0)
    lag, taken = 6, 0
    for _, kind, hop, offset in events:
        index = offsets.index(offset)
        if kind == 0:
            ref = held.at[slot(main + offset, side, core)]
            remote(ref, p_recv.at[index], partner).wait_recv()
            for way in (1, -1):
                along_side(offset, index, 1, way)
            finished(main + offset, side, len(done))
        else:
            for sign in (1, -1):
                ref = piece(main + offset, side - sign * hop, core, hop, sign)
                remote(ref, s_recv.at[index, (sign + 1) // 2, hop - 1], partner).wait_recv()
                if hop < far:
                    along_side(offset, index, hop + 1, sign)
                    finished(main + offset, side - sign * hop, len(done))
            if hop == far:
                finished(main + offset, side + far, len(done))
        while taken < len(done) - lag:
            from_partner(taken)
            taken += 1
    while taken < len(done):
        from_partner(taken)
        taken += 1
    sent = (size - 1) * (size + 1) + size * size
    drained = held.at[pl.ds(0, sent)]
    pltpu.make_async_copy(drained, drained, send_sem).wait()
    pltpu.make_async_copy(held, all_ref, out_sem).wait()


def gather_right(own, size):
    owners = 2 * size * size
    return pl.pallas_call(
        functools.partial(gather_kernel, size),
        out_shape=jax.ShapeDtypeStruct((owners, *own.shape), own.dtype),
        in_specs=[pl.BlockSpec(memory_space=pl.ANY)],
        out_specs=pl.BlockSpec(memory_space=pl.ANY),
        scratch_shapes=[
            pltpu.VMEM((owners, *own.shape), own.dtype),
            pltpu.SemaphoreType.DMA((size,)),
            pltpu.SemaphoreType.DMA((size, 2, size // 2)),
            pltpu.SemaphoreType.DMA((size * size,)),
            pltpu.SemaphoreType.DMA,
            pltpu.SemaphoreType.DMA,
            pltpu.SemaphoreType.DMA,
        ],
        compiler_params=GATHER_RING,
        name="gather_right",
    )(own)


def shards(
    homolog_stack_tensor,
    occupancy_indicator,
    chain_existence_flags,
    focus_normal_factor,
    focus_normal_addend,
    probe_index_weights,
    payload_valve_weights,
    logistic_valve_addend,
    focus_exit_weights,
    focus_exit_addend,
    product_mean_layer_stretch,
    product_mean_layer_shift,
    twin_map_matrix,
    twin_map_shift,
    couple_map_matrix,
    couple_map_shift,
):
    seqs, residues = occupancy_indicator.shape
    width = homolog_stack_tensor.shape[-1]
    size = lax.axis_size("dap_0")
    row = lambda v: v[None, :]
    after, left, right, inverse = attend(
        lax.axis_index(DAP)[None],
        exchange(homolog_stack_tensor, size),
        occupancy_indicator,
        row(chain_existence_flags),
        row(focus_normal_factor),
        row(focus_normal_addend),
        probe_index_weights,
        payload_valve_weights,
        row(logistic_valve_addend),
        focus_exit_weights,
        row(focus_exit_addend),
        row(product_mean_layer_stretch),
        row(product_mean_layer_shift),
        twin_map_matrix.T,
        row(twin_map_shift),
    )
    right_all = gather_right(right, size)
    pair_rows = pairs(right_all, left, inverse, couple_map_matrix, row(couple_map_shift))
    return (after, pair_rows)


def solution(mesh):
    split = Mesh(
        mesh.devices.reshape(mesh.shape["grp"], 8, 8, 2), ("grp", "dap_0", "dap_1", "dap_2")
    )
    return jax.shard_map(
        shards,
        mesh=split,
        in_specs=(
            P(GRP_DAP, None, None),
            P("grp", None),
            P("grp"),
            P(),
            P(),
            P(),
            P(),
            P(),
            P(),
            P(),
            P(),
            P(),
            P(),
            P(),
            P(),
            P(),
        ),
        out_specs=(P("grp", DAP, None), P(GRP_DAP, None, None)),
        check_vma=False,
    )
```

```python
import functools

import jax
import jax.numpy as jnp
from jax import lax
from jax.experimental import pallas as pl
from jax.experimental.pallas import tpu as pltpu
from jax.sharding import Mesh
from jax.sharding import PartitionSpec as P

HEAD_COUNT = 8
HEAD_CHANNELS = 32
OUTER_CHANNELS = 32
PAIR_DIM = 128
DAP = ("dap_0", "dap_1", "dap_2")
GRP_DAP = ("grp", "dap_0", "dap_1", "dap_2")
F32 = jnp.float32
BF16 = jnp.bfloat16
VMEM_LIMIT = 60 * 1024 * 1024


EPSILON = 1e-05
MASKED = -100000.0


def normalize(widened, gain, offset):
    centred = widened - jnp.mean(widened, axis=-1, keepdims=True)
    variance = jnp.mean(centred * centred, axis=-1, keepdims=True)
    return (centred * lax.rsqrt(variance + EPSILON) * gain + offset).astype(BF16)


def contract_lanes(a, b):
    return lax.dot_general(a, b, (((1,), (1,)), ((), ())), preferred_element_type=F32)


def one_hot(rows, columns, test):
    row = lax.broadcasted_iota(jnp.int32, (rows, columns), 0)
    column = lax.broadcasted_iota(jnp.int32, (rows, columns), 1)
    return jnp.where(test(row, column), 1.0, 0.0)


def attend_kernel(
    place_ref, x_ref, present_ref, chain_ref, gain_ref, offset_ref, qk_ref, vg_ref, gate_ref,
    exit_ref, exit_add_ref, gain2_ref, offset2_ref, twin_ref, shift_ref,
    after_ref, left_ref, right_ref, inverse_ref,
    xs, ys, keep, left_sum, right_sum,
):
    sites, seqs, width = xs.shape
    residues = present_ref.shape[1]
    pack = sites * OUTER_CHANNELS
    inner = HEAD_COUNT * HEAD_CHANNELS
    place = place_ref[0]
    core = lax.rem(place, 2)
    blocks = x_ref.shape[0] // (2 * sites * OUTER_CHANNELS)
    span = seqs // blocks

    pick = one_hot(
        sites * span, 2 * sites * span,
        lambda o, k: k == (o % span) * (2 * sites) + core * sites + o // span,
    ).astype(BF16)
    for b in range(blocks):
        rows = jnp.dot(
            pick, x_ref[2 * sites * span * b : 2 * sites * span * (b + 1), :],
            preferred_element_type=F32,
        ).astype(BF16)
        for r in range(sites):
            xs[r, span * b : span * (b + 1), :] = rows[span * r : span * (r + 1)]

    half = seqs // 2
    order = one_hot(
        seqs, seqs,
        lambda o, k: k == ((o % half) // 2) * 4 + (o // half) * 2 + o % 2,
    )
    order = (order * chain_ref[...].astype(F32)).astype(BF16)
    present = present_ref[...].astype(F32)
    live = jnp.dot(order, present.astype(BF16), preferred_element_type=F32).astype(BF16)
    select = one_hot(
        residues, pack, lambda j, c: j == place * sites + c // OUTER_CHANNELS
    ).astype(BF16)
    select_t = one_hot(
        pack, residues, lambda c, j: j == place * sites + c % sites
    ).astype(BF16)
    live_l = jnp.dot(live, select, preferred_element_type=F32)
    live_r = contract_lanes(select_t, live)
    keep[...] = live_r[:8]
    live_t = contract_lanes(present.T.astype(BF16), order).astype(BF16)
    counts = jnp.dot(live_t, live_l.astype(BF16), preferred_element_type=F32)
    inverse_ref[...] = 1.0 / jnp.maximum(counts, 1.0)

    head_of_lane = lax.broadcasted_iota(jnp.int32, (1, inner), 1) // HEAD_CHANNELS
    left_sum[...] = jnp.zeros_like(left_sum)
    right_sum[...] = jnp.zeros_like(right_sum)

    def one_site(r, carry):
        x = xs[r].astype(F32)
        normed = normalize(x, gain_ref[...], offset_ref[...])
        query_key = jnp.dot(normed, qk_ref[...], preferred_element_type=F32)
        value_gate = jnp.dot(normed, vg_ref[...], preferred_element_type=F32)
        query = (query_key[:, :inner] * HEAD_CHANNELS ** (-0.5)).astype(BF16)
        key = query_key[:, inner:].astype(BF16)
        value = value_gate[:, :inner].astype(BF16)
        gate = jax.nn.sigmoid(value_gate[:, inner:] + gate_ref[...])
        alive = keep[pl.ds(r, 1), :] > 0
        mixed = jnp.zeros((seqs, inner), F32)
        for h in range(HEAD_COUNT):
            own = head_of_lane == h
            query_h = query * own.astype(F32).astype(BF16)
            scores = jnp.where(alive, contract_lanes(query_h, key), MASKED)
            exponent = jnp.exp(scores - jnp.max(scores, axis=-1, keepdims=True))
            total = jnp.sum(exponent, axis=-1, keepdims=True)
            part = jnp.dot(exponent.astype(BF16), value, preferred_element_type=F32)
            mixed = jnp.where(own, part * (1.0 / total), mixed)
        gated = (mixed * gate).astype(BF16)
        update = jnp.dot(gated, exit_ref[...], preferred_element_type=F32) + exit_add_ref[...]
        after = (x + update).astype(BF16)
        ys[r] = after
        again = normalize(after.astype(F32), gain2_ref[...], offset2_ref[...])
        channels = 2 * OUTER_CHANNELS
        spread_l = one_hot(
            pack, channels,
            lambda o, c: (c == o % OUTER_CHANNELS) & (o // OUTER_CHANNELS == r),
        ).astype(BF16)
        spread_r = one_hot(
            pack, channels,
            lambda o, c: (c == OUTER_CHANNELS + o // sites) & (o % sites == r),
        ).astype(BF16)
        twin_l = jnp.dot(spread_l, twin_ref[...], preferred_element_type=F32).astype(BF16)
        twin_r = jnp.dot(spread_r, twin_ref[...], preferred_element_type=F32).astype(BF16)
        left_sum[...] += contract_lanes(again, twin_l)
        right_sum[...] += contract_lanes(twin_r, again)
        return carry

    lax.fori_loop(0, sites, one_site, 0)
    channels = 2 * OUTER_CHANNELS
    shift = shift_ref[...]
    across = one_hot(pack, channels, lambda o, c: c == OUTER_CHANNELS + o // sites)
    shift_r = jnp.sum(across * shift, axis=1, keepdims=True)
    column = jnp.sum(
        one_hot(channels, channels, lambda a, c: a == c) * shift, axis=1, keepdims=True
    )
    down = one_hot(channels, pack, lambda c, o: c == o % OUTER_CHANNELS)
    shift_l = jnp.sum(down * column, axis=0, keepdims=True)
    left_ref[...] = ((left_sum[...] + shift_l) * live_l).astype(BF16)
    right_ref[...] = ((right_sum[...] + shift_r) * live_r).astype(BF16)

    group = 2 * span
    place_back = one_hot(
        group * sites, group * sites,
        lambda o, k: k
        == (
            ((o % sites) * 2 + (o // (2 * sites)) % 2) * span
            + (o // (4 * sites)) * 2
            + (o // sites) % 2
        ),
    ).astype(BF16)
    for g in range(seqs // group):
        stack = jnp.concatenate(
            [
                ys[r, half * c + span * g : half * c + span * (g + 1), :]
                for r in range(sites)
                for c in range(2)
            ],
            axis=0,
        )
        rows = jnp.dot(place_back, stack, preferred_element_type=F32).astype(BF16)
        after_ref[group * g : group * (g + 1)] = rows.reshape(group, sites, width)


def attend(place, x, present, *rest):
    seqs, residues = present.shape
    width = x.shape[1]
    sites = x.shape[0] // (2 * seqs)
    pack = sites * OUTER_CHANNELS
    vmem = pl.BlockSpec(memory_space=pltpu.VMEM)
    return pl.pallas_call(
        attend_kernel,
        out_shape=(
            jax.ShapeDtypeStruct((seqs, sites, width), BF16),
            jax.ShapeDtypeStruct((seqs, pack), BF16),
            jax.ShapeDtypeStruct((pack, seqs), BF16),
            jax.ShapeDtypeStruct((residues, pack), F32),
        ),
        in_specs=[pl.BlockSpec(memory_space=pltpu.SMEM)] + [vmem] * (2 + len(rest)),
        out_specs=(vmem,) * 4,
        scratch_shapes=[
            pltpu.VMEM((sites, seqs, width), BF16),
            pltpu.VMEM((sites, seqs, width), BF16),
            pltpu.VMEM((8, seqs), F32),
            pltpu.VMEM((seqs, pack), F32),
            pltpu.VMEM((pack, seqs), F32),
        ],
        compiler_params=pltpu.CompilerParams(vmem_limit_bytes=VMEM_LIMIT),
        name="attend",
    )(place, x, present, *rest)


def ring_order(size):
    far = size // 2
    offsets = [0]
    for hop in range(1, far):
        offsets += [-hop, hop]
    offsets.append(far)
    first = {0: 0.0, 1: 4.0, 2: 5.4}
    events = []
    for offset in offsets:
        hop = abs(offset)
        ready = first.get(hop, 5.4 + 3.3 * (hop - 2) - 2.6 * (hop - 3))
        if offset:
            events.append((ready, 0, 0, offset))
        for hop in range(1, far + 1):
            events.append((ready + 3.3 * hop + 0.01, 1, hop, offset))
    return sorted(events, key=lambda event: event[:2]), offsets


def pair_kernel(
    size, own_ref, left_ref, inverse_ref, couple_ref, shift_ref, out_ref,
    held, terms, blocks, wide, total, couple, left, inverse,
    p_recv, s_recv, x_recv, send_sem, in_sem,
):
    far = size // 2
    chips = size * size
    y, x, core = (lax.axis_index(a) for a in DAP)
    pack = own_ref.shape[0]
    half = pack // 2
    sites = out_ref.shape[0]
    chip_rows = 2 * sites
    halves = OUTER_CHANNELS // 2
    mesh = pl.DeviceIdType.MESH

    def at(first, second):
        row = jnp.where(core == 0, second, first)
        column = jnp.where(core == 0, first, second)
        return lax.rem(row + size, size), lax.rem(column + size, size)

    main = jnp.where(core == 0, x, y)
    side = jnp.where(core == 0, y, x)

    def device(first, second):
        row, column = at(first, second)
        return {"dap_0": row, "dap_1": column}

    def chip(first, second):
        row, column = at(main + first, side + second)
        return row * size + column

    def slot(first, second):
        return chip(first, second) * 2 + core

    events, offsets = ring_order(size)
    partner = {"dap_2": 1 - core}
    neighbours = [device(main + step, side) for step in (1, -1, 2, -2)]
    neighbours += [device(main, side + 1), device(main, side - 1), partner]
    own_copy = pltpu.make_async_copy(own_ref, held.at[slot(0, 0)], in_sem.at[0])
    own_copy.start()
    loads = [
        pltpu.make_async_copy(a, b, in_sem.at[1 + i])
        for i, (a, b) in enumerate(
            ((couple_ref, couple), (left_ref, left), (inverse_ref, inverse))
        )
    ]
    for load in loads:
        load.start()
    barrier = pltpu.get_barrier_semaphore()
    for neighbour in neighbours:
        pl.semaphore_signal(barrier, inc=1, device_id=neighbour, device_id_type=mesh)
    pl.semaphore_wait(barrier, len(neighbours))
    own_copy.wait()

    def part(ref, sign):
        return ref.at[pl.ds(0 if sign > 0 else half, half)]

    def remote(ref, recv, target):
        return pltpu.make_async_remote_copy(
            src_ref=ref, dst_ref=ref, send_sem=send_sem, recv_sem=recv,
            device_id=target, device_id_type=mesh,
        )

    def main_sem(offset, sign):
        return p_recv.at[offsets.index(offset) + (1 if offset == far and sign < 0 else 0)]

    def along_main(origin, sign, step):
        reach = origin - sign * step
        ref = held.at[slot(origin, 0)]
        if abs(reach) == far:
            reach, ref = far, part(ref, sign)
        remote(ref, main_sem(reach, sign), device(main + sign * step, side)).start()

    def along_side(offset, hop, sign):
        ref = held.at[slot(offset, -sign * (hop - 1))]
        if hop == far:
            ref = part(ref, sign)
        recv = s_recv.at[offsets.index(offset), (sign + 1) // 2, hop - 1]
        remote(ref, recv, device(main, side + sign)).start()

    def reduced(second):
        return second if second > -far else far

    done = []

    def finished(first, second):
        remote(held.at[slot(first, second)], x_recv.at[len(done)], partner).start()
        done.append((first, reduced(second)))

    for sign in (1, -1):
        along_side(0, 1, sign)
    for step in (2, 1):
        for sign in (1, -1):
            along_main(0, sign, step)
    finished(0, 0)

    for load in loads:
        load.wait()
    wide[...] = couple[...].astype(F32)
    blocks[...] = jnp.zeros_like(blocks)
    for e in range(OUTER_CHANNELS):
        rows = wide[pl.ds(e, OUTER_CHANNELS, stride=OUTER_CHANNELS), :].astype(BF16)
        for i in range(sites):
            row = e * pack + i * OUTER_CHANNELS
            blocks[row : row + OUTER_CHANNELS, i * PAIR_DIM : (i + 1) * PAIR_DIM] = rows

    lower = lax.broadcasted_iota(jnp.int32, (1, chip_rows, 1), 1) < sites

    def from_partner(first, second):
        ref = held.at[chip(first, second) * 2 + (1 - core)]
        remote(ref, x_recv.at[done.index((second, first))], partner).wait_recv()

    def multiply(unit, members):
        quad = []
        for member in members:
            from_partner(*member)
            first = chip(*member) * 2
            quad += [held[first], held[first + 1]]
        sums = jnp.dot(jnp.concatenate(quad, axis=0), left[...], preferred_element_type=F32)
        sums = sums.reshape(4, halves, chip_rows, pack)
        even, odd = [], []
        for t, member in enumerate(members):
            a, b = sums[2 * t], sums[2 * t + 1]
            first = pl.multiple_of(chip(*member) * chip_rows, chip_rows)
            scale = inverse[pl.ds(first, chip_rows), :][None]
            even.append(jnp.where(lower, a, pltpu.roll(b, sites, 1)) * scale)
            odd.append(jnp.where(lower, pltpu.roll(a, sites, 1), b) * scale)
        rows = slice(2 * chip_rows * unit, 2 * chip_rows * (unit + 1))
        even = jnp.concatenate(even, axis=1).astype(BF16)
        odd = jnp.concatenate(odd, axis=1).astype(BF16)
        for e in range(halves):
            terms[rows, 2 * e * pack : (2 * e + 1) * pack] = even[e]
            terms[rows, (2 * e + 1) * pack : (2 * e + 2) * pack] = odd[e]

    placed = []

    def project(first, count):
        rows = slice(chip_rows * first, chip_rows * (first + count))
        result = jnp.dot(terms[rows, :], blocks[...], preferred_element_type=F32)
        for k in range(count):
            row = pl.multiple_of(chip(*placed[first + k]) * chip_rows, chip_rows)
            total[pl.ds(row, chip_rows), :] = result[chip_rows * k : chip_rows * (k + 1)]

    def advance(lag):
        while True:
            ready = [
                (max(done.index(m), done.index(m[::-1])), m)
                for m in done
                if m not in placed and m[::-1] in done
            ]
            ready = [m for at, m in sorted(ready) if at < len(done) - lag]
            if len(ready) < 2:
                return
            multiply(len(placed) // 2, ready[:2])
            placed.extend(ready[:2])
            if len(placed) == chips // 2:
                project(0, chips // 2)

    for _, kind, hop, offset in events:
        if kind == 0:
            ref = held.at[slot(offset, 0)]
            if offset == far:
                for sign in (1, -1):
                    remote(part(ref, sign), main_sem(far, sign), partner).wait_recv()
            else:
                remote(ref, main_sem(offset, 1), partner).wait_recv()
            if abs(offset) == 2:
                sign = -offset // 2
                along_main(offset, sign, 2)
                along_main(offset, sign, 1)
            for way in (1, -1):
                along_side(offset, 1, way)
            finished(offset, 0)
        else:
            for sign in (1, -1):
                ref = held.at[slot(offset, -sign * hop)]
                if hop == far:
                    ref = part(ref, sign)
                recv = s_recv.at[offsets.index(offset), (sign + 1) // 2, hop - 1]
                remote(ref, recv, partner).wait_recv()
                if hop < far:
                    along_side(offset, hop + 1, sign)
                    finished(offset, -sign * hop)
            if hop == far:
                finished(offset, far)
        advance(5)
    advance(0)
    project(chips // 2, chips // 2)
    for i in range(sites):
        rows = total[:, i * PAIR_DIM : (i + 1) * PAIR_DIM] + shift_ref[...]
        out_ref[i] = rows.astype(BF16)
    sent = (size - 1) * (size + 1) + size * size
    drained = held.at[pl.ds(0, sent)]
    pltpu.make_async_copy(drained, drained, send_sem).wait()


def pairs(right, left, inverse, couple, shift, size):
    pack, seqs = right.shape
    residues = inverse.shape[0]
    owners = 2 * size * size
    sites = pack // OUTER_CHANNELS
    hbm = pl.BlockSpec(memory_space=pl.ANY)
    vmem = pl.BlockSpec(memory_space=pltpu.VMEM)
    return pl.pallas_call(
        functools.partial(pair_kernel, size),
        in_specs=[hbm, hbm, hbm, hbm, vmem],
        out_specs=vmem,
        out_shape=jax.ShapeDtypeStruct((sites, residues, PAIR_DIM), BF16),
        scratch_shapes=[
            pltpu.VMEM((owners, pack, seqs), BF16),
            pltpu.VMEM((residues, OUTER_CHANNELS * pack), BF16),
            pltpu.VMEM((OUTER_CHANNELS * pack, sites * PAIR_DIM), BF16),
            pltpu.VMEM(couple.shape, F32),
            pltpu.VMEM((residues, sites * PAIR_DIM), F32),
            pltpu.VMEM(couple.shape, BF16),
            pltpu.VMEM(left.shape, BF16),
            pltpu.VMEM(inverse.shape, F32),
            pltpu.SemaphoreType.DMA((size + 1,)),
            pltpu.SemaphoreType.DMA((size, 2, size // 2)),
            pltpu.SemaphoreType.DMA((size * size,)),
            pltpu.SemaphoreType.DMA,
            pltpu.SemaphoreType.DMA((4,)),
        ],
        compiler_params=pltpu.CompilerParams(
            vmem_limit_bytes=VMEM_LIMIT, collective_id=1, has_side_effects=True
        ),
        name="pairs",
    )(right, left, inverse, couple, shift)


def exchange_kernel(size, x_ref, out_ref, sent, got, swap_send, swap_got, own_sem):
    y, x, core = (lax.axis_index(a) for a in DAP)
    chips = size * size
    partner = {"dap_2": 1 - core}
    here = y * size + x
    far = size // 2
    steps = [(dy, dx) for dy in range(size) for dx in range(size) if dy or dx]
    away = lambda d: min(d, size - d)
    steps.sort(key=lambda d: -(away(d[0]) + away(d[1])))
    mesh = pl.DeviceIdType.MESH

    def chip(step):
        return lax.rem(y + step[0], size), lax.rem(x + step[1], size)

    own = pltpu.make_async_copy(x_ref.at[:, here], out_ref.at[core, here], own_sem)
    own.start()
    barrier = pltpu.get_barrier_semaphore()
    for step in steps:
        row, column = chip(step)
        pl.semaphore_signal(
            barrier, inc=1, device_id={"dap_0": row, "dap_1": column}, device_id_type=mesh
        )
    pl.semaphore_signal(barrier, inc=1, device_id=partner, device_id_type=mesh)
    pl.semaphore_wait(barrier, chips)
    for step in steps:
        row, column = chip(step)
        pltpu.make_async_remote_copy(
            src_ref=x_ref.at[:, row * size + column], dst_ref=out_ref.at[core, here],
            send_sem=sent, recv_sem=got, device_id={"dap_0": row, "dap_1": column},
            device_id_type=mesh,
        ).start()
    own.wait()
    others = out_ref.at[core, pl.ds(0, chips - 1)]
    pltpu.make_async_copy(others, others, got).wait()
    swap = pltpu.make_async_remote_copy(
        src_ref=out_ref.at[core], dst_ref=out_ref.at[core], send_sem=swap_send,
        recv_sem=swap_got, device_id=partner, device_id_type=mesh,
    )
    swap.start()
    pltpu.make_async_copy(others, others, sent).wait()
    swap.wait()


def exchange(x, size):
    seqs, residues, width = x.shape
    chips = size * size
    x = x.reshape(seqs, chips, residues // chips, width)
    out = pl.pallas_call(
        functools.partial(exchange_kernel, size),
        out_shape=jax.ShapeDtypeStruct((2, chips, seqs, residues // chips, width), x.dtype),
        in_specs=[pl.BlockSpec(memory_space=pl.ANY)],
        out_specs=pl.BlockSpec(memory_space=pl.ANY),
        scratch_shapes=[pltpu.SemaphoreType.DMA] * 5,
        compiler_params=pltpu.CompilerParams(
            vmem_limit_bytes=VMEM_LIMIT, collective_id=2, has_side_effects=True
        ),
        name="exchange",
    )(x)
    return out.reshape(2 * seqs * residues, width)


GATHER_RING = pltpu.CompilerParams(
    vmem_limit_bytes=VMEM_LIMIT, collective_id=1, has_side_effects=True
)


def ring_order(size):
    far = size // 2
    offsets = [0]
    for hop in range(1, far):
        offsets += [-hop, hop]
    offsets.append(far)
    events = []
    for offset in offsets:
        ready = 2.6 + 1.4 * abs(offset) if offset else 0.0
        if offset:
            events.append((ready, 0, 0, offset))
        for hop in range(1, far + 1):
            events.append((ready + 3.3 * hop + 0.01, 1, hop, offset))
    return sorted(events, key=lambda event: event[:2]), offsets


def gather_kernel(size, own_ref, all_ref, held, p_recv, s_recv, x_recv, send_sem, out_sem, in_sem):
    far = size // 2
    y, x, core = (lax.axis_index(a) for a in DAP)
    half = own_ref.shape[0] // 2

    def at(first, second):
        row = jnp.where(core == 0, second, first)
        column = jnp.where(core == 0, first, second)
        return lax.rem(row + size, size), lax.rem(column + size, size)

    main = jnp.where(core == 0, x, y)
    side = jnp.where(core == 0, y, x)

    def device(first, second):
        row, column = at(first, second)
        return {"dap_0": row, "dap_1": column}

    def slot(first, second, which):
        row, column = at(first, second)
        return (row * size + column) * 2 + which

    partner = {"dap_2": 1 - core}
    events, offsets = ring_order(size)
    neighbours = [device(main + offset, side) for offset in offsets if offset]
    neighbours += [device(main, side + 1), device(main, side - 1), partner]
    barrier = pltpu.get_barrier_semaphore()
    own_copy = pltpu.make_async_copy(own_ref, held.at[slot(main, side, core)], in_sem)
    own_copy.start()
    for neighbour in neighbours:
        pl.semaphore_signal(
            barrier, inc=1, device_id=neighbour, device_id_type=pl.DeviceIdType.MESH
        )
    pl.semaphore_wait(barrier, len(neighbours))
    own_copy.wait()

    def piece(first, second, which, hop, sign):
        ref = held.at[slot(first, second, which)]
        if hop < far:
            return ref
        return ref.at[pl.ds(0 if sign > 0 else half, half)]

    def remote(ref, recv, target):
        return pltpu.make_async_remote_copy(
            src_ref=ref, dst_ref=ref, send_sem=send_sem, recv_sem=recv,
            device_id=target, device_id_type=pl.DeviceIdType.MESH,
        )

    def along_main(offset):
        ref = held.at[slot(main, side, core)]
        remote(ref, p_recv.at[offsets.index(offset)], device(main - offset, side)).start()

    def along_side(offset, index, hop, sign):
        ref = piece(main + offset, side - sign * (hop - 1), core, hop, sign)
        remote(ref, s_recv.at[index, (sign + 1) // 2, hop - 1], device(main, side + sign)).start()

    def finished(first, second, order):
        ref = held.at[slot(first, second, core)]
        remote(ref, x_recv.at[order], partner).start()
        pltpu.make_async_copy(ref, all_ref.at[slot(first, second, core)], out_sem).start()
        done.append((first, second))

    def from_partner(order):
        first, second = done[order]
        ref = held.at[swapped_slot(first, second)]
        remote(ref, x_recv.at[order], partner).wait_recv()
        pltpu.make_async_copy(ref, all_ref.at[swapped_slot(first, second)], out_sem).start()

    def swapped_slot(first, second):
        d_first, d_second = first - main, second - side
        row = jnp.where(core == 0, main_row + d_first, main_row + d_second)
        column = jnp.where(core == 0, main_column + d_second, main_column + d_first)
        row, column = lax.rem(row + size, size), lax.rem(column + size, size)
        return (row * size + column) * 2 + (1 - core)

    main_row, main_column = y, x
    done = []
    for sign in (1, -1):
        along_side(0, 0, 1, sign)
    for offset in offsets:
        if offset:
            along_main(offset)
    finished(main, side, 0)
    lag, taken = 6, 0
    for _, kind, hop, offset in events:
        index = offsets.index(offset)
        if kind == 0:
            ref = held.at[slot(main + offset, side, core)]
            remote(ref, p_recv.at[index], partner).wait_recv()
            for way in (1, -1):
                along_side(offset, index, 1, way)
            finished(main + offset, side, len(done))
        else:
            for sign in (1, -1):
                ref = piece(main + offset, side - sign * hop, core, hop, sign)
                remote(ref, s_recv.at[index, (sign + 1) // 2, hop - 1], partner).wait_recv()
                if hop < far:
                    along_side(offset, index, hop + 1, sign)
                    finished(main + offset, side - sign * hop, len(done))
            if hop == far:
                finished(main + offset, side + far, len(done))
        while taken < len(done) - lag:
            from_partner(taken)
            taken += 1
    while taken < len(done):
        from_partner(taken)
        taken += 1
    sent = (size - 1) * (size + 1) + size * size
    drained = held.at[pl.ds(0, sent)]
    pltpu.make_async_copy(drained, drained, send_sem).wait()
    pltpu.make_async_copy(held, all_ref, out_sem).wait()


def gather_right(own, size):
    owners = 2 * size * size
    return pl.pallas_call(
        functools.partial(gather_kernel, size),
        out_shape=jax.ShapeDtypeStruct((owners, *own.shape), own.dtype),
        in_specs=[pl.BlockSpec(memory_space=pl.ANY)],
        out_specs=pl.BlockSpec(memory_space=pl.ANY),
        scratch_shapes=[
            pltpu.VMEM((owners, *own.shape), own.dtype),
            pltpu.SemaphoreType.DMA((size,)),
            pltpu.SemaphoreType.DMA((size, 2, size // 2)),
            pltpu.SemaphoreType.DMA((size * size,)),
            pltpu.SemaphoreType.DMA,
            pltpu.SemaphoreType.DMA,
            pltpu.SemaphoreType.DMA,
        ],
        compiler_params=GATHER_RING,
        name="gather_right",
    )(own)


def shards(
    homolog_stack_tensor,
    occupancy_indicator,
    chain_existence_flags,
    focus_normal_factor,
    focus_normal_addend,
    probe_index_weights,
    payload_valve_weights,
    logistic_valve_addend,
    focus_exit_weights,
    focus_exit_addend,
    product_mean_layer_stretch,
    product_mean_layer_shift,
    twin_map_matrix,
    twin_map_shift,
    couple_map_matrix,
    couple_map_shift,
):
    seqs, residues = occupancy_indicator.shape
    width = homolog_stack_tensor.shape[-1]
    size = lax.axis_size("dap_0")
    row = lambda v: v[None, :]
    after, left, right, inverse = attend(
        lax.axis_index(DAP)[None],
        exchange(homolog_stack_tensor, size),
        occupancy_indicator,
        row(chain_existence_flags),
        row(focus_normal_factor),
        row(focus_normal_addend),
        probe_index_weights,
        payload_valve_weights,
        row(logistic_valve_addend),
        focus_exit_weights,
        row(focus_exit_addend),
        row(product_mean_layer_stretch),
        row(product_mean_layer_shift),
        twin_map_matrix.T,
        row(twin_map_shift),
    )
    pair_rows = pairs(right, left, inverse, couple_map_matrix, row(couple_map_shift), size)
    return (after, pair_rows)


def solution(mesh):
    split = Mesh(
        mesh.devices.reshape(mesh.shape["grp"], 8, 8, 2), ("grp", "dap_0", "dap_1", "dap_2")
    )
    return jax.shard_map(
        shards,
        mesh=split,
        in_specs=(
            P(GRP_DAP, None, None),
            P("grp", None),
            P("grp"),
            P(),
            P(),
            P(),
            P(),
            P(),
            P(),
            P(),
            P(),
            P(),
            P(),
            P(),
            P(),
            P(),
        ),
        out_specs=(P("grp", DAP, None), P(GRP_DAP, None, None)),
        check_vma=False,
    )
```

```python
import functools

import jax
import jax.numpy as jnp
from jax import lax
from jax.experimental import pallas as pl
from jax.experimental.pallas import tpu as pltpu
from jax.sharding import Mesh
from jax.sharding import PartitionSpec as P

HEAD_COUNT = 8
HEAD_CHANNELS = 32
OUTER_CHANNELS = 32
PAIR_DIM = 128
DAP = ("dap_0", "dap_1", "dap_2")
GRP_DAP = ("grp", "dap_0", "dap_1", "dap_2")
F32 = jnp.float32
BF16 = jnp.bfloat16
VMEM_LIMIT = 60 * 1024 * 1024


EPSILON = 1e-05
MASKED = -100000.0


def normalize(widened, gain, offset):
    centred = widened - jnp.mean(widened, axis=-1, keepdims=True)
    variance = jnp.mean(centred * centred, axis=-1, keepdims=True)
    return (centred * lax.rsqrt(variance + EPSILON) * gain + offset).astype(BF16)


def contract_lanes(a, b):
    return lax.dot_general(a, b, (((1,), (1,)), ((), ())), preferred_element_type=F32)


def one_hot(rows, columns, test):
    row = lax.broadcasted_iota(jnp.int32, (rows, columns), 0)
    column = lax.broadcasted_iota(jnp.int32, (rows, columns), 1)
    return jnp.where(test(row, column), 1.0, 0.0)


def core_kernel(
    size, x_ref, present_ref, chain_ref, gain_ref, offset_ref, qk_ref, vg_ref, gate_ref,
    exit_ref, exit_add_ref, gain2_ref, offset2_ref, twin_ref, shift_ref, couple_ref,
    pair_shift_ref,
    after_ref, out_ref,
    xs, ys, keep, inverse, chunks, columns, blocks, wide, sums, terms, total, stage, placed,
    main_recv, side_recv, swap_recv, out_recv, sends, local_sem,
):
    sites, seqs, width = xs.shape
    residues = present_ref.shape[1]
    pack = sites * OUTER_CHANNELS
    inner = HEAD_COUNT * HEAD_CHANNELS
    channels = 2 * OUTER_CHANNELS
    chip_rows = 2 * sites
    far = size // 2
    mesh = pl.DeviceIdType.MESH
    y, x, core = (lax.axis_index(a) for a in DAP)
    main = jnp.where(core == 0, x, y)
    side = jnp.where(core == 0, y, x)

    def chip(first, second):
        first, second = lax.rem(first + size, size), lax.rem(second + size, size)
        return jnp.where(core == 0, second * size + first, first * size + second)

    def device(first, second):
        first, second = lax.rem(first + size, size), lax.rem(second + size, size)
        return {
            "dap_0": jnp.where(core == 0, second, first),
            "dap_1": jnp.where(core == 0, first, second),
        }

    partner = {"dap_2": 1 - core}
    barrier = pltpu.get_barrier_semaphore()
    neighbours = [device(main + k, side) for k in range(1, size)]
    neighbours += [device(main, side + k) for k in (1, -1, 2, -2)] + [partner]
    for neighbour in neighbours:
        pl.semaphore_signal(barrier, inc=1, device_id=neighbour, device_id_type=mesh)

    groups = x_ref.shape[0] // (2 * sites * OUTER_CHANNELS)
    span = seqs // groups
    pick = one_hot(
        sites * span, 2 * sites * span,
        lambda o, k: k == (o % span) * (2 * sites) + core * sites + o // span,
    ).astype(BF16)
    for b in range(groups):
        rows = jnp.dot(
            pick, x_ref[2 * sites * span * b : 2 * sites * span * (b + 1), :],
            preferred_element_type=F32,
        ).astype(BF16)
        for r in range(sites):
            xs[r, span * b : span * (b + 1), :] = rows[span * r : span * (r + 1)]

    half = seqs // 2
    order = one_hot(
        seqs, seqs,
        lambda o, k: k == ((o % half) // 2) * 4 + (o // half) * 2 + o % 2,
    )
    order = (order * chain_ref[...].astype(F32)).astype(BF16)
    present = present_ref[...].astype(F32).astype(BF16)
    live = jnp.dot(order, present, preferred_element_type=F32).astype(BF16)
    own_site = (chip(main, side) * 2 + core) * sites
    select = one_hot(8, residues, lambda o, j: j == own_site + o).astype(BF16)
    keep[...] = contract_lanes(select, live)

    head_of_lane = lax.broadcasted_iota(jnp.int32, (1, inner), 1) // HEAD_CHANNELS
    shift = jnp.sum(
        one_hot(channels, channels, lambda o, c: o == c) * shift_ref[...], axis=1, keepdims=True
    )

    def remote(src, dst, send, recv, target):
        return pltpu.make_async_remote_copy(
            src_ref=src, dst_ref=dst, send_sem=sends.at[send], recv_sem=recv,
            device_id=target, device_id_type=mesh,
        )

    def index(offset):
        return offset % size

    def ring(r, along_main, origin, sign, step):
        reach = origin - sign * step
        if along_main:
            ref = lambda offset: chunks.at[index(offset), r]
            target, recv, send = device(main + sign * step, side), main_recv, 0
        else:
            ref = lambda offset: columns.at[index(offset), core, r]
            target, recv, send = device(main, side + sign * step), side_recv, 1
        src, dst = ref(origin), ref(reach)
        where = index(reach)
        if abs(reach) == far:
            rows = (channels if along_main else OUTER_CHANNELS) // 2
            first = 0 if sign > 0 else rows
            src, dst = src.at[pl.ds(first, rows)], dst.at[pl.ds(first, rows)]
            where = far if sign > 0 else size
        return remote(src, dst, send, recv.at[r, where], target)

    def swap(r, offset):
        return remote(
            chunks.at[index(offset), r, pl.ds(OUTER_CHANNELS, OUTER_CHANNELS)],
            columns.at[index(offset), core, r], 2, swap_recv.at[r, index(offset)], partner,
        )

    def swap_wait(r, offset):
        ref = columns.at[index(offset), 1 - core, r]
        remote(ref, ref, 2, swap_recv.at[r, index(offset)], partner).wait_recv()

    def launch(r):
        for step in (2, 1):
            for along_main in (True, False):
                for sign in (1, -1):
                    ring(r, along_main, 0, sign, step).start()
        swap(r, 0).start()

    def relay(r):
        for along_main in (True, False):
            for sign in (1, -1):
                ring(r, along_main, 0, sign, 2).wait_recv()
                ring(r, along_main, -2 * sign, sign, 2).start()
                ring(r, along_main, -2 * sign, sign, 1).start()
                if along_main:
                    swap(r, -2 * sign).start()
        for sign in (1, -1):
            ring(r, True, 0, sign, 1).wait_recv()
            swap(r, -sign).start()

    def relay_far(r):
        for sign in (1, -1):
            ring(r, True, -2 * sign, sign, 1).wait_recv()
            swap(r, -3 * sign).start()
        for sign in (1, -1):
            ring(r, True, -2 * sign, sign, 2).wait_recv()
        swap(r, far).start()

    def one_site(r, carry):
        x = xs[r].astype(F32)
        normed = normalize(x, gain_ref[...], offset_ref[...])
        query_key = jnp.dot(normed, qk_ref[...], preferred_element_type=F32)
        value_gate = jnp.dot(normed, vg_ref[...], preferred_element_type=F32)
        query = (query_key[:, :inner] * HEAD_CHANNELS ** (-0.5)).astype(BF16)
        key = query_key[:, inner:].astype(BF16)
        value = value_gate[:, :inner].astype(BF16)
        gate = jax.nn.sigmoid(value_gate[:, inner:] + gate_ref[...])
        present_row = keep[pl.ds(r, 1), :]
        alive = present_row > 0
        mixed = jnp.zeros((seqs, inner), F32)
        for h in range(HEAD_COUNT):
            own = head_of_lane == h
            query_h = query * own.astype(F32).astype(BF16)
            scores = jnp.where(alive, contract_lanes(query_h, key), MASKED)
            exponent = jnp.exp(scores - jnp.max(scores, axis=-1, keepdims=True))
            weight = jnp.sum(exponent, axis=-1, keepdims=True)
            part = jnp.dot(exponent.astype(BF16), value, preferred_element_type=F32)
            mixed = jnp.where(own, part * (1.0 / weight), mixed)
        gated = (mixed * gate).astype(BF16)
        update = jnp.dot(gated, exit_ref[...], preferred_element_type=F32) + exit_add_ref[...]
        after = (x + update).astype(BF16)
        again = normalize(after.astype(F32), gain2_ref[...], offset2_ref[...])
        both = ((contract_lanes(twin_ref[...], again) + shift) * present_row).astype(BF16)
        chunks[0, r] = both
        columns[0, core, r] = both[OUTER_CHANNELS:]
        ys[r] = after

        @pl.when(r == 0)
        def _():
            pl.semaphore_wait(barrier, len(neighbours))

        launch(r)

        @pl.when(r >= 2)
        def _():
            relay(r - 2)

        return carry

    lax.fori_loop(0, sites, one_site, 0)

    group = 2 * span
    place_back = one_hot(
        group * sites, group * sites,
        lambda o, k: k
        == (
            ((o % sites) * 2 + (o // (2 * sites)) % 2) * span
            + (o // (4 * sites)) * 2
            + (o // sites) % 2
        ),
    ).astype(BF16)
    for g in range(seqs // group):
        stack = jnp.concatenate(
            [
                ys[r, half * c + span * g : half * c + span * (g + 1), :]
                for r in range(sites)
                for c in range(2)
            ],
            axis=0,
        )
        rows = jnp.dot(place_back, stack, preferred_element_type=F32).astype(BF16)
        placed[group * g : group * (g + 1)] = rows.reshape(group, sites, width)

    wide[...] = couple_ref[...].astype(F32)
    blocks[...] = jnp.zeros_like(blocks)
    for e in range(OUTER_CHANNELS):
        rows = wide[pl.ds(e, OUTER_CHANNELS, stride=OUTER_CHANNELS), :].astype(BF16)
        for i in range(sites):
            row = e * pack + i * OUTER_CHANNELS
            blocks[row : row + OUTER_CHANNELS, i * PAIR_DIM : (i + 1) * PAIR_DIM] = rows
    relay(sites - 2)

    def row_site(k):
        first = lax.rem(main + k // sites, size)
        at = jnp.where(core == 0, side * size + first, first * size + side)
        return (at * 2 + core) * sites + k % sites

    def column_site(k):
        second = lax.rem(side + k // chip_rows, size)
        at = jnp.where(core == 0, second * size + main, main * size + second)
        return at * chip_rows + k % chip_rows

    lanes = size * sites
    row_pick = one_hot(
        residues, 128, lambda j, k: (j == row_site(k)) & (k < lanes)
    ).astype(BF16)
    column_pick = one_hot(size * chip_rows, residues, lambda k, j: j == column_site(k)).astype(BF16)
    live_rows = jnp.dot(live, row_pick, preferred_element_type=F32).astype(BF16)
    live_columns = contract_lanes(column_pick, live).astype(BF16)
    counts = jnp.dot(live_columns, live_rows, preferred_element_type=F32).astype(BF16)
    spread = one_hot(128, size * pack, lambda k, l: k == l // OUTER_CHANNELS).astype(BF16)
    counts = jnp.dot(counts, spread, preferred_element_type=F32)
    inverse[...] = 1.0 / jnp.maximum(counts, 1.0)

    after_copy = pltpu.make_async_copy(placed, after_ref, local_sem.at[0])
    after_copy.start()
    relay(sites - 1)

    near = [0, -1, 1, -2, 2]
    quads = [(-2, 2), (-1, 1), (0, -3), (3, far)]
    batches = [[far, -3, 3, 2], [0, -1, 1, -2]]
    ranks = batches[0] + batches[1]
    turn = [0]

    def multiply(offset, q):
        members = [index(b) for b in quads[q]]
        quad = jnp.concatenate(
            [columns[b].reshape(chip_rows * OUTER_CHANNELS, seqs) for b in members], axis=0
        )
        left = chunks[index(offset), :, :OUTER_CHANNELS, :].reshape(pack, seqs)
        buffer = turn[0] % 2
        turn[0] += 1
        sums[buffer] = contract_lanes(quad, left)
        lanes = slice(pack * index(offset), pack * (index(offset) + 1))
        scale = jnp.concatenate(
            [inverse[chip_rows * b : chip_rows * (b + 1), lanes] for b in members], axis=0
        )
        first = ranks.index(offset) * size * chip_rows + 2 * chip_rows * q
        for e in range(OUTER_CHANNELS):
            rows = sums[buffer, pl.ds(e, 2 * chip_rows, stride=OUTER_CHANNELS), :]
            terms[first : first + 2 * chip_rows, e * pack : (e + 1) * pack] = (
                rows * scale
            ).astype(BF16)

    def project(batch):
        count = size * chip_rows
        first = batch * len(batches[0]) * count
        rows = slice(first, first + len(batches[0]) * count)
        result = jnp.dot(terms[rows, :], blocks[...], preferred_element_type=F32)
        for k in range(len(batches[0])):
            for q, members in enumerate(quads):
                for t, b in enumerate(members):
                    row = k * count + (2 * q + t) * chip_rows
                    to = lax.rem(side + b + size, size) * chip_rows
                    to = pl.multiple_of(first + k * count + to, chip_rows)
                    total[pl.ds(to, chip_rows), :] = result[row : row + chip_rows]
        for k in range(len(batches[0])):
            at = batch * len(batches[0]) + k
            for i in range(sites):
                part = total[at * count : (at + 1) * count, i * PAIR_DIM : (i + 1) * PAIR_DIM]
                part = (part + pair_shift_ref[...]).astype(BF16)
                stage[at, i] = part.reshape(size, chip_rows, PAIR_DIM)

    def deliver(batch):
        for offset in batches[batch]:
            src = stage.at[ranks.index(offset)]
            for c in range(2):

                @pl.when(core == c)
                def _():
                    dst = out_ref.at[:, :, main] if c == 0 else out_ref.at[:, main]
                    if offset:
                        remote(src, dst, 3, out_recv, device(main + offset, side)).start()
                    else:
                        pltpu.make_async_copy(src, dst, local_sem.at[1]).start()

    for r in range(sites):
        for sign in (1, -1):
            ring(r, False, 0, sign, 1).wait_recv()
        for offset in near:
            swap_wait(r, offset)
    for q in (0, 1):
        for offset in near:
            multiply(offset, q)
    for r in range(sites):
        relay_far(r)
    for r in range(sites):
        for step in (1, 2):
            for sign in (1, -1):
                ring(r, False, -2 * sign, sign, step).wait_recv()
        for offset in (-3, 3, far):
            swap_wait(r, offset)
    for batch in (0, 1):
        for offset in batches[batch]:
            for q in range(len(quads)):
                if q > 1 or offset not in near:
                    multiply(offset, q)
        project(batch)
        deliver(batch)

    for buffer, send in (
        (chunks.at[pl.ds(0, size - 1)], 0),
        (columns.at[pl.ds(0, size - 1), 0], 1),
        (columns.at[:, 0], 2),
        (stage.at[pl.ds(0, size - 1)], 3),
    ):
        pltpu.make_async_copy(buffer, buffer, sends.at[send]).wait()
    arrived = stage.at[pl.ds(0, size - 1)]
    pltpu.make_async_copy(arrived, arrived, out_recv).wait()
    own = stage.at[ranks.index(0)]
    pltpu.make_async_copy(own, own, local_sem.at[1]).wait()
    after_copy.wait()


def attend_pairs(x, present, *rest, size):
    seqs, residues = present.shape
    width = x.shape[1]
    sites = x.shape[0] // (2 * seqs)
    pack = sites * OUTER_CHANNELS
    chip_rows = 2 * sites
    couple = rest[-2]
    count = size * chip_rows
    hbm = pl.BlockSpec(memory_space=pl.ANY)
    vmem = pl.BlockSpec(memory_space=pltpu.VMEM)
    dma = pltpu.SemaphoreType.DMA
    return pl.pallas_call(
        functools.partial(core_kernel, size),
        out_shape=(
            jax.ShapeDtypeStruct((seqs, sites, width), BF16),
            jax.ShapeDtypeStruct((sites, size, size, chip_rows, PAIR_DIM), BF16),
        ),
        in_specs=[vmem] * (2 + len(rest)),
        out_specs=(hbm, hbm),
        scratch_shapes=[
            pltpu.VMEM((sites, seqs, width), BF16),
            pltpu.VMEM((sites, seqs, width), BF16),
            pltpu.VMEM((8, seqs), F32),
            pltpu.VMEM((count, size * pack), F32),
            pltpu.VMEM((size, sites, 2 * OUTER_CHANNELS, seqs), BF16),
            pltpu.VMEM((size, 2, sites, OUTER_CHANNELS, seqs), BF16),
            pltpu.VMEM((OUTER_CHANNELS * pack, sites * PAIR_DIM), BF16),
            pltpu.VMEM(couple.shape, F32),
            pltpu.VMEM((2, 2 * chip_rows * OUTER_CHANNELS, pack), F32),
            pltpu.VMEM((size * count, OUTER_CHANNELS * pack), BF16),
            pltpu.VMEM((size * count, sites * PAIR_DIM), F32),
            pltpu.VMEM((size, sites, size, chip_rows, PAIR_DIM), BF16),
            pltpu.VMEM((seqs, sites, width), BF16),
            dma((sites, size + 1)),
            dma((sites, size + 1)),
            dma((sites, size)),
            dma,
            dma((4,)),
            dma((2,)),
        ],
        compiler_params=pltpu.CompilerParams(
            vmem_limit_bytes=VMEM_LIMIT, collective_id=1, has_side_effects=True
        ),
        name="attend_pairs",
    )(x, present, *rest)


def exchange_kernel(size, x_ref, out_ref, sent, got, swap_send, swap_got, own_sem):
    y, x, core = (lax.axis_index(a) for a in DAP)
    chips = size * size
    partner = {"dap_2": 1 - core}
    here = y * size + x
    far = size // 2
    steps = [(dy, dx) for dy in range(size) for dx in range(size) if dy or dx]
    away = lambda d: min(d, size - d)
    steps.sort(key=lambda d: -(away(d[0]) + away(d[1])))
    mesh = pl.DeviceIdType.MESH

    def chip(step):
        return lax.rem(y + step[0], size), lax.rem(x + step[1], size)

    own = pltpu.make_async_copy(x_ref.at[:, here], out_ref.at[core, here], own_sem)
    own.start()
    barrier = pltpu.get_barrier_semaphore()
    for step in steps:
        row, column = chip(step)
        pl.semaphore_signal(
            barrier, inc=1, device_id={"dap_0": row, "dap_1": column}, device_id_type=mesh
        )
    pl.semaphore_signal(barrier, inc=1, device_id=partner, device_id_type=mesh)
    pl.semaphore_wait(barrier, chips)
    for step in steps:
        row, column = chip(step)
        pltpu.make_async_remote_copy(
            src_ref=x_ref.at[:, row * size + column], dst_ref=out_ref.at[core, here],
            send_sem=sent, recv_sem=got, device_id={"dap_0": row, "dap_1": column},
            device_id_type=mesh,
        ).start()
    own.wait()
    others = out_ref.at[core, pl.ds(0, chips - 1)]
    pltpu.make_async_copy(others, others, got).wait()
    swap = pltpu.make_async_remote_copy(
        src_ref=out_ref.at[core], dst_ref=out_ref.at[core], send_sem=swap_send,
        recv_sem=swap_got, device_id=partner, device_id_type=mesh,
    )
    swap.start()
    pltpu.make_async_copy(others, others, sent).wait()
    swap.wait()


def exchange(x, size):
    seqs, residues, width = x.shape
    chips = size * size
    x = x.reshape(seqs, chips, residues // chips, width)
    out = pl.pallas_call(
        functools.partial(exchange_kernel, size),
        out_shape=jax.ShapeDtypeStruct((2, chips, seqs, residues // chips, width), x.dtype),
        in_specs=[pl.BlockSpec(memory_space=pl.ANY)],
        out_specs=pl.BlockSpec(memory_space=pl.ANY),
        scratch_shapes=[pltpu.SemaphoreType.DMA] * 5,
        compiler_params=pltpu.CompilerParams(
            vmem_limit_bytes=VMEM_LIMIT, collective_id=2, has_side_effects=True
        ),
        name="exchange",
    )(x)
    return out.reshape(2 * seqs * residues, width)


GATHER_RING = pltpu.CompilerParams(
    vmem_limit_bytes=VMEM_LIMIT, collective_id=1, has_side_effects=True
)


def ring_order(size):
    far = size // 2
    offsets = [0]
    for hop in range(1, far):
        offsets += [-hop, hop]
    offsets.append(far)
    events = []
    for offset in offsets:
        ready = 2.6 + 1.4 * abs(offset) if offset else 0.0
        if offset:
            events.append((ready, 0, 0, offset))
        for hop in range(1, far + 1):
            events.append((ready + 3.3 * hop + 0.01, 1, hop, offset))
    return sorted(events, key=lambda event: event[:2]), offsets


def gather_kernel(size, own_ref, all_ref, held, p_recv, s_recv, x_recv, send_sem, out_sem, in_sem):
    far = size // 2
    y, x, core = (lax.axis_index(a) for a in DAP)
    half = own_ref.shape[0] // 2

    def at(first, second):
        row = jnp.where(core == 0, second, first)
        column = jnp.where(core == 0, first, second)
        return lax.rem(row + size, size), lax.rem(column + size, size)

    main = jnp.where(core == 0, x, y)
    side = jnp.where(core == 0, y, x)

    def device(first, second):
        row, column = at(first, second)
        return {"dap_0": row, "dap_1": column}

    def slot(first, second, which):
        row, column = at(first, second)
        return (row * size + column) * 2 + which

    partner = {"dap_2": 1 - core}
    events, offsets = ring_order(size)
    neighbours = [device(main + offset, side) for offset in offsets if offset]
    neighbours += [device(main, side + 1), device(main, side - 1), partner]
    barrier = pltpu.get_barrier_semaphore()
    own_copy = pltpu.make_async_copy(own_ref, held.at[slot(main, side, core)], in_sem)
    own_copy.start()
    for neighbour in neighbours:
        pl.semaphore_signal(
            barrier, inc=1, device_id=neighbour, device_id_type=pl.DeviceIdType.MESH
        )
    pl.semaphore_wait(barrier, len(neighbours))
    own_copy.wait()

    def piece(first, second, which, hop, sign):
        ref = held.at[slot(first, second, which)]
        if hop < far:
            return ref
        return ref.at[pl.ds(0 if sign > 0 else half, half)]

    def remote(ref, recv, target):
        return pltpu.make_async_remote_copy(
            src_ref=ref, dst_ref=ref, send_sem=send_sem, recv_sem=recv,
            device_id=target, device_id_type=pl.DeviceIdType.MESH,
        )

    def along_main(offset):
        ref = held.at[slot(main, side, core)]
        remote(ref, p_recv.at[offsets.index(offset)], device(main - offset, side)).start()

    def along_side(offset, index, hop, sign):
        ref = piece(main + offset, side - sign * (hop - 1), core, hop, sign)
        remote(ref, s_recv.at[index, (sign + 1) // 2, hop - 1], device(main, side + sign)).start()

    def finished(first, second, order):
        ref = held.at[slot(first, second, core)]
        remote(ref, x_recv.at[order], partner).start()
        pltpu.make_async_copy(ref, all_ref.at[slot(first, second, core)], out_sem).start()
        done.append((first, second))

    def from_partner(order):
        first, second = done[order]
        ref = held.at[swapped_slot(first, second)]
        remote(ref, x_recv.at[order], partner).wait_recv()
        pltpu.make_async_copy(ref, all_ref.at[swapped_slot(first, second)], out_sem).start()

    def swapped_slot(first, second):
        d_first, d_second = first - main, second - side
        row = jnp.where(core == 0, main_row + d_first, main_row + d_second)
        column = jnp.where(core == 0, main_column + d_second, main_column + d_first)
        row, column = lax.rem(row + size, size), lax.rem(column + size, size)
        return (row * size + column) * 2 + (1 - core)

    main_row, main_column = y, x
    done = []
    for sign in (1, -1):
        along_side(0, 0, 1, sign)
    for offset in offsets:
        if offset:
            along_main(offset)
    finished(main, side, 0)
    lag, taken = 6, 0
    for _, kind, hop, offset in events:
        index = offsets.index(offset)
        if kind == 0:
            ref = held.at[slot(main + offset, side, core)]
            remote(ref, p_recv.at[index], partner).wait_recv()
            for way in (1, -1):
                along_side(offset, index, 1, way)
            finished(main + offset, side, len(done))
        else:
            for sign in (1, -1):
                ref = piece(main + offset, side - sign * hop, core, hop, sign)
                remote(ref, s_recv.at[index, (sign + 1) // 2, hop - 1], partner).wait_recv()
                if hop < far:
                    along_side(offset, index, hop + 1, sign)
                    finished(main + offset, side - sign * hop, len(done))
            if hop == far:
                finished(main + offset, side + far, len(done))
        while taken < len(done) - lag:
            from_partner(taken)
            taken += 1
    while taken < len(done):
        from_partner(taken)
        taken += 1
    sent = (size - 1) * (size + 1) + size * size
    drained = held.at[pl.ds(0, sent)]
    pltpu.make_async_copy(drained, drained, send_sem).wait()
    pltpu.make_async_copy(held, all_ref, out_sem).wait()


def gather_right(own, size):
    owners = 2 * size * size
    return pl.pallas_call(
        functools.partial(gather_kernel, size),
        out_shape=jax.ShapeDtypeStruct((owners, *own.shape), own.dtype),
        in_specs=[pl.BlockSpec(memory_space=pl.ANY)],
        out_specs=pl.BlockSpec(memory_space=pl.ANY),
        scratch_shapes=[
            pltpu.VMEM((owners, *own.shape), own.dtype),
            pltpu.SemaphoreType.DMA((size,)),
            pltpu.SemaphoreType.DMA((size, 2, size // 2)),
            pltpu.SemaphoreType.DMA((size * size,)),
            pltpu.SemaphoreType.DMA,
            pltpu.SemaphoreType.DMA,
            pltpu.SemaphoreType.DMA,
        ],
        compiler_params=GATHER_RING,
        name="gather_right",
    )(own)


def shards(
    homolog_stack_tensor,
    occupancy_indicator,
    chain_existence_flags,
    focus_normal_factor,
    focus_normal_addend,
    probe_index_weights,
    payload_valve_weights,
    logistic_valve_addend,
    focus_exit_weights,
    focus_exit_addend,
    product_mean_layer_stretch,
    product_mean_layer_shift,
    twin_map_matrix,
    twin_map_shift,
    couple_map_matrix,
    couple_map_shift,
):
    seqs, residues = occupancy_indicator.shape
    width = homolog_stack_tensor.shape[-1]
    size = lax.axis_size("dap_0")
    row = lambda v: v[None, :]
    after, pair_rows = attend_pairs(
        exchange(homolog_stack_tensor, size),
        occupancy_indicator,
        row(chain_existence_flags),
        row(focus_normal_factor),
        row(focus_normal_addend),
        probe_index_weights,
        payload_valve_weights,
        row(logistic_valve_addend),
        focus_exit_weights,
        row(focus_exit_addend),
        row(product_mean_layer_stretch),
        row(product_mean_layer_shift),
        twin_map_matrix.T,
        row(twin_map_shift),
        couple_map_matrix,
        row(couple_map_shift),
        size=size,
    )
    return (after, pair_rows.reshape(-1, residues, PAIR_DIM))


def solution(mesh):
    split = Mesh(
        mesh.devices.reshape(mesh.shape["grp"], 8, 8, 2), ("grp", "dap_0", "dap_1", "dap_2")
    )
    return jax.shard_map(
        shards,
        mesh=split,
        in_specs=(
            P(GRP_DAP, None, None),
            P("grp", None),
            P("grp"),
            P(),
            P(),
            P(),
            P(),
            P(),
            P(),
            P(),
            P(),
            P(),
            P(),
            P(),
            P(),
            P(),
        ),
        out_specs=(P("grp", DAP, None), P(GRP_DAP, None, None)),
        check_vma=False,
    )
```

```python
import functools

import jax
import jax.numpy as jnp
from jax import lax
from jax.experimental import pallas as pl
from jax.experimental.pallas import tpu as pltpu
from jax.sharding import Mesh
from jax.sharding import PartitionSpec as P

HEAD_COUNT = 8
HEAD_CHANNELS = 32
OUTER_CHANNELS = 32
PAIR_DIM = 128
DAP = ("dap_0", "dap_1", "dap_2")
GRP_DAP = ("grp", "dap_0", "dap_1", "dap_2")
F32 = jnp.float32
BF16 = jnp.bfloat16
VMEM_LIMIT = 60 * 1024 * 1024
PITCH = 40


EPSILON = 1e-05
MASKED = -100000.0


def normalize(widened, gain, offset):
    centred = widened - jnp.mean(widened, axis=-1, keepdims=True)
    variance = jnp.mean(centred * centred, axis=-1, keepdims=True)
    return (centred * lax.rsqrt(variance + EPSILON) * gain + offset).astype(BF16)


def contract_lanes(a, b):
    return lax.dot_general(a, b, (((1,), (1,)), ((), ())), preferred_element_type=F32)


def one_hot(rows, columns, test):
    row = lax.broadcasted_iota(jnp.int32, (rows, columns), 0)
    column = lax.broadcasted_iota(jnp.int32, (rows, columns), 1)
    return jnp.where(test(row, column), 1.0, 0.0)


def core_kernel(
    size, source_ref, present_hbm, qk_hbm, vg_hbm, exit_hbm, couple_hbm, chain_ref, gain_ref,
    offset_ref, gate_ref, exit_add_ref, gain2_ref, offset2_ref, twin_ref, shift_ref,
    pair_shift_ref,
    after_ref, out_ref,
    landed, present_ref, qk_ref, vg_ref, exit_ref, couple_ref, xs, ys, keep, inverse, chunks, columns, blocks, wide, sums, terms, total, stage, placed,
    main_recv, side_recv, swap_recv, out_recv, sends, local_sem, load_sem, got, sent, crossed,
):
    sites, seqs, width = xs.shape
    residues = present_ref.shape[1]
    pack = sites * OUTER_CHANNELS
    inner = HEAD_COUNT * HEAD_CHANNELS
    channels = 2 * OUTER_CHANNELS
    chip_rows = 2 * sites
    far = size // 2
    mesh = pl.DeviceIdType.MESH
    y, x, core = (lax.axis_index(a) for a in DAP)
    main = jnp.where(core == 0, x, y)
    side = jnp.where(core == 0, y, x)

    def chip(first, second):
        first, second = lax.rem(first + size, size), lax.rem(second + size, size)
        return jnp.where(core == 0, second * size + first, first * size + second)

    def device(first, second):
        first, second = lax.rem(first + size, size), lax.rem(second + size, size)
        return {
            "dap_0": jnp.where(core == 0, second, first),
            "dap_1": jnp.where(core == 0, first, second),
        }

    partner = {"dap_2": 1 - core}
    chips = size * size
    here = y * size + x
    away = lambda d: min(d, size - d)
    steps = [(dy, dx) for dy in range(size) for dx in range(size) if dy or dx]
    steps.sort(key=lambda d: -(away(d[0]) + away(d[1])))
    barrier = pltpu.get_barrier_semaphore()
    for dy, dx in steps:
        peer = {"dap_0": lax.rem(y + dy, size), "dap_1": lax.rem(x + dx, size)}
        pl.semaphore_signal(barrier, inc=1, device_id=peer, device_id_type=mesh)
    pl.semaphore_signal(barrier, inc=1, device_id=partner, device_id_type=mesh)
    own_rows = pltpu.make_async_copy(
        source_ref.at[:, here], landed.at[core, here], local_sem.at[2]
    )
    own_rows.start()
    loads = [
        pltpu.make_async_copy(a, b, load_sem.at[i])
        for i, (a, b) in enumerate(
            (
                (present_hbm, present_ref),
                (couple_hbm, couple_ref),
                (qk_hbm, qk_ref),
                (vg_hbm, vg_ref),
                (exit_hbm, exit_ref),
            )
        )
    ]
    for load in loads:
        load.start()
    pl.semaphore_wait(barrier, chips)
    for dy, dx in steps:
        row, column = lax.rem(y + dy, size), lax.rem(x + dx, size)
        pltpu.make_async_remote_copy(
            src_ref=source_ref.at[:, row * size + column], dst_ref=landed.at[core, here],
            send_sem=sent, recv_sem=got, device_id={"dap_0": row, "dap_1": column},
            device_id_type=mesh,
        ).start()
    for load in loads:
        load.wait()

    half = seqs // 2
    order = one_hot(
        seqs, seqs,
        lambda o, k: k == ((o % half) // 2) * 4 + (o // half) * 2 + o % 2,
    )
    order = (order * chain_ref[...].astype(F32)).astype(BF16)
    present = present_ref[...].astype(F32).astype(BF16)
    live = jnp.dot(order, present, preferred_element_type=F32).astype(BF16)
    own_site = (chip(main, side) * 2 + core) * sites
    select = one_hot(8, residues, lambda o, j: j == own_site + o).astype(BF16)
    keep[...] = contract_lanes(select, live)

    head_of_lane = lax.broadcasted_iota(jnp.int32, (1, inner), 1) // HEAD_CHANNELS
    shift = jnp.sum(
        one_hot(channels, channels, lambda o, c: o == c) * shift_ref[...], axis=1, keepdims=True
    )

    wide[...] = couple_ref[...].astype(F32)
    blocks[...] = jnp.zeros_like(blocks)
    for e in range(OUTER_CHANNELS):
        rows = wide[pl.ds(e, OUTER_CHANNELS, stride=OUTER_CHANNELS), :].astype(BF16)
        for i in range(sites):
            row = e * pack + i * OUTER_CHANNELS
            blocks[row : row + OUTER_CHANNELS, i * PAIR_DIM : (i + 1) * PAIR_DIM] = rows
    def row_site(k):
        first = lax.rem(main + k // sites, size)
        at = jnp.where(core == 0, side * size + first, first * size + side)
        return (at * 2 + core) * sites + k % sites

    def column_site(k):
        second = lax.rem(side + k // chip_rows, size)
        at = jnp.where(core == 0, second * size + main, main * size + second)
        return at * chip_rows + k % chip_rows

    lanes = size * sites
    row_pick = one_hot(
        residues, 128, lambda j, k: (j == row_site(k)) & (k < lanes)
    ).astype(BF16)
    column_pick = one_hot(size * chip_rows, residues, lambda k, j: j == column_site(k)).astype(BF16)
    live_rows = jnp.dot(live, row_pick, preferred_element_type=F32).astype(BF16)
    live_columns = contract_lanes(column_pick, live).astype(BF16)
    counts = jnp.dot(live_columns, live_rows, preferred_element_type=F32).astype(BF16)
    spread = one_hot(128, size * pack, lambda k, l: k == l // OUTER_CHANNELS).astype(BF16)
    counts = jnp.dot(counts, spread, preferred_element_type=F32)
    inverse[...] = 1.0 / jnp.maximum(counts, 1.0)

    others = landed.at[core, pl.ds(0, chips - 1)]
    own_rows.wait()
    pltpu.make_async_copy(others, others, got).wait()
    cross = pltpu.make_async_remote_copy(
        src_ref=landed.at[core], dst_ref=landed.at[core], send_sem=crossed.at[0],
        recv_sem=crossed.at[1], device_id=partner, device_id_type=mesh,
    )
    cross.start()

    span = OUTER_CHANNELS
    pick = one_hot(
        sites * span, 2 * sites * span,
        lambda o, k: k == (o % span) * (2 * sites) + core * sites + o // span,
    ).astype(BF16)
    band = 2 * sites * span

    def sort_rows(which):
        rows_in = landed[which].reshape(chips * 2 * 2 * sites, width)
        for b in range(half // span):
            rows = jnp.dot(
                pick, rows_in[band * b : band * (b + 1)], preferred_element_type=F32
            ).astype(BF16)
            for r in range(sites):
                first = pl.multiple_of(which * half + span * b, span)
                xs[r, pl.ds(first, span), :] = rows[span * r : span * (r + 1)]

    sort_rows(core)
    pltpu.make_async_copy(others, others, sent).wait()
    cross.wait()
    sort_rows(1 - core)

    def remote(src, dst, send, recv, target):
        return pltpu.make_async_remote_copy(
            src_ref=src, dst_ref=dst, send_sem=sends.at[send], recv_sem=recv,
            device_id=target, device_id_type=mesh,
        )

    def index(offset):
        return offset % size

    def ring(r, along_main, origin, sign, step, whole=False):
        reach = origin - sign * step
        if along_main:
            ref = lambda offset: chunks.at[index(offset), r]
            target, recv, send = device(main + sign * step, side), main_recv, 0
        else:
            ref = lambda offset: columns.at[index(offset), core, r]
            target, recv, send = device(main, side + sign * step), side_recv, 1
        src, dst = ref(origin), ref(reach)
        where = index(reach)
        if abs(reach) == far and not whole:
            rows = (channels if along_main else OUTER_CHANNELS) // 2
            first = 0 if sign > 0 else rows
            src, dst = src.at[pl.ds(first, rows)], dst.at[pl.ds(first, rows)]
            where = far if sign > 0 else size
        return remote(src, dst, send, recv.at[r, where], target)

    def swap(r, offset):
        return remote(
            chunks.at[index(offset), r, pl.ds(OUTER_CHANNELS, OUTER_CHANNELS)],
            columns.at[index(offset), core, r], 2, swap_recv.at[r, index(offset)], partner,
        )

    def swap_wait(r, offset):
        ref = columns.at[index(offset), 1 - core, r]
        remote(ref, ref, 2, swap_recv.at[r, index(offset)], partner).wait_recv()

    def launch(r):
        for step in (2, 1):
            for along_main in (True, False):
                for sign in (1, -1):
                    ring(r, along_main, 0, sign, step).start()
        swap(r, 0).start()

    def launch_all(r):
        for step in (far, 3, 2, 1):
            for along_main in (True, False):
                for sign in (1, -1) if step < far else (1,):
                    ring(r, along_main, 0, sign, step, True).start()
        swap(r, 0).start()

    def relay_all(r):
        for step in (1, 2, 3, far):
            for sign in (1, -1) if step < far else (1,):
                ring(r, True, 0, sign, step, True).wait_recv()
                swap(r, index(-sign * step)).start()

    def relay(r):
        for along_main in (True, False):
            for sign in (1, -1):
                ring(r, along_main, 0, sign, 2).wait_recv()
                ring(r, along_main, -2 * sign, sign, 2).start()
                ring(r, along_main, -2 * sign, sign, 1).start()
                if along_main:
                    swap(r, -2 * sign).start()
        for sign in (1, -1):
            ring(r, True, 0, sign, 1).wait_recv()
            swap(r, -sign).start()

    def relay_far(r):
        for sign in (1, -1):
            ring(r, True, -2 * sign, sign, 1).wait_recv()
            swap(r, -3 * sign).start()
        for sign in (1, -1):
            ring(r, True, -2 * sign, sign, 2).wait_recv()
        swap(r, far).start()

    def one_site(r, carry):
        x = xs[r].astype(F32)
        normed = normalize(x, gain_ref[...], offset_ref[...])
        query_key = jnp.dot(normed, qk_ref[...], preferred_element_type=F32)
        value_gate = jnp.dot(normed, vg_ref[...], preferred_element_type=F32)
        query = (query_key[:, :inner] * HEAD_CHANNELS ** (-0.5)).astype(BF16)
        key = query_key[:, inner:].astype(BF16)
        value = value_gate[:, :inner].astype(BF16)
        gate = jax.nn.sigmoid(value_gate[:, inner:] + gate_ref[...])
        present_row = keep[pl.ds(r, 1), :]
        alive = present_row > 0
        mixed = jnp.zeros((seqs, inner), F32)
        for h in range(HEAD_COUNT):
            own = head_of_lane == h
            query_h = query * own.astype(F32).astype(BF16)
            scores = jnp.where(alive, contract_lanes(query_h, key), MASKED)
            exponent = jnp.exp(scores - jnp.max(scores, axis=-1, keepdims=True))
            weight = jnp.sum(exponent, axis=-1, keepdims=True)
            part = jnp.dot(exponent.astype(BF16), value, preferred_element_type=F32)
            mixed = jnp.where(own, part * (1.0 / weight), mixed)
        gated = (mixed * gate).astype(BF16)
        update = jnp.dot(gated, exit_ref[...], preferred_element_type=F32) + exit_add_ref[...]
        after = (x + update).astype(BF16)
        again = normalize(after.astype(F32), gain2_ref[...], offset2_ref[...])
        both = ((contract_lanes(twin_ref[...], again) + shift) * present_row).astype(BF16)
        chunks[0, r] = both
        columns[0, core, r] = both[OUTER_CHANNELS:]
        ys[r] = after

        @pl.when(r < sites - 1)
        def _():
            launch(r)

        @pl.when(r == sites - 1)
        def _():
            launch_all(r)

        @pl.when(r >= 2)
        def _():
            relay(r - 2)

        return carry

    lax.fori_loop(0, sites, one_site, 0)

    group = 2 * span
    place_back = one_hot(
        group * sites, group * sites,
        lambda o, k: k
        == (
            ((o % sites) * 2 + (o // (2 * sites)) % 2) * span
            + (o // (4 * sites)) * 2
            + (o // sites) % 2
        ),
    ).astype(BF16)
    for g in range(seqs // group):
        stack = jnp.concatenate(
            [
                ys[r, half * c + span * g : half * c + span * (g + 1), :]
                for r in range(sites)
                for c in range(2)
            ],
            axis=0,
        )
        rows = jnp.dot(place_back, stack, preferred_element_type=F32).astype(BF16)
        placed[group * g : group * (g + 1)] = rows.reshape(group, sites, width)

    relay(sites - 2)
    after_copy = pltpu.make_async_copy(placed, after_ref, local_sem.at[0])
    after_copy.start()
    for r in range(sites - 1):
        relay_far(r)
    relay_all(sites - 1)

    near = [0, -1, 1, -2, 2]
    quads = [(-2, 2), (-1, 1), (0, -3), (3, far)]
    batches = [[far, -3], [3, 2], [-2, 1, -1, 0]]
    ranks = sum(batches, [])
    turn = [0]

    def multiply(offset, q):
        members = [index(b) for b in quads[q]]
        quad = jnp.concatenate(
            [columns[b].reshape(chip_rows * OUTER_CHANNELS, seqs) for b in members], axis=0
        )
        left = chunks[index(offset), :, :OUTER_CHANNELS, :].reshape(pack, seqs)
        buffer = turn[0] % 2
        turn[0] += 1
        product = contract_lanes(quad, left)
        for j in range(2 * chip_rows):
            sums[buffer, PITCH * j : PITCH * j + OUTER_CHANNELS, :] = product[
                OUTER_CHANNELS * j : OUTER_CHANNELS * (j + 1)
            ]
        lanes = slice(pack * index(offset), pack * (index(offset) + 1))
        scale = jnp.concatenate(
            [inverse[chip_rows * b : chip_rows * (b + 1), lanes] for b in members], axis=0
        )
        first = ranks.index(offset) * size * chip_rows + 2 * chip_rows * q
        for e in range(OUTER_CHANNELS):
            rows = sums[buffer, pl.ds(e, 2 * chip_rows, stride=PITCH), :]
            terms[first : first + 2 * chip_rows, e * pack : (e + 1) * pack] = (
                rows * scale
            ).astype(BF16)

    def project(batch):
        count = size * chip_rows
        first = ranks.index(batches[batch][0])
        rows = slice(first * count, (first + len(batches[batch])) * count)
        result = jnp.dot(terms[rows, :], blocks[...], preferred_element_type=F32)
        for k in range(len(batches[batch])):
            for q, members in enumerate(quads):
                for t, b in enumerate(members):
                    row = k * count + (2 * q + t) * chip_rows
                    to = lax.rem(side + b + size, size) * chip_rows
                    to = pl.multiple_of((first + k) * count + to, chip_rows)
                    total[pl.ds(to, chip_rows), :] = result[row : row + chip_rows]
        for at in range(first, first + len(batches[batch])):
            for i in range(sites):
                part = total[at * count : (at + 1) * count, i * PAIR_DIM : (i + 1) * PAIR_DIM]
                part = (part + pair_shift_ref[...]).astype(BF16)
                stage[at, i] = part.reshape(size, chip_rows, PAIR_DIM)

    def deliver(batch):
        for offset in batches[batch]:
            src = stage.at[ranks.index(offset)]
            for c in range(2):

                @pl.when(core == c)
                def _():
                    dst = out_ref.at[:, :, main] if c == 0 else out_ref.at[:, main]
                    if offset:
                        remote(src, dst, 3, out_recv, device(main + offset, side)).start()
                    else:
                        pltpu.make_async_copy(src, dst, local_sem.at[1]).start()

    for r in range(sites):
        for sign in (1, -1):
            ring(r, False, 0, sign, 1).wait_recv()
        for offset in near:
            swap_wait(r, offset)
    for sign in (1, -1):
        ring(sites - 1, False, 0, sign, 2).wait_recv()
    for q in (0, 1):
        for offset in near:
            multiply(offset, q)
    for r in range(sites - 1):
        for step in (1, 2):
            for sign in (1, -1):
                ring(r, False, -2 * sign, sign, step).wait_recv()
    for sign in (1, -1):
        ring(sites - 1, False, 0, sign, 3, True).wait_recv()
    ring(sites - 1, False, 0, 1, far, True).wait_recv()
    for r in range(sites):
        for offset in (-3, 3, far):
            swap_wait(r, offset)
    for batch in range(len(batches)):
        for offset in batches[batch]:
            for q in range(len(quads)):
                if q > 1 or offset not in near:
                    multiply(offset, q)
        project(batch)
        deliver(batch)

    for buffer, send in (
        (chunks.at[pl.ds(0, size - 1)], 0),
        (columns.at[pl.ds(0, size - 1), 0], 1),
        (columns.at[:, 0], 2),
        (stage.at[pl.ds(0, size - 1)], 3),
    ):
        pltpu.make_async_copy(buffer, buffer, sends.at[send]).wait()
    arrived = stage.at[pl.ds(0, size - 1)]
    pltpu.make_async_copy(arrived, arrived, out_recv).wait()
    own = stage.at[ranks.index(0)]
    pltpu.make_async_copy(own, own, local_sem.at[1]).wait()
    after_copy.wait()


def attend_pairs(x, large, small, size):
    seqs, residues = large[0].shape
    part, _, width = x.shape
    chips = size * size
    chip_rows = residues // chips
    sites = chip_rows // 2
    pack = sites * OUTER_CHANNELS
    couple = large[-1]
    count = size * chip_rows
    x = x.reshape(part, chips, chip_rows, width)
    hbm = pl.BlockSpec(memory_space=pl.ANY)
    vmem = pl.BlockSpec(memory_space=pltpu.VMEM)
    dma = pltpu.SemaphoreType.DMA
    return pl.pallas_call(
        functools.partial(core_kernel, size),
        out_shape=(
            jax.ShapeDtypeStruct((seqs, sites, width), BF16),
            jax.ShapeDtypeStruct((sites, size, size, chip_rows, PAIR_DIM), BF16),
        ),
        in_specs=[hbm] * (1 + len(large)) + [vmem] * len(small),
        out_specs=(hbm, hbm),
        scratch_shapes=[
            pltpu.VMEM((2, chips, part, chip_rows, width), BF16),
            *[pltpu.VMEM(a.shape, a.dtype) for a in (large[0], *large[1:])],
            pltpu.VMEM((sites, seqs, width), BF16),
            pltpu.VMEM((sites, seqs, width), BF16),
            pltpu.VMEM((8, seqs), F32),
            pltpu.VMEM((count, size * pack), F32),
            pltpu.VMEM((size, sites, 2 * OUTER_CHANNELS, seqs), BF16),
            pltpu.VMEM((size, 2, sites, OUTER_CHANNELS, seqs), BF16),
            pltpu.VMEM((OUTER_CHANNELS * pack, sites * PAIR_DIM), BF16),
            pltpu.VMEM(couple.shape, F32),
            pltpu.VMEM((2, 2 * chip_rows * PITCH, pack), F32),
            pltpu.VMEM((size * count, OUTER_CHANNELS * pack), BF16),
            pltpu.VMEM((size * count, sites * PAIR_DIM), F32),
            pltpu.VMEM((size, sites, size, chip_rows, PAIR_DIM), BF16),
            pltpu.VMEM((seqs, sites, width), BF16),
            dma((sites, size + 1)),
            dma((sites, size + 1)),
            dma((sites, size)),
            dma,
            dma((4,)),
            dma((3,)),
            dma((5,)),
            dma,
            dma,
            dma((2,)),
        ],
        compiler_params=pltpu.CompilerParams(
            vmem_limit_bytes=VMEM_LIMIT, collective_id=1, has_side_effects=True
        ),
        name="attend_pairs",
    )(x, *large, *small)


def shards(
    homolog_stack_tensor,
    occupancy_indicator,
    chain_existence_flags,
    focus_normal_factor,
    focus_normal_addend,
    probe_index_weights,
    payload_valve_weights,
    logistic_valve_addend,
    focus_exit_weights,
    focus_exit_addend,
    product_mean_layer_stretch,
    product_mean_layer_shift,
    twin_map_matrix,
    twin_map_shift,
    couple_map_matrix,
    couple_map_shift,
):
    seqs, residues = occupancy_indicator.shape
    width = homolog_stack_tensor.shape[-1]
    size = lax.axis_size("dap_0")
    row = lambda v: v[None, :]
    after, pair_rows = attend_pairs(
        homolog_stack_tensor,
        (
            occupancy_indicator,
            probe_index_weights,
            payload_valve_weights,
            focus_exit_weights,
            couple_map_matrix,
        ),
        (
            row(chain_existence_flags),
            row(focus_normal_factor),
            row(focus_normal_addend),
            row(logistic_valve_addend),
            row(focus_exit_addend),
            row(product_mean_layer_stretch),
            row(product_mean_layer_shift),
            twin_map_matrix.T,
            row(twin_map_shift),
            row(couple_map_shift),
        ),
        size,
    )
    return (after, pair_rows.reshape(-1, residues, PAIR_DIM))


def solution(mesh):
    split = Mesh(
        mesh.devices.reshape(mesh.shape["grp"], 8, 8, 2), ("grp", "dap_0", "dap_1", "dap_2")
    )
    return jax.shard_map(
        shards,
        mesh=split,
        in_specs=(
            P(GRP_DAP, None, None),
            P("grp", None),
            P("grp"),
            P(),
            P(),
            P(),
            P(),
            P(),
            P(),
            P(),
            P(),
            P(),
            P(),
            P(),
            P(),
            P(),
        ),
        out_specs=(P("grp", DAP, None), P(GRP_DAP, None, None)),
        check_vma=False,
    )
```

```python
import functools

import jax
import jax.numpy as jnp
from jax import lax
from jax.experimental import pallas as pl
from jax.experimental.pallas import tpu as pltpu
from jax.sharding import Mesh
from jax.sharding import PartitionSpec as P

HEAD_COUNT = 8
HEAD_CHANNELS = 32
OUTER_CHANNELS = 32
PAIR_DIM = 128
DAP = ("dap_0", "dap_1", "dap_2")
GRP_DAP = ("grp", "dap_0", "dap_1", "dap_2")
F32 = jnp.float32
BF16 = jnp.bfloat16
VMEM_LIMIT = 60 * 1024 * 1024
PITCH = 40


EPSILON = 1e-05
MASKED = -100000.0


def normalize(widened, gain, offset):
    centred = widened - jnp.mean(widened, axis=-1, keepdims=True)
    variance = jnp.mean(centred * centred, axis=-1, keepdims=True)
    return (centred * lax.rsqrt(variance + EPSILON) * gain + offset).astype(BF16)


def contract_lanes(a, b):
    return lax.dot_general(a, b, (((1,), (1,)), ((), ())), preferred_element_type=F32)


def one_hot(rows, columns, test):
    row = lax.broadcasted_iota(jnp.int32, (rows, columns), 0)
    column = lax.broadcasted_iota(jnp.int32, (rows, columns), 1)
    return jnp.where(test(row, column), 1.0, 0.0)


def core_kernel(
    size, source_ref, present_hbm, qk_hbm, vg_hbm, exit_hbm, couple_hbm, chain_ref, gain_ref,
    offset_ref, gate_ref, exit_add_ref, gain2_ref, offset2_ref, twin_ref, shift_ref,
    pair_shift_ref,
    after_ref, out_ref,
    landed, present_ref, qk_ref, vg_ref, exit_ref, couple_ref, xs, ys, keep, inverse, chunks, columns, blocks, wide, sums, terms, total, stage, placed,
    main_recv, side_recv, swap_recv, out_recv, sends, local_sem, load_sem, got, sent, crossed,
    cross_recv,
):
    sites, seqs, width = xs.shape
    residues = present_ref.shape[1]
    pack = sites * OUTER_CHANNELS
    inner = HEAD_COUNT * HEAD_CHANNELS
    channels = 2 * OUTER_CHANNELS
    chip_rows = 2 * sites
    far = size // 2
    mesh = pl.DeviceIdType.MESH
    y, x, core = (lax.axis_index(a) for a in DAP)
    main = jnp.where(core == 0, x, y)
    side = jnp.where(core == 0, y, x)

    def chip(first, second):
        first, second = lax.rem(first + size, size), lax.rem(second + size, size)
        return jnp.where(core == 0, second * size + first, first * size + second)

    def device(first, second):
        first, second = lax.rem(first + size, size), lax.rem(second + size, size)
        return {
            "dap_0": jnp.where(core == 0, second, first),
            "dap_1": jnp.where(core == 0, first, second),
        }

    partner = {"dap_2": 1 - core}
    chips = size * size
    here = y * size + x
    away = lambda d: min(d, size - d)
    steps = [(dy, dx) for dy in range(size) for dx in range(size) if dy or dx]
    steps.sort(key=lambda d: (-away(d[0]), d[0], -away(d[1])))
    barrier = pltpu.get_barrier_semaphore()
    for dy, dx in steps:
        peer = {"dap_0": lax.rem(y + dy, size), "dap_1": lax.rem(x + dx, size)}
        pl.semaphore_signal(barrier, inc=1, device_id=peer, device_id_type=mesh)
    pl.semaphore_signal(barrier, inc=1, device_id=partner, device_id_type=mesh)
    for k in range(1, size):
        for peer in (device(main + k, side), device(main, side + k)):
            pl.semaphore_signal(
                barrier, inc=1, device_id={**peer, **partner}, device_id_type=mesh
            )
    own_rows = pltpu.make_async_copy(
        source_ref.at[:, here], landed.at[core, here], local_sem.at[2]
    )
    own_rows.start()
    loads = [
        pltpu.make_async_copy(a, b, load_sem.at[i])
        for i, (a, b) in enumerate(
            (
                (present_hbm, present_ref),
                (couple_hbm, couple_ref),
                (qk_hbm, qk_ref),
                (vg_hbm, vg_ref),
                (exit_hbm, exit_ref),
            )
        )
    ]
    for load in loads:
        load.start()
    pl.semaphore_wait(barrier, chips + 2 * (size - 1))
    for dy, dx in steps:
        row, column = lax.rem(y + dy, size), lax.rem(x + dx, size)
        pltpu.make_async_remote_copy(
            src_ref=source_ref.at[:, row * size + column], dst_ref=landed.at[core, here],
            send_sem=sent, recv_sem=got.at[dy], device_id={"dap_0": row, "dap_1": column},
            device_id_type=mesh,
        ).start()
    for load in loads:
        load.wait()

    half = seqs // 2
    order = one_hot(
        seqs, seqs,
        lambda o, k: k == ((o % half) // 2) * 4 + (o // half) * 2 + o % 2,
    )
    order = (order * chain_ref[...].astype(F32)).astype(BF16)
    present = present_ref[...].astype(F32).astype(BF16)
    live = jnp.dot(order, present, preferred_element_type=F32).astype(BF16)
    own_site = (chip(main, side) * 2 + core) * sites
    select = one_hot(8, residues, lambda o, j: j == own_site + o).astype(BF16)
    keep[...] = contract_lanes(select, live)

    head_of_lane = lax.broadcasted_iota(jnp.int32, (1, inner), 1) // HEAD_CHANNELS
    shift = jnp.sum(
        one_hot(channels, channels, lambda o, c: o == c) * shift_ref[...], axis=1, keepdims=True
    )

    wide[...] = couple_ref[...].astype(F32)
    blocks[...] = jnp.zeros_like(blocks)
    for e in range(OUTER_CHANNELS):
        rows = wide[pl.ds(e, OUTER_CHANNELS, stride=OUTER_CHANNELS), :].astype(BF16)
        for i in range(sites):
            row = e * pack + i * OUTER_CHANNELS
            blocks[row : row + OUTER_CHANNELS, i * PAIR_DIM : (i + 1) * PAIR_DIM] = rows
    def row_site(k):
        first = lax.rem(main + k // sites, size)
        at = jnp.where(core == 0, side * size + first, first * size + side)
        return (at * 2 + core) * sites + k % sites

    def column_site(k):
        second = lax.rem(side + k // chip_rows, size)
        at = jnp.where(core == 0, second * size + main, main * size + second)
        return at * chip_rows + k % chip_rows

    lanes = size * sites
    row_pick = one_hot(
        residues, 128, lambda j, k: (j == row_site(k)) & (k < lanes)
    ).astype(BF16)
    column_pick = one_hot(size * chip_rows, residues, lambda k, j: j == column_site(k)).astype(BF16)
    live_rows = jnp.dot(live, row_pick, preferred_element_type=F32).astype(BF16)
    live_columns = contract_lanes(column_pick, live).astype(BF16)
    counts = jnp.dot(live_columns, live_rows, preferred_element_type=F32).astype(BF16)
    spread = one_hot(128, size * pack, lambda k, l: k == l // OUTER_CHANNELS).astype(BF16)
    counts = jnp.dot(counts, spread, preferred_element_type=F32)
    inverse[...] = 1.0 / jnp.maximum(counts, 1.0)

    def row_of(which, dy, count):
        first = lax.rem(y - dy + size, size) * size
        return landed.at[which, pl.ds(first, count)]

    def cross(which, dy):
        ref = row_of(which, dy, size)
        return pltpu.make_async_remote_copy(
            src_ref=ref, dst_ref=ref, send_sem=crossed, recv_sem=cross_recv.at[dy],
            device_id=partner, device_id_type=mesh,
        )

    order_of_rows = sorted(range(size), key=lambda dy: (-away(dy), dy))
    own_rows.wait()
    for dy in order_of_rows:
        ref = row_of(core, dy, size if dy else size - 1)
        pltpu.make_async_copy(ref, ref, got.at[dy]).wait()
        cross(core, dy).start()

    span = OUTER_CHANNELS
    pick = one_hot(
        sites * span, 2 * sites * span,
        lambda o, k: k == (o % span) * (2 * sites) + core * sites + o // span,
    ).astype(BF16)
    band = 2 * sites * span

    def sort_rows(which):
        rows_in = landed[which].reshape(chips * 2 * 2 * sites, width)
        for b in range(half // span):
            rows = jnp.dot(
                pick, rows_in[band * b : band * (b + 1)], preferred_element_type=F32
            ).astype(BF16)
            for r in range(sites):
                first = pl.multiple_of(which * half + span * b, span)
                xs[r, pl.ds(first, span), :] = rows[span * r : span * (r + 1)]

    sort_rows(core)
    others = landed.at[core, pl.ds(0, chips - 1)]
    pltpu.make_async_copy(others, others, sent).wait()
    for dy in order_of_rows:
        cross(1 - core, dy).wait_recv()
    pltpu.make_async_copy(landed.at[core], landed.at[core], crossed).wait()
    sort_rows(1 - core)

    def remote(src, dst, send, recv, target):
        return pltpu.make_async_remote_copy(
            src_ref=src, dst_ref=dst, send_sem=sends.at[send], recv_sem=recv,
            device_id=target, device_id_type=mesh,
        )

    def index(offset):
        return offset % size

    around = [far, 3, -3, 2, -2, 1, -1]

    def left_to(r, offset):
        return remote(
            chunks.at[0, r], chunks.at[index(offset), r], 0,
            main_recv.at[r, index(offset)], device(main - offset, side),
        )

    def right_to(r, offset):
        return remote(
            columns.at[0, core, r], columns.at[index(offset), core, r], 1,
            side_recv.at[r, index(offset)], device(main, side - offset),
        )

    def right_across(r, offset, which):
        target = partner if offset == 0 else {**device(main - offset, side), **partner}
        return remote(
            columns.at[0, core, r], columns.at[index(offset), which, r], 2,
            swap_recv.at[r, index(offset)], target,
        )

    def launch(r):
        for offset in around:
            right_to(r, offset).start()
            right_across(r, offset, core).start()
        right_across(r, 0, core).start()
        for offset in around:
            left_to(r, offset).start()

    def arrive(offsets):
        for r in range(sites):
            for offset in offsets:
                right_across(r, offset, 1 - core).wait_recv()
                if offset:
                    right_to(r, offset).wait_recv()
                    left_to(r, offset).wait_recv()

    def one_site(r, carry):
        x = xs[r].astype(F32)
        normed = normalize(x, gain_ref[...], offset_ref[...])
        query_key = jnp.dot(normed, qk_ref[...], preferred_element_type=F32)
        value_gate = jnp.dot(normed, vg_ref[...], preferred_element_type=F32)
        query = (query_key[:, :inner] * HEAD_CHANNELS ** (-0.5)).astype(BF16)
        key = query_key[:, inner:].astype(BF16)
        value = value_gate[:, :inner].astype(BF16)
        gate = jax.nn.sigmoid(value_gate[:, inner:] + gate_ref[...])
        present_row = keep[pl.ds(r, 1), :]
        alive = present_row > 0
        mixed = jnp.zeros((seqs, inner), F32)
        for h in range(HEAD_COUNT):
            own = head_of_lane == h
            query_h = query * own.astype(F32).astype(BF16)
            scores = jnp.where(alive, contract_lanes(query_h, key), MASKED)
            exponent = jnp.exp(scores - jnp.max(scores, axis=-1, keepdims=True))
            weight = jnp.sum(exponent, axis=-1, keepdims=True)
            part = jnp.dot(exponent.astype(BF16), value, preferred_element_type=F32)
            mixed = jnp.where(own, part * (1.0 / weight), mixed)
        gated = (mixed * gate).astype(BF16)
        update = jnp.dot(gated, exit_ref[...], preferred_element_type=F32) + exit_add_ref[...]
        after = (x + update).astype(BF16)
        again = normalize(after.astype(F32), gain2_ref[...], offset2_ref[...])
        both = ((contract_lanes(twin_ref[...], again) + shift) * present_row).astype(BF16)
        chunks[0, r] = both[:OUTER_CHANNELS]
        columns[0, core, r] = both[OUTER_CHANNELS:]
        ys[r] = after

        launch(r)
        return carry

    lax.fori_loop(0, sites, one_site, 0)

    group = 2 * span
    place_back = one_hot(
        group * sites, group * sites,
        lambda o, k: k
        == (
            ((o % sites) * 2 + (o // (2 * sites)) % 2) * span
            + (o // (4 * sites)) * 2
            + (o // sites) % 2
        ),
    ).astype(BF16)
    for g in range(seqs // group):
        stack = jnp.concatenate(
            [
                ys[r, half * c + span * g : half * c + span * (g + 1), :]
                for r in range(sites)
                for c in range(2)
            ],
            axis=0,
        )
        rows = jnp.dot(place_back, stack, preferred_element_type=F32).astype(BF16)
        placed[group * g : group * (g + 1)] = rows.reshape(group, sites, width)

    after_copy = pltpu.make_async_copy(placed, after_ref, local_sem.at[0])
    after_copy.start()

    near = [0, -1, 1, -2, 2]
    quads = [(-2, 2), (-1, 1), (0, -3), (3, far)]
    batches = [[far, -3], [3, 2], [-2, 1, -1, 0]]
    ranks = sum(batches, [])
    turn = [0]

    def multiply(offset, q):
        members = [index(b) for b in quads[q]]
        quad = jnp.concatenate(
            [columns[b].reshape(chip_rows * OUTER_CHANNELS, seqs) for b in members], axis=0
        )
        left = chunks[index(offset)].reshape(pack, seqs)
        buffer = turn[0] % 2
        turn[0] += 1
        product = contract_lanes(quad, left)
        for j in range(2 * chip_rows):
            sums[buffer, PITCH * j : PITCH * j + OUTER_CHANNELS, :] = product[
                OUTER_CHANNELS * j : OUTER_CHANNELS * (j + 1)
            ]
        lanes = slice(pack * index(offset), pack * (index(offset) + 1))
        scale = jnp.concatenate(
            [inverse[chip_rows * b : chip_rows * (b + 1), lanes] for b in members], axis=0
        )
        first = ranks.index(offset) * size * chip_rows + 2 * chip_rows * q
        for e in range(OUTER_CHANNELS):
            rows = sums[buffer, pl.ds(e, 2 * chip_rows, stride=PITCH), :]
            terms[first : first + 2 * chip_rows, e * pack : (e + 1) * pack] = (
                rows * scale
            ).astype(BF16)

    def project(batch):
        count = size * chip_rows
        first = ranks.index(batches[batch][0])
        rows = slice(first * count, (first + len(batches[batch])) * count)
        result = jnp.dot(terms[rows, :], blocks[...], preferred_element_type=F32)
        for k in range(len(batches[batch])):
            for q, members in enumerate(quads):
                for t, b in enumerate(members):
                    row = k * count + (2 * q + t) * chip_rows
                    to = lax.rem(side + b + size, size) * chip_rows
                    to = pl.multiple_of((first + k) * count + to, chip_rows)
                    total[pl.ds(to, chip_rows), :] = result[row : row + chip_rows]
        for at in range(first, first + len(batches[batch])):
            for i in range(sites):
                part = total[at * count : (at + 1) * count, i * PAIR_DIM : (i + 1) * PAIR_DIM]
                part = (part + pair_shift_ref[...]).astype(BF16)
                stage[at, i] = part.reshape(size, chip_rows, PAIR_DIM)

    def deliver(batch):
        for offset in batches[batch]:
            src = stage.at[ranks.index(offset)]
            for c in range(2):

                @pl.when(core == c)
                def _():
                    dst = out_ref.at[:, :, main] if c == 0 else out_ref.at[:, main]
                    if offset:
                        remote(src, dst, 3, out_recv, device(main + offset, side)).start()
                    else:
                        pltpu.make_async_copy(src, dst, local_sem.at[1]).start()

    arrive(near)
    for q in (0, 1):
        for offset in near:
            multiply(offset, q)
    arrive((-3, 3, far))
    for batch in range(len(batches)):
        for offset in batches[batch]:
            for q in range(len(quads)):
                if q > 1 or offset not in near:
                    multiply(offset, q)
        project(batch)
        deliver(batch)

    for buffer, send in (
        (columns.at[pl.ds(0, size - 1), 0], 0),
        (columns.at[pl.ds(0, size - 1), 0], 1),
        (columns.at[:, 0], 2),
        (stage.at[pl.ds(0, size - 1)], 3),
    ):
        pltpu.make_async_copy(buffer, buffer, sends.at[send]).wait()
    arrived = stage.at[pl.ds(0, size - 1)]
    pltpu.make_async_copy(arrived, arrived, out_recv).wait()
    own = stage.at[ranks.index(0)]
    pltpu.make_async_copy(own, own, local_sem.at[1]).wait()
    after_copy.wait()


def attend_pairs(x, large, small, size):
    seqs, residues = large[0].shape
    part, _, width = x.shape
    chips = size * size
    chip_rows = residues // chips
    sites = chip_rows // 2
    pack = sites * OUTER_CHANNELS
    couple = large[-1]
    count = size * chip_rows
    x = x.reshape(part, chips, chip_rows, width)
    hbm = pl.BlockSpec(memory_space=pl.ANY)
    vmem = pl.BlockSpec(memory_space=pltpu.VMEM)
    dma = pltpu.SemaphoreType.DMA
    return pl.pallas_call(
        functools.partial(core_kernel, size),
        out_shape=(
            jax.ShapeDtypeStruct((seqs, sites, width), BF16),
            jax.ShapeDtypeStruct((sites, size, size, chip_rows, PAIR_DIM), BF16),
        ),
        in_specs=[hbm] * (1 + len(large)) + [vmem] * len(small),
        out_specs=(hbm, hbm),
        scratch_shapes=[
            pltpu.VMEM((2, chips, part, chip_rows, width), BF16),
            *[pltpu.VMEM(a.shape, a.dtype) for a in (large[0], *large[1:])],
            pltpu.VMEM((sites, seqs, width), BF16),
            pltpu.VMEM((sites, seqs, width), BF16),
            pltpu.VMEM((8, seqs), F32),
            pltpu.VMEM((count, size * pack), F32),
            pltpu.VMEM((size, sites, OUTER_CHANNELS, seqs), BF16),
            pltpu.VMEM((size, 2, sites, OUTER_CHANNELS, seqs), BF16),
            pltpu.VMEM((OUTER_CHANNELS * pack, sites * PAIR_DIM), BF16),
            pltpu.VMEM(couple.shape, F32),
            pltpu.VMEM((2, 2 * chip_rows * PITCH, pack), F32),
            pltpu.VMEM((size * count, OUTER_CHANNELS * pack), BF16),
            pltpu.VMEM((size * count, sites * PAIR_DIM), F32),
            pltpu.VMEM((size, sites, size, chip_rows, PAIR_DIM), BF16),
            pltpu.VMEM((seqs, sites, width), BF16),
            dma((sites, size + 1)),
            dma((sites, size + 1)),
            dma((sites, size)),
            dma,
            dma((4,)),
            dma((3,)),
            dma((5,)),
            dma((size,)),
            dma,
            dma,
            dma((size,)),
        ],
        compiler_params=pltpu.CompilerParams(
            vmem_limit_bytes=VMEM_LIMIT, collective_id=1, has_side_effects=True
        ),
        name="attend_pairs",
    )(x, *large, *small)


def hand_over_kernel(*refs):
    count = len(refs) // 4
    sources, targets, held = refs[:count], refs[count : 2 * count], refs[2 * count : 3 * count]
    into, out_of = refs[3 * count :][:2]
    pieces = []
    for source, target, room in zip(sources, targets, held):
        for k in range(4):
            rows = pl.ds(k * source.shape[0] // 4, source.shape[0] // 4)
            at = len(pieces)
            pieces.append(
                (
                    pltpu.make_async_copy(source.at[rows], room.at[rows], into.at[at]),
                    pltpu.make_async_copy(room.at[rows], target.at[rows], out_of.at[at]),
                )
            )
    for first, _ in pieces:
        first.start()
    for first, second in pieces:
        first.wait()
        second.start()
    for _, second in pieces:
        second.wait()


def hand_over(*arrays):
    hbm = pl.BlockSpec(memory_space=pl.ANY)
    return pl.pallas_call(
        hand_over_kernel,
        out_shape=tuple(jax.ShapeDtypeStruct(a.shape, a.dtype) for a in arrays),
        in_specs=[hbm] * len(arrays),
        out_specs=(hbm,) * len(arrays),
        scratch_shapes=[pltpu.VMEM(a.shape, a.dtype) for a in arrays]
        + [pltpu.SemaphoreType.DMA((4 * len(arrays),))] * 2,
        name="hand_over",
    )(*arrays)


def shards(
    homolog_stack_tensor,
    occupancy_indicator,
    chain_existence_flags,
    focus_normal_factor,
    focus_normal_addend,
    probe_index_weights,
    payload_valve_weights,
    logistic_valve_addend,
    focus_exit_weights,
    focus_exit_addend,
    product_mean_layer_stretch,
    product_mean_layer_shift,
    twin_map_matrix,
    twin_map_shift,
    couple_map_matrix,
    couple_map_shift,
):
    seqs, residues = occupancy_indicator.shape
    width = homolog_stack_tensor.shape[-1]
    size = lax.axis_size("dap_0")
    row = lambda v: v[None, :]
    after, pair_rows = attend_pairs(
        homolog_stack_tensor,
        (
            occupancy_indicator,
            probe_index_weights,
            payload_valve_weights,
            focus_exit_weights,
            couple_map_matrix,
        ),
        (
            row(chain_existence_flags),
            row(focus_normal_factor),
            row(focus_normal_addend),
            row(logistic_valve_addend),
            row(focus_exit_addend),
            row(product_mean_layer_stretch),
            row(product_mean_layer_shift),
            twin_map_matrix.T,
            row(twin_map_shift),
            row(couple_map_shift),
        ),
        size,
    )
    return hand_over(after, pair_rows.reshape(-1, residues, PAIR_DIM))


def solution(mesh):
    split = Mesh(
        mesh.devices.reshape(mesh.shape["grp"], 8, 8, 2), ("grp", "dap_0", "dap_1", "dap_2")
    )
    return jax.shard_map(
        shards,
        mesh=split,
        in_specs=(
            P(GRP_DAP, None, None),
            P("grp", None),
            P("grp"),
            P(),
            P(),
            P(),
            P(),
            P(),
            P(),
            P(),
            P(),
            P(),
            P(),
            P(),
            P(),
            P(),
        ),
        out_specs=(P("grp", DAP, None), P(GRP_DAP, None, None)),
        check_vma=False,
    )
```

```python
import functools

import jax
import jax.numpy as jnp
from jax import lax
from jax.experimental import pallas as pl
from jax.experimental.pallas import tpu as pltpu
from jax.sharding import Mesh
from jax.sharding import PartitionSpec as P

HEAD_COUNT = 8
HEAD_CHANNELS = 32
OUTER_CHANNELS = 32
PAIR_DIM = 128
DAP = ("dap_0", "dap_1", "dap_2")
GRP_DAP = ("grp", "dap_0", "dap_1", "dap_2")
F32 = jnp.float32
BF16 = jnp.bfloat16
VMEM_LIMIT = 60 * 1024 * 1024
PITCH = 40


EPSILON = 1e-05
MASKED = -100000.0


def normalize(widened, gain, offset):
    centred = widened - jnp.mean(widened, axis=-1, keepdims=True)
    variance = jnp.mean(centred * centred, axis=-1, keepdims=True)
    return (centred * lax.rsqrt(variance + EPSILON) * gain + offset).astype(BF16)


def contract_lanes(a, b):
    return lax.dot_general(a, b, (((1,), (1,)), ((), ())), preferred_element_type=F32)


def one_hot(rows, columns, test):
    row = lax.broadcasted_iota(jnp.int32, (rows, columns), 0)
    column = lax.broadcasted_iota(jnp.int32, (rows, columns), 1)
    return jnp.where(test(row, column), 1.0, 0.0)


def core_kernel(
    size, source_ref, present_hbm, qk_hbm, vg_hbm, exit_hbm, couple_hbm, chain_ref, gain_ref,
    offset_ref, gate_ref, exit_add_ref, gain2_ref, offset2_ref, twin_ref, shift_ref,
    pair_shift_ref,
    after_ref, out_ref,
    landed, present_ref, qk_ref, vg_ref, exit_ref, couple_ref, xs, ys, keep, inverse, chunks, columns, blocks, wide, sums, terms, total, stage, placed,
    main_recv, side_recv, swap_recv, out_recv, sends, local_sem, load_sem, got, sent, crossed,
):
    sites, seqs, width = xs.shape
    residues = present_ref.shape[1]
    pack = sites * OUTER_CHANNELS
    inner = HEAD_COUNT * HEAD_CHANNELS
    channels = 2 * OUTER_CHANNELS
    chip_rows = 2 * sites
    far = size // 2
    mesh = pl.DeviceIdType.MESH
    y, x, core = (lax.axis_index(a) for a in DAP)
    main = jnp.where(core == 0, x, y)
    side = jnp.where(core == 0, y, x)

    def chip(first, second):
        first, second = lax.rem(first + size, size), lax.rem(second + size, size)
        return jnp.where(core == 0, second * size + first, first * size + second)

    def device(first, second):
        first, second = lax.rem(first + size, size), lax.rem(second + size, size)
        return {
            "dap_0": jnp.where(core == 0, second, first),
            "dap_1": jnp.where(core == 0, first, second),
        }

    partner = {"dap_2": 1 - core}
    chips = size * size
    here = y * size + x
    away = lambda d: min(d, size - d)
    steps = [(dy, dx) for dy in range(size) for dx in range(size) if dy or dx]
    steps.sort(key=lambda d: -(away(d[0]) + away(d[1])))
    barrier = pltpu.get_barrier_semaphore()
    for dy, dx in steps:
        peer = {"dap_0": lax.rem(y + dy, size), "dap_1": lax.rem(x + dx, size)}
        pl.semaphore_signal(barrier, inc=1, device_id=peer, device_id_type=mesh)
    pl.semaphore_signal(barrier, inc=1, device_id=partner, device_id_type=mesh)
    own_rows = pltpu.make_async_copy(
        source_ref.at[:, here], landed.at[core, here], local_sem.at[2]
    )
    own_rows.start()
    loads = [
        pltpu.make_async_copy(a, b, load_sem.at[i])
        for i, (a, b) in enumerate(
            (
                (present_hbm, present_ref),
                (couple_hbm, couple_ref),
                (qk_hbm, qk_ref),
                (vg_hbm, vg_ref),
                (exit_hbm, exit_ref),
            )
        )
    ]
    for load in loads:
        load.start()
    pl.semaphore_wait(barrier, chips)
    for dy, dx in steps:
        row, column = lax.rem(y + dy, size), lax.rem(x + dx, size)
        pltpu.make_async_remote_copy(
            src_ref=source_ref.at[:, row * size + column], dst_ref=landed.at[core, here],
            send_sem=sent, recv_sem=got, device_id={"dap_0": row, "dap_1": column},
            device_id_type=mesh,
        ).start()
    for load in loads:
        load.wait()

    half = seqs // 2
    order = one_hot(
        seqs, seqs,
        lambda o, k: k == ((o % half) // 2) * 4 + (o // half) * 2 + o % 2,
    )
    order = (order * chain_ref[...].astype(F32)).astype(BF16)
    present = present_ref[...].astype(F32).astype(BF16)
    live = jnp.dot(order, present, preferred_element_type=F32).astype(BF16)
    own_site = (chip(main, side) * 2 + core) * sites
    select = one_hot(8, residues, lambda o, j: j == own_site + o).astype(BF16)
    keep[...] = contract_lanes(select, live)

    head_of_lane = lax.broadcasted_iota(jnp.int32, (1, inner), 1) // HEAD_CHANNELS
    shift = jnp.sum(
        one_hot(channels, channels, lambda o, c: o == c) * shift_ref[...], axis=1, keepdims=True
    )

    wide[...] = couple_ref[...].astype(F32)
    blocks[...] = jnp.zeros_like(blocks)
    for e in range(OUTER_CHANNELS):
        rows = wide[pl.ds(e, OUTER_CHANNELS, stride=OUTER_CHANNELS), :].astype(BF16)
        for i in range(sites):
            row = e * pack + i * OUTER_CHANNELS
            blocks[row : row + OUTER_CHANNELS, i * PAIR_DIM : (i + 1) * PAIR_DIM] = rows
    def row_site(k):
        first = lax.rem(main + k // sites, size)
        at = jnp.where(core == 0, side * size + first, first * size + side)
        return (at * 2 + core) * sites + k % sites

    def column_site(k):
        second = lax.rem(side + k // chip_rows, size)
        at = jnp.where(core == 0, second * size + main, main * size + second)
        return at * chip_rows + k % chip_rows

    lanes = size * sites
    row_pick = one_hot(
        residues, 128, lambda j, k: (j == row_site(k)) & (k < lanes)
    ).astype(BF16)
    column_pick = one_hot(size * chip_rows, residues, lambda k, j: j == column_site(k)).astype(BF16)
    live_rows = jnp.dot(live, row_pick, preferred_element_type=F32).astype(BF16)
    live_columns = contract_lanes(column_pick, live).astype(BF16)
    counts = jnp.dot(live_columns, live_rows, preferred_element_type=F32).astype(BF16)
    spread = one_hot(128, size * pack, lambda k, l: k == l // OUTER_CHANNELS).astype(BF16)
    counts = jnp.dot(counts, spread, preferred_element_type=F32)
    inverse[...] = 1.0 / jnp.maximum(counts, 1.0)

    others = landed.at[core, pl.ds(0, chips - 1)]
    own_rows.wait()
    pltpu.make_async_copy(others, others, got).wait()
    cross = pltpu.make_async_remote_copy(
        src_ref=landed.at[core], dst_ref=landed.at[core], send_sem=crossed.at[0],
        recv_sem=crossed.at[1], device_id=partner, device_id_type=mesh,
    )
    cross.start()

    span = OUTER_CHANNELS
    pick = one_hot(
        sites * span, 2 * sites * span,
        lambda o, k: k == (o % span) * (2 * sites) + core * sites + o // span,
    ).astype(BF16)
    band = 2 * sites * span

    def sort_rows(which):
        rows_in = landed[which].reshape(chips * 2 * 2 * sites, width)
        for b in range(half // span):
            rows = jnp.dot(
                pick, rows_in[band * b : band * (b + 1)], preferred_element_type=F32
            ).astype(BF16)
            for r in range(sites):
                first = pl.multiple_of(which * half + span * b, span)
                xs[r, pl.ds(first, span), :] = rows[span * r : span * (r + 1)]

    sort_rows(core)
    pltpu.make_async_copy(others, others, sent).wait()
    cross.wait()
    sort_rows(1 - core)

    def remote(src, dst, send, recv, target):
        return pltpu.make_async_remote_copy(
            src_ref=src, dst_ref=dst, send_sem=sends.at[send], recv_sem=recv,
            device_id=target, device_id_type=mesh,
        )

    def index(offset):
        return offset % size

    def hop(r, way, origin, sign, step, cross=False):
        reach = origin - sign * step
        if way == 0:
            ref = lambda offset: chunks.at[index(offset), r]
            target = device(main + sign * step, side)
        else:
            which = core if way == 1 or cross else 1 - core
            ref = lambda offset: columns.at[index(offset), which, r]
            target = device(main, side + sign * step)
            if cross:
                target = {**device(main + sign * step, side), **partner}
        src, dst = ref(origin), ref(reach)
        where = index(reach)
        if abs(reach) == far:
            rows = OUTER_CHANNELS // 2
            first = pl.ds(0 if sign > 0 else rows, rows)
            src, dst = src.at[first], dst.at[first]
            where = far if sign > 0 else size
        return remote(src, dst, way, (main_recv, side_recv, swap_recv)[way].at[r, where], target)

    def swap(r, which):
        ref = columns.at[0, which, r]
        return remote(ref, ref, 2, swap_recv.at[r, 0], partner)

    def launch(r):
        for step in (2, 1):
            for sign in (1, -1):
                hop(r, 1, 0, sign, step).start()
                hop(r, 2, 0, sign, step, True).start()
        swap(r, core).start()
        for step in (2, 1):
            for sign in (1, -1):
                hop(r, 0, 0, sign, step).start()

    def relay(r):
        for way in (1, 2, 0):
            for sign in (1, -1):
                hop(r, way, 0, sign, 2).wait_recv()
                hop(r, way, -2 * sign, sign, 2).start()
                hop(r, way, -2 * sign, sign, 1).start()

    def arrive_near(r):
        swap(r, 1 - core).wait_recv()
        for way in (1, 2, 0):
            for sign in (1, -1):
                hop(r, way, 0, sign, 1).wait_recv()

    def arrive_far(r):
        for way in (1, 2, 0):
            for step in (1, 2):
                for sign in (1, -1):
                    hop(r, way, -2 * sign, sign, step).wait_recv()

    def one_site(r, carry):
        x = xs[r].astype(F32)
        normed = normalize(x, gain_ref[...], offset_ref[...])
        query_key = jnp.dot(normed, qk_ref[...], preferred_element_type=F32)
        value_gate = jnp.dot(normed, vg_ref[...], preferred_element_type=F32)
        query = (query_key[:, :inner] * HEAD_CHANNELS ** (-0.5)).astype(BF16)
        key = query_key[:, inner:].astype(BF16)
        value = value_gate[:, :inner].astype(BF16)
        gate = jax.nn.sigmoid(value_gate[:, inner:] + gate_ref[...])
        present_row = keep[pl.ds(r, 1), :]
        alive = present_row > 0
        mixed = jnp.zeros((seqs, inner), F32)
        for h in range(HEAD_COUNT):
            own = head_of_lane == h
            query_h = query * own.astype(F32).astype(BF16)
            scores = jnp.where(alive, contract_lanes(query_h, key), MASKED)
            exponent = jnp.exp(scores - jnp.max(scores, axis=-1, keepdims=True))
            weight = jnp.sum(exponent, axis=-1, keepdims=True)
            part = jnp.dot(exponent.astype(BF16), value, preferred_element_type=F32)
            mixed = jnp.where(own, part * (1.0 / weight), mixed)
        gated = (mixed * gate).astype(BF16)
        update = jnp.dot(gated, exit_ref[...], preferred_element_type=F32) + exit_add_ref[...]
        after = (x + update).astype(BF16)
        again = normalize(after.astype(F32), gain2_ref[...], offset2_ref[...])
        both = ((contract_lanes(twin_ref[...], again) + shift) * present_row).astype(BF16)
        chunks[0, r] = both[:OUTER_CHANNELS]
        columns[0, core, r] = both[OUTER_CHANNELS:]
        ys[r] = after

        launch(r)

        @pl.when(r >= 2)
        def _():
            relay(r - 2)

        return carry

    lax.fori_loop(0, sites, one_site, 0)

    group = 2 * span
    place_back = one_hot(
        group * sites, group * sites,
        lambda o, k: k
        == (
            ((o % sites) * 2 + (o // (2 * sites)) % 2) * span
            + (o // (4 * sites)) * 2
            + (o // sites) % 2
        ),
    ).astype(BF16)
    for g in range(seqs // group):
        stack = jnp.concatenate(
            [
                ys[r, half * c + span * g : half * c + span * (g + 1), :]
                for r in range(sites)
                for c in range(2)
            ],
            axis=0,
        )
        rows = jnp.dot(place_back, stack, preferred_element_type=F32).astype(BF16)
        placed[group * g : group * (g + 1)] = rows.reshape(group, sites, width)

    relay(sites - 2)
    after_copy = pltpu.make_async_copy(placed, after_ref, local_sem.at[0])
    after_copy.start()
    relay(sites - 1)

    near = [0, -1, 1, -2, 2]
    quads = [(-2, 2), (-1, 1), (0, -3), (3, far)]
    batches = [[far, -3], [3, 2], [-2, 1, -1, 0]]
    ranks = sum(batches, [])
    turn = [0]

    def multiply(offset, q):
        members = [index(b) for b in quads[q]]
        quad = jnp.concatenate(
            [columns[b].reshape(chip_rows * OUTER_CHANNELS, seqs) for b in members], axis=0
        )
        left = chunks[index(offset)].reshape(pack, seqs)
        buffer = turn[0] % 2
        turn[0] += 1
        product = contract_lanes(quad, left)
        for j in range(2 * chip_rows):
            sums[buffer, PITCH * j : PITCH * j + OUTER_CHANNELS, :] = product[
                OUTER_CHANNELS * j : OUTER_CHANNELS * (j + 1)
            ]
        lanes = slice(pack * index(offset), pack * (index(offset) + 1))
        scale = jnp.concatenate(
            [inverse[chip_rows * b : chip_rows * (b + 1), lanes] for b in members], axis=0
        )
        first = ranks.index(offset) * size * chip_rows + 2 * chip_rows * q
        for e in range(OUTER_CHANNELS):
            rows = sums[buffer, pl.ds(e, 2 * chip_rows, stride=PITCH), :]
            terms[first : first + 2 * chip_rows, e * pack : (e + 1) * pack] = (
                rows * scale
            ).astype(BF16)

    def project(batch):
        count = size * chip_rows
        first = ranks.index(batches[batch][0])
        rows = slice(first * count, (first + len(batches[batch])) * count)
        result = jnp.dot(terms[rows, :], blocks[...], preferred_element_type=F32)
        for k in range(len(batches[batch])):
            for q, members in enumerate(quads):
                for t, b in enumerate(members):
                    row = k * count + (2 * q + t) * chip_rows
                    to = lax.rem(side + b + size, size) * chip_rows
                    to = pl.multiple_of((first + k) * count + to, chip_rows)
                    total[pl.ds(to, chip_rows), :] = result[row : row + chip_rows]
        for at in range(first, first + len(batches[batch])):
            for i in range(sites):
                part = total[at * count : (at + 1) * count, i * PAIR_DIM : (i + 1) * PAIR_DIM]
                part = (part + pair_shift_ref[...]).astype(BF16)
                stage[at, i] = part.reshape(size, chip_rows, PAIR_DIM)

    def deliver(batch):
        for offset in batches[batch]:
            src = stage.at[ranks.index(offset)]
            for c in range(2):

                @pl.when(core == c)
                def _():
                    dst = out_ref.at[:, :, main] if c == 0 else out_ref.at[:, main]
                    if offset:
                        remote(src, dst, 3, out_recv, device(main + offset, side)).start()
                    else:
                        pltpu.make_async_copy(src, dst, local_sem.at[1]).start()

    for r in range(sites):
        arrive_near(r)
    for q in (0, 1):
        for offset in near:
            multiply(offset, q)
    for r in range(sites):
        arrive_far(r)
    for batch in range(len(batches)):
        for offset in batches[batch]:
            for q in range(len(quads)):
                if q > 1 or offset not in near:
                    multiply(offset, q)
        project(batch)
        deliver(batch)

    for buffer, send in (
        (columns.at[pl.ds(0, size - 1), 0], 0),
        (columns.at[pl.ds(0, size - 1), 0], 1),
        (columns.at[:, 0], 2),
        (stage.at[pl.ds(0, size - 1)], 3),
    ):
        pltpu.make_async_copy(buffer, buffer, sends.at[send]).wait()
    arrived = stage.at[pl.ds(0, size - 1)]
    pltpu.make_async_copy(arrived, arrived, out_recv).wait()
    own = stage.at[ranks.index(0)]
    pltpu.make_async_copy(own, own, local_sem.at[1]).wait()
    after_copy.wait()


def attend_pairs(x, large, small, size):
    seqs, residues = large[0].shape
    part, _, width = x.shape
    chips = size * size
    chip_rows = residues // chips
    sites = chip_rows // 2
    pack = sites * OUTER_CHANNELS
    couple = large[-1]
    count = size * chip_rows
    x = x.reshape(part, chips, chip_rows, width)
    hbm = pl.BlockSpec(memory_space=pl.ANY)
    vmem = pl.BlockSpec(memory_space=pltpu.VMEM)
    dma = pltpu.SemaphoreType.DMA
    return pl.pallas_call(
        functools.partial(core_kernel, size),
        out_shape=(
            jax.ShapeDtypeStruct((seqs, sites, width), BF16),
            jax.ShapeDtypeStruct((sites, size, size, chip_rows, PAIR_DIM), BF16),
        ),
        in_specs=[hbm] * (1 + len(large)) + [vmem] * len(small),
        out_specs=(hbm, hbm),
        scratch_shapes=[
            pltpu.VMEM((2, chips, part, chip_rows, width), BF16),
            *[pltpu.VMEM(a.shape, a.dtype) for a in (large[0], *large[1:])],
            pltpu.VMEM((sites, seqs, width), BF16),
            pltpu.VMEM((sites, seqs, width), BF16),
            pltpu.VMEM((8, seqs), F32),
            pltpu.VMEM((count, size * pack), F32),
            pltpu.VMEM((size, sites, OUTER_CHANNELS, seqs), BF16),
            pltpu.VMEM((size, 2, sites, OUTER_CHANNELS, seqs), BF16),
            pltpu.VMEM((OUTER_CHANNELS * pack, sites * PAIR_DIM), BF16),
            pltpu.VMEM(couple.shape, F32),
            pltpu.VMEM((2, 2 * chip_rows * PITCH, pack), F32),
            pltpu.VMEM((size * count, OUTER_CHANNELS * pack), BF16),
            pltpu.VMEM((size * count, sites * PAIR_DIM), F32),
            pltpu.VMEM((size, sites, size, chip_rows, PAIR_DIM), BF16),
            pltpu.VMEM((seqs, sites, width), BF16),
            dma((sites, size + 1)),
            dma((sites, size + 1)),
            dma((sites, size + 1)),
            dma,
            dma((4,)),
            dma((3,)),
            dma((5,)),
            dma,
            dma,
            dma((2,)),
        ],
        compiler_params=pltpu.CompilerParams(
            vmem_limit_bytes=VMEM_LIMIT, collective_id=1, has_side_effects=True
        ),
        name="attend_pairs",
    )(x, *large, *small)


def hand_over_kernel(*refs):
    count = len(refs) // 4
    sources, targets, held = refs[:count], refs[count : 2 * count], refs[2 * count : 3 * count]
    into, out_of = refs[3 * count :][:2]
    pieces = []
    for source, target, room in zip(sources, targets, held):
        for k in range(4):
            rows = pl.ds(k * source.shape[0] // 4, source.shape[0] // 4)
            at = len(pieces)
            pieces.append(
                (
                    pltpu.make_async_copy(source.at[rows], room.at[rows], into.at[at]),
                    pltpu.make_async_copy(room.at[rows], target.at[rows], out_of.at[at]),
                )
            )
    for first, _ in pieces:
        first.start()
    for first, second in pieces:
        first.wait()
        second.start()
    for _, second in pieces:
        second.wait()


def hand_over(*arrays):
    hbm = pl.BlockSpec(memory_space=pl.ANY)
    return pl.pallas_call(
        hand_over_kernel,
        out_shape=tuple(jax.ShapeDtypeStruct(a.shape, a.dtype) for a in arrays),
        in_specs=[hbm] * len(arrays),
        out_specs=(hbm,) * len(arrays),
        scratch_shapes=[pltpu.VMEM(a.shape, a.dtype) for a in arrays]
        + [pltpu.SemaphoreType.DMA((4 * len(arrays),))] * 2,
        name="hand_over",
    )(*arrays)


def shards(
    homolog_stack_tensor,
    occupancy_indicator,
    chain_existence_flags,
    focus_normal_factor,
    focus_normal_addend,
    probe_index_weights,
    payload_valve_weights,
    logistic_valve_addend,
    focus_exit_weights,
    focus_exit_addend,
    product_mean_layer_stretch,
    product_mean_layer_shift,
    twin_map_matrix,
    twin_map_shift,
    couple_map_matrix,
    couple_map_shift,
):
    seqs, residues = occupancy_indicator.shape
    width = homolog_stack_tensor.shape[-1]
    size = lax.axis_size("dap_0")
    row = lambda v: v[None, :]
    after, pair_rows = attend_pairs(
        homolog_stack_tensor,
        (
            occupancy_indicator,
            probe_index_weights,
            payload_valve_weights,
            focus_exit_weights,
            couple_map_matrix,
        ),
        (
            row(chain_existence_flags),
            row(focus_normal_factor),
            row(focus_normal_addend),
            row(logistic_valve_addend),
            row(focus_exit_addend),
            row(product_mean_layer_stretch),
            row(product_mean_layer_shift),
            twin_map_matrix.T,
            row(twin_map_shift),
            row(couple_map_shift),
        ),
        size,
    )
    return hand_over(after, pair_rows.reshape(-1, residues, PAIR_DIM))


def solution(mesh):
    split = Mesh(
        mesh.devices.reshape(mesh.shape["grp"], 8, 8, 2), ("grp", "dap_0", "dap_1", "dap_2")
    )
    return jax.shard_map(
        shards,
        mesh=split,
        in_specs=(
            P(GRP_DAP, None, None),
            P("grp", None),
            P("grp"),
            P(),
            P(),
            P(),
            P(),
            P(),
            P(),
            P(),
            P(),
            P(),
            P(),
            P(),
            P(),
            P(),
        ),
        out_specs=(P("grp", DAP, None), P(GRP_DAP, None, None)),
        check_vma=False,
    )
```

```python
import functools

import jax
import jax.numpy as jnp
from jax import lax
from jax.experimental import pallas as pl
from jax.experimental.pallas import tpu as pltpu
from jax.sharding import Mesh
from jax.sharding import PartitionSpec as P

HEAD_COUNT = 8
HEAD_CHANNELS = 32
OUTER_CHANNELS = 32
PAIR_DIM = 128
DAP = ("dap_0", "dap_1", "dap_2")
GRP_DAP = ("grp", "dap_0", "dap_1", "dap_2")
F32 = jnp.float32
BF16 = jnp.bfloat16
VMEM_LIMIT = 60 * 1024 * 1024
PITCH = 40


EPSILON = 1e-05
MASKED = -100000.0


def normalize(widened, gain, offset):
    centred = widened - jnp.mean(widened, axis=-1, keepdims=True)
    variance = jnp.mean(centred * centred, axis=-1, keepdims=True)
    return (centred * lax.rsqrt(variance + EPSILON) * gain + offset).astype(BF16)


def contract_lanes(a, b):
    return lax.dot_general(a, b, (((1,), (1,)), ((), ())), preferred_element_type=F32)


def one_hot(rows, columns, test):
    row = lax.broadcasted_iota(jnp.int32, (rows, columns), 0)
    column = lax.broadcasted_iota(jnp.int32, (rows, columns), 1)
    return jnp.where(test(row, column), 1.0, 0.0)


def core_kernel(
    size, source_ref, present_hbm, qk_hbm, vg_hbm, exit_hbm, couple_hbm, chain_ref, gain_ref,
    offset_ref, gate_ref, exit_add_ref, gain2_ref, offset2_ref, twin_ref, shift_ref,
    pair_shift_ref,
    after_ref, out_ref,
    source, landed, present_ref, qk_ref, vg_ref, exit_ref, couple_ref, xs, ys, keep, inverse, chunks, columns, blocks, wide, sums, terms, total, stage, placed,
    main_recv, side_recv, swap_recv, out_recv, sends, local_sem, load_sem, got, sent, crossed,
):
    sites, seqs, width = xs.shape
    residues = present_ref.shape[1]
    pack = sites * OUTER_CHANNELS
    inner = HEAD_COUNT * HEAD_CHANNELS
    channels = 2 * OUTER_CHANNELS
    chip_rows = 2 * sites
    far = size // 2
    mesh = pl.DeviceIdType.MESH
    y, x, core = (lax.axis_index(a) for a in DAP)
    main = jnp.where(core == 0, x, y)
    side = jnp.where(core == 0, y, x)

    def chip(first, second):
        first, second = lax.rem(first + size, size), lax.rem(second + size, size)
        return jnp.where(core == 0, second * size + first, first * size + second)

    def device(first, second):
        first, second = lax.rem(first + size, size), lax.rem(second + size, size)
        return {
            "dap_0": jnp.where(core == 0, second, first),
            "dap_1": jnp.where(core == 0, first, second),
        }

    partner = {"dap_2": 1 - core}
    chips = size * size
    here = y * size + x
    away = lambda d: min(d, size - d)
    steps = [(dy, dx) for dy in range(size) for dx in range(size) if dy or dx]
    steps.sort(key=lambda d: -(away(d[0]) + away(d[1])))
    barrier = pltpu.get_barrier_semaphore()
    for dy, dx in steps:
        peer = {"dap_0": lax.rem(y + dy, size), "dap_1": lax.rem(x + dx, size)}
        pl.semaphore_signal(barrier, inc=1, device_id=peer, device_id_type=mesh)
    pl.semaphore_signal(barrier, inc=1, device_id=partner, device_id_type=mesh)
    own_rows = pltpu.make_async_copy(
        source_ref.at[:, here], landed.at[core, here], local_sem.at[2]
    )
    own_rows.start()
    loads = [
        pltpu.make_async_copy(a, b, load_sem.at[i])
        for i, (a, b) in enumerate(
            (
                (source_ref, source),
                (present_hbm, present_ref),
                (couple_hbm, couple_ref),
                (qk_hbm, qk_ref),
                (vg_hbm, vg_ref),
                (exit_hbm, exit_ref),
            )
        )
    ]
    for load in loads:
        load.start()
    pl.semaphore_wait(barrier, chips)
    loads[0].wait()
    for dy, dx in steps:
        row, column = lax.rem(y + dy, size), lax.rem(x + dx, size)
        pltpu.make_async_remote_copy(
            src_ref=source.at[:, row * size + column], dst_ref=landed.at[core, here],
            send_sem=sent, recv_sem=got, device_id={"dap_0": row, "dap_1": column},
            device_id_type=mesh,
        ).start()
    for load in loads[1:]:
        load.wait()

    half = seqs // 2
    order = one_hot(
        seqs, seqs,
        lambda o, k: k == ((o % half) // 2) * 4 + (o // half) * 2 + o % 2,
    )
    order = (order * chain_ref[...].astype(F32)).astype(BF16)
    present = present_ref[...].astype(F32).astype(BF16)
    live = jnp.dot(order, present, preferred_element_type=F32).astype(BF16)
    own_site = (chip(main, side) * 2 + core) * sites
    select = one_hot(8, residues, lambda o, j: j == own_site + o).astype(BF16)
    keep[...] = contract_lanes(select, live)

    head_of_lane = lax.broadcasted_iota(jnp.int32, (1, inner), 1) // HEAD_CHANNELS
    shift = jnp.sum(
        one_hot(channels, channels, lambda o, c: o == c) * shift_ref[...], axis=1, keepdims=True
    )

    wide[...] = couple_ref[...].astype(F32)
    blocks[...] = jnp.zeros_like(blocks)
    for e in range(OUTER_CHANNELS):
        rows = wide[pl.ds(e, OUTER_CHANNELS, stride=OUTER_CHANNELS), :].astype(BF16)
        for i in range(sites):
            row = e * pack + i * OUTER_CHANNELS
            blocks[row : row + OUTER_CHANNELS, i * PAIR_DIM : (i + 1) * PAIR_DIM] = rows
    def row_site(k):
        first = lax.rem(main + k // sites, size)
        at = jnp.where(core == 0, side * size + first, first * size + side)
        return (at * 2 + core) * sites + k % sites

    def column_site(k):
        second = lax.rem(side + k // chip_rows, size)
        at = jnp.where(core == 0, second * size + main, main * size + second)
        return at * chip_rows + k % chip_rows

    lanes = size * sites
    row_pick = one_hot(
        residues, 128, lambda j, k: (j == row_site(k)) & (k < lanes)
    ).astype(BF16)
    column_pick = one_hot(size * chip_rows, residues, lambda k, j: j == column_site(k)).astype(BF16)
    live_rows = jnp.dot(live, row_pick, preferred_element_type=F32).astype(BF16)
    live_columns = contract_lanes(column_pick, live).astype(BF16)
    counts = jnp.dot(live_columns, live_rows, preferred_element_type=F32).astype(BF16)
    spread = one_hot(128, size * pack, lambda k, l: k == l // OUTER_CHANNELS).astype(BF16)
    counts = jnp.dot(counts, spread, preferred_element_type=F32)
    inverse[...] = 1.0 / jnp.maximum(counts, 1.0)

    others = landed.at[core, pl.ds(0, chips - 1)]
    own_rows.wait()
    pltpu.make_async_copy(others, others, got).wait()
    cross = pltpu.make_async_remote_copy(
        src_ref=landed.at[core], dst_ref=landed.at[core], send_sem=crossed.at[0],
        recv_sem=crossed.at[1], device_id=partner, device_id_type=mesh,
    )
    cross.start()

    span = OUTER_CHANNELS
    pick = one_hot(
        sites * span, 2 * sites * span,
        lambda o, k: k == (o % span) * (2 * sites) + core * sites + o // span,
    ).astype(BF16)
    band = 2 * sites * span

    def sort_rows(which):
        rows_in = landed[which].reshape(chips * 2 * 2 * sites, width)
        for b in range(half // span):
            rows = jnp.dot(
                pick, rows_in[band * b : band * (b + 1)], preferred_element_type=F32
            ).astype(BF16)
            for r in range(sites):
                first = pl.multiple_of(which * half + span * b, span)
                xs[r, pl.ds(first, span), :] = rows[span * r : span * (r + 1)]

    sort_rows(core)
    pltpu.make_async_copy(others, others, sent).wait()
    cross.wait()
    sort_rows(1 - core)

    def remote(src, dst, send, recv, target):
        return pltpu.make_async_remote_copy(
            src_ref=src, dst_ref=dst, send_sem=sends.at[send], recv_sem=recv,
            device_id=target, device_id_type=mesh,
        )

    def index(offset):
        return offset % size

    def hop(r, way, origin, sign, step, cross=False):
        reach = origin - sign * step
        if way == 0:
            ref = lambda offset: chunks.at[index(offset), r]
            target = device(main + sign * step, side)
        else:
            which = core if way == 1 or cross else 1 - core
            ref = lambda offset: columns.at[index(offset), which, r]
            target = device(main, side + sign * step)
            if cross:
                target = {**device(main + sign * step, side), **partner}
        src, dst = ref(origin), ref(reach)
        where = index(reach)
        if abs(reach) == far:
            rows = OUTER_CHANNELS // 2
            first = pl.ds(0 if sign > 0 else rows, rows)
            src, dst = src.at[first], dst.at[first]
            where = far if sign > 0 else size
        return remote(src, dst, way, (main_recv, side_recv, swap_recv)[way].at[r, where], target)

    def swap(r, which):
        ref = columns.at[0, which, r]
        return remote(ref, ref, 2, swap_recv.at[r, 0], partner)

    def launch(r):
        for step in (2, 1):
            for sign in (1, -1):
                hop(r, 1, 0, sign, step).start()
                hop(r, 2, 0, sign, step, True).start()
        swap(r, core).start()
        for step in (2, 1):
            for sign in (1, -1):
                hop(r, 0, 0, sign, step).start()

    def relay(r):
        for way in (1, 2, 0):
            for sign in (1, -1):
                hop(r, way, 0, sign, 2).wait_recv()
                hop(r, way, -2 * sign, sign, 2).start()
                hop(r, way, -2 * sign, sign, 1).start()

    def arrive_near(r):
        swap(r, 1 - core).wait_recv()
        for way in (1, 2, 0):
            for sign in (1, -1):
                hop(r, way, 0, sign, 1).wait_recv()

    def arrive_far(r):
        for way in (1, 2, 0):
            for step in (1, 2):
                for sign in (1, -1):
                    hop(r, way, -2 * sign, sign, step).wait_recv()

    def one_site(r, carry):
        x = xs[r].astype(F32)
        normed = normalize(x, gain_ref[...], offset_ref[...])
        query_key = jnp.dot(normed, qk_ref[...], preferred_element_type=F32)
        value_gate = jnp.dot(normed, vg_ref[...], preferred_element_type=F32)
        query = (query_key[:, :inner] * HEAD_CHANNELS ** (-0.5)).astype(BF16)
        key = query_key[:, inner:].astype(BF16)
        value = value_gate[:, :inner].astype(BF16)
        gate = jax.nn.sigmoid(value_gate[:, inner:] + gate_ref[...])
        present_row = keep[pl.ds(r, 1), :]
        alive = present_row > 0
        mixed = jnp.zeros((seqs, inner), F32)
        for h in range(HEAD_COUNT):
            own = head_of_lane == h
            query_h = query * own.astype(F32).astype(BF16)
            scores = jnp.where(alive, contract_lanes(query_h, key), MASKED)
            exponent = jnp.exp(scores - jnp.max(scores, axis=-1, keepdims=True))
            weight = jnp.sum(exponent, axis=-1, keepdims=True)
            part = jnp.dot(exponent.astype(BF16), value, preferred_element_type=F32)
            mixed = jnp.where(own, part * (1.0 / weight), mixed)
        gated = (mixed * gate).astype(BF16)
        update = jnp.dot(gated, exit_ref[...], preferred_element_type=F32) + exit_add_ref[...]
        after = (x + update).astype(BF16)
        again = normalize(after.astype(F32), gain2_ref[...], offset2_ref[...])
        both = ((contract_lanes(twin_ref[...], again) + shift) * present_row).astype(BF16)
        chunks[0, r] = both[:OUTER_CHANNELS]
        columns[0, core, r] = both[OUTER_CHANNELS:]
        ys[r] = after

        launch(r)

        @pl.when(r >= 2)
        def _():
            relay(r - 2)

        return carry

    lax.fori_loop(0, sites, one_site, 0)

    group = 2 * span
    place_back = one_hot(
        group * sites, group * sites,
        lambda o, k: k
        == (
            ((o % sites) * 2 + (o // (2 * sites)) % 2) * span
            + (o // (4 * sites)) * 2
            + (o // sites) % 2
        ),
    ).astype(BF16)
    for g in range(seqs // group):
        stack = jnp.concatenate(
            [
                ys[r, half * c + span * g : half * c + span * (g + 1), :]
                for r in range(sites)
                for c in range(2)
            ],
            axis=0,
        )
        rows = jnp.dot(place_back, stack, preferred_element_type=F32).astype(BF16)
        placed[group * g : group * (g + 1)] = rows.reshape(group, sites, width)

    relay(sites - 2)
    after_copy = pltpu.make_async_copy(placed, after_ref, local_sem.at[0])
    after_copy.start()
    relay(sites - 1)

    near = [0, -1, 1, -2, 2]
    quads = [(-2, 2), (-1, 1), (0, -3), (3, far)]
    batches = [[far, -3], [3, 2], [-2, 1, -1, 0]]
    ranks = sum(batches, [])
    turn = [0]

    def multiply(pair, q):
        members = [index(b) for b in quads[q]]
        quad = jnp.concatenate(
            [columns[b].reshape(chip_rows * OUTER_CHANNELS, seqs) for b in members], axis=0
        )
        left = jnp.concatenate([chunks[index(o)].reshape(pack, seqs) for o in pair], axis=0)
        product = contract_lanes(quad, left)
        turn[0] += 1
        for k, offset in enumerate(pair):
            buffer = 2 * (turn[0] % 2) + k
            for j in range(2 * chip_rows):
                sums[buffer, PITCH * j : PITCH * j + OUTER_CHANNELS, :] = product[
                    OUTER_CHANNELS * j : OUTER_CHANNELS * (j + 1), pack * k : pack * (k + 1)
                ]
            lanes = slice(pack * index(offset), pack * (index(offset) + 1))
            scale = jnp.concatenate(
                [inverse[chip_rows * b : chip_rows * (b + 1), lanes] for b in members], axis=0
            )
            first = ranks.index(offset) * size * chip_rows + 2 * chip_rows * q
            for e in range(OUTER_CHANNELS):
                rows = sums[buffer, pl.ds(e, 2 * chip_rows, stride=PITCH), :]
                terms[first : first + 2 * chip_rows, e * pack : (e + 1) * pack] = (
                    rows * scale
                ).astype(BF16)

    def project(batch):
        count = size * chip_rows
        first = ranks.index(batches[batch][0])
        rows = slice(first * count, (first + len(batches[batch])) * count)
        result = jnp.dot(terms[rows, :], blocks[...], preferred_element_type=F32)
        for k in range(len(batches[batch])):
            for q, members in enumerate(quads):
                for t, b in enumerate(members):
                    row = k * count + (2 * q + t) * chip_rows
                    to = lax.rem(side + b + size, size) * chip_rows
                    to = pl.multiple_of((first + k) * count + to, chip_rows)
                    total[pl.ds(to, chip_rows), :] = result[row : row + chip_rows]
        for at in range(first, first + len(batches[batch])):
            for i in range(sites):
                part = total[at * count : (at + 1) * count, i * PAIR_DIM : (i + 1) * PAIR_DIM]
                part = (part + pair_shift_ref[...]).astype(BF16)
                stage[at, i] = part.reshape(size, chip_rows, PAIR_DIM)

    def deliver(batch):
        for offset in batches[batch]:
            src = stage.at[ranks.index(offset)]
            for c in range(2):

                @pl.when(core == c)
                def _():
                    dst = out_ref.at[:, :, main] if c == 0 else out_ref.at[:, main]
                    if offset:
                        remote(src, dst, 3, out_recv, device(main + offset, side)).start()
                    else:
                        pltpu.make_async_copy(src, dst, local_sem.at[1]).start()

    for r in range(sites):
        arrive_near(r)
    pairs = [tuple(batch[k : k + 2]) for batch in batches for k in range(0, len(batch), 2)]
    early = [pair for pair in pairs if all(offset in near for offset in pair)]
    for q in (0, 1):
        for pair in early:
            multiply(pair, q)
    for r in range(sites):
        arrive_far(r)
    for batch in range(len(batches)):
        for pair in pairs:
            for q in range(len(quads)):
                if pair[0] in batches[batch] and (q > 1 or pair not in early):
                    multiply(pair, q)
        project(batch)
        deliver(batch)

    for buffer, send in (
        (columns.at[pl.ds(0, size - 1), 0], 0),
        (columns.at[pl.ds(0, size - 1), 0], 1),
        (columns.at[:, 0], 2),
        (stage.at[pl.ds(0, size - 1)], 3),
    ):
        pltpu.make_async_copy(buffer, buffer, sends.at[send]).wait()
    arrived = stage.at[pl.ds(0, size - 1)]
    pltpu.make_async_copy(arrived, arrived, out_recv).wait()
    own = stage.at[ranks.index(0)]
    pltpu.make_async_copy(own, own, local_sem.at[1]).wait()
    after_copy.wait()


def attend_pairs(x, large, small, size):
    seqs, residues = large[0].shape
    part, _, width = x.shape
    chips = size * size
    chip_rows = residues // chips
    sites = chip_rows // 2
    pack = sites * OUTER_CHANNELS
    couple = large[-1]
    count = size * chip_rows
    x = x.reshape(part, chips, chip_rows, width)
    hbm = pl.BlockSpec(memory_space=pl.ANY)
    vmem = pl.BlockSpec(memory_space=pltpu.VMEM)
    dma = pltpu.SemaphoreType.DMA
    return pl.pallas_call(
        functools.partial(core_kernel, size),
        out_shape=(
            jax.ShapeDtypeStruct((seqs, sites, width), BF16),
            jax.ShapeDtypeStruct((sites, size, size, chip_rows, PAIR_DIM), BF16),
        ),
        in_specs=[hbm] * (1 + len(large)) + [vmem] * len(small),
        out_specs=(hbm, hbm),
        scratch_shapes=[
            pltpu.VMEM(x.shape, BF16),
            pltpu.VMEM((2, chips, part, chip_rows, width), BF16),
            *[pltpu.VMEM(a.shape, a.dtype) for a in (large[0], *large[1:])],
            pltpu.VMEM((sites, seqs, width), BF16),
            pltpu.VMEM((sites, seqs, width), BF16),
            pltpu.VMEM((8, seqs), F32),
            pltpu.VMEM((count, size * pack), F32),
            pltpu.VMEM((size, sites, OUTER_CHANNELS, seqs), BF16),
            pltpu.VMEM((size, 2, sites, OUTER_CHANNELS, seqs), BF16),
            pltpu.VMEM((OUTER_CHANNELS * pack, sites * PAIR_DIM), BF16),
            pltpu.VMEM(couple.shape, F32),
            pltpu.VMEM((4, 2 * chip_rows * PITCH, pack), F32),
            pltpu.VMEM((size * count, OUTER_CHANNELS * pack), BF16),
            pltpu.VMEM((size * count, sites * PAIR_DIM), F32),
            pltpu.VMEM((size, sites, size, chip_rows, PAIR_DIM), BF16),
            pltpu.VMEM((seqs, sites, width), BF16),
            dma((sites, size + 1)),
            dma((sites, size + 1)),
            dma((sites, size + 1)),
            dma,
            dma((4,)),
            dma((3,)),
            dma((6,)),
            dma,
            dma,
            dma((2,)),
        ],
        compiler_params=pltpu.CompilerParams(
            vmem_limit_bytes=VMEM_LIMIT, collective_id=1, has_side_effects=True
        ),
        name="attend_pairs",
    )(x, *large, *small)


def hand_over_kernel(*refs):
    count = len(refs) // 4
    sources, targets, held = refs[:count], refs[count : 2 * count], refs[2 * count : 3 * count]
    into, out_of = refs[3 * count :][:2]
    pieces = []
    for source, target, room in zip(sources, targets, held):
        for k in range(4):
            rows = pl.ds(k * source.shape[0] // 4, source.shape[0] // 4)
            at = len(pieces)
            pieces.append(
                (
                    pltpu.make_async_copy(source.at[rows], room.at[rows], into.at[at]),
                    pltpu.make_async_copy(room.at[rows], target.at[rows], out_of.at[at]),
                )
            )
    for first, _ in pieces:
        first.start()
    for first, second in pieces:
        first.wait()
        second.start()
    for _, second in pieces:
        second.wait()


def hand_over(*arrays):
    hbm = pl.BlockSpec(memory_space=pl.ANY)
    return pl.pallas_call(
        hand_over_kernel,
        out_shape=tuple(jax.ShapeDtypeStruct(a.shape, a.dtype) for a in arrays),
        in_specs=[hbm] * len(arrays),
        out_specs=(hbm,) * len(arrays),
        scratch_shapes=[pltpu.VMEM(a.shape, a.dtype) for a in arrays]
        + [pltpu.SemaphoreType.DMA((4 * len(arrays),))] * 2,
        name="hand_over",
    )(*arrays)


def shards(
    homolog_stack_tensor,
    occupancy_indicator,
    chain_existence_flags,
    focus_normal_factor,
    focus_normal_addend,
    probe_index_weights,
    payload_valve_weights,
    logistic_valve_addend,
    focus_exit_weights,
    focus_exit_addend,
    product_mean_layer_stretch,
    product_mean_layer_shift,
    twin_map_matrix,
    twin_map_shift,
    couple_map_matrix,
    couple_map_shift,
):
    seqs, residues = occupancy_indicator.shape
    width = homolog_stack_tensor.shape[-1]
    size = lax.axis_size("dap_0")
    row = lambda v: v[None, :]
    after, pair_rows = attend_pairs(
        homolog_stack_tensor,
        (
            occupancy_indicator,
            probe_index_weights,
            payload_valve_weights,
            focus_exit_weights,
            couple_map_matrix,
        ),
        (
            row(chain_existence_flags),
            row(focus_normal_factor),
            row(focus_normal_addend),
            row(logistic_valve_addend),
            row(focus_exit_addend),
            row(product_mean_layer_stretch),
            row(product_mean_layer_shift),
            twin_map_matrix.T,
            row(twin_map_shift),
            row(couple_map_shift),
        ),
        size,
    )
    return hand_over(after, pair_rows.reshape(-1, residues, PAIR_DIM))


def solution(mesh):
    split = Mesh(
        mesh.devices.reshape(mesh.shape["grp"], 8, 8, 2), ("grp", "dap_0", "dap_1", "dap_2")
    )
    return jax.shard_map(
        shards,
        mesh=split,
        in_specs=(
            P(GRP_DAP, None, None),
            P("grp", None),
            P("grp"),
            P(),
            P(),
            P(),
            P(),
            P(),
            P(),
            P(),
            P(),
            P(),
            P(),
            P(),
            P(),
            P(),
        ),
        out_specs=(P("grp", DAP, None), P(GRP_DAP, None, None)),
        check_vma=False,
    )
```
